32 devices in a mesh: dp: 2 (over x), ep: 16 (over z, y, core).
Axes of the slice: x: 2, y: 2, z: 4, core: 2. Of those that a mesh axis runs over, the one named last changes fastest.
Arguments:
- tokens: bfloat16 [4096, 2048], P(('dp', 'ep')), parts along dimension 0
- expert_ids: int32 [4096, 8], P(('dp', 'ep')), parts along dimension 0
- norm_gain: bfloat16 [2048], replicated
- w_router: bfloat16 [2048, 128], replicated
- w_gate: bfloat16 [128, 2048, 768], P('ep')
- w_up: bfloat16 [128, 2048, 768], P('ep')
- w_down: bfloat16 [128, 768, 2048], P('ep')
Outputs:
- output: bfloat16 [4096, 2048], P(('dp', 'ep')), parts along dimension 0
There are 2 independent parts. The reference program is written for one: setup_inputs(seed, part) draws one part's arguments, and reference() takes and returns one part's arrays. A program takes and returns all parts, laid end to end along the dimension named above; an argument that names none is the same for every part.
All inputs are finite; a program needn't handle non-finite values.
Results may differ from the reference program's by a relative error of at most 0.00575139.
Values are sent between devices in bfloat16 or wider.
A program may use at most 1 GiB of HBM per device.

```python
import jax
import jax.numpy as jnp
from jax import lax

D = 2048
EXPERTS = 128
TOP = 8
FF = 768
TOKENS_DEV = 128
EP_SIZE = 16
BLOCK_ROWS = 128

TOKENS = EP_SIZE * TOKENS_DEV
PAIRS = TOKENS * TOP
E_LOCAL = EXPERTS // EP_SIZE
NUM_BLOCKS = PAIRS // BLOCK_ROWS + EXPERTS + 1
NORM_EPS = 1e-5


def draw_routes(route_key):
    sub_keys = jax.random.split(route_key, 6)
    pair_dev = TOKENS_DEV * TOP
    half_mean = pair_dev // (2 * EP_SIZE)
    hot_dev = jax.random.randint(sub_keys[0], (), 0, EP_SIZE)
    rotation = jax.random.randint(sub_keys[1], (), 0, EP_SIZE - 1)
    rest_weight = jax.random.randint(sub_keys[2], (EP_SIZE - 2,), 1, 3)
    rest_cum = jnp.concatenate([jnp.zeros((1,), jnp.int32), jnp.cumsum(rest_weight)])
    rest_bound = (pair_dev - 7 * half_mean) * rest_cum // rest_cum[-1]
    pattern = jnp.concatenate([jnp.full((1,), 4 * half_mean, jnp.int32), rest_bound[1:] - rest_bound[:-1]])
    src_dev = jnp.arange(EP_SIZE)[:, None]
    dst_dev = jnp.arange(EP_SIZE)[None, :]
    shift_idx = ((dst_dev - hot_dev - 1) % EP_SIZE - src_dev - rotation) % (EP_SIZE - 1)
    dev_load = jnp.where(dst_dev == hot_dev, 3 * half_mean, pattern[shift_idx])
    split_weight = jax.random.randint(sub_keys[3], (EP_SIZE, EP_SIZE, E_LOCAL), 1, 4)
    split_cum = jnp.concatenate([jnp.zeros((EP_SIZE, EP_SIZE, 1), jnp.int32), jnp.cumsum(split_weight, axis=2)], axis=2)
    split_bound = dev_load[:, :, None] * split_cum // split_cum[:, :, -1:]
    expert_count = (split_bound[:, :, 1:] - split_bound[:, :, :-1]).reshape(EP_SIZE, EXPERTS)
    count_end = jnp.cumsum(expert_count, axis=1)
    positions = jnp.arange(pair_dev)
    sorted_ids = jax.vmap(lambda end_row: jnp.searchsorted(end_row, positions, side='right'))(count_end)
    by_token = sorted_ids.reshape(EP_SIZE, TOP, TOKENS_DEV).transpose(0, 2, 1)
    tok_perm = jax.vmap(lambda perm_key: jax.random.permutation(perm_key, TOKENS_DEV))(jax.random.split(sub_keys[4], EP_SIZE))
    by_token = jnp.take_along_axis(by_token, jnp.broadcast_to(tok_perm[:, :, None], (EP_SIZE, TOKENS_DEV, TOP)), axis=1)
    turn = jax.random.randint(sub_keys[5], (EP_SIZE, TOKENS_DEV, 1), 0, TOP)
    col_idx = (jnp.arange(TOP)[None, None, :] + turn) % TOP
    by_token = jnp.take_along_axis(by_token, col_idx, axis=2)
    return by_token.reshape(TOKENS, TOP).astype(jnp.int32)


def setup_inputs(seed: int = 0, part: int = 0) -> dict:
    part_key = jax.random.fold_in(jax.random.key(seed), part)
    tok_key, route_key = jax.random.split(part_key)
    shared = jax.random.split(jax.random.key(seed + 1), 5)
    tokens = jax.random.normal(tok_key, (TOKENS, D), jnp.float32).astype(jnp.bfloat16)
    norm_gain = (1.0 + 0.3 * jax.random.normal(shared[0], (D,), jnp.float32)).astype(jnp.bfloat16)
    w_router = (jax.random.normal(shared[1], (D, EXPERTS), jnp.float32) * D ** -0.5).astype(jnp.bfloat16)
    w_gate = (jax.random.normal(shared[2], (EXPERTS, D, FF), jnp.float32) * D ** -0.5).astype(jnp.bfloat16)
    w_up = (jax.random.normal(shared[3], (EXPERTS, D, FF), jnp.float32) * D ** -0.5).astype(jnp.bfloat16)
    w_down = (jax.random.normal(shared[4], (EXPERTS, FF, D), jnp.float32) * (EXPERTS / 4 * FF ** -0.5)).astype(jnp.bfloat16)
    expert_ids = draw_routes(route_key)
    return {'tokens': tokens, 'expert_ids': expert_ids, 'norm_gain': norm_gain, 'w_router': w_router, 'w_gate': w_gate, 'w_up': w_up, 'w_down': w_down}


def reference(tokens, expert_ids, norm_gain, w_router, w_gate, w_up, w_down):
    tok32 = tokens.astype(jnp.float32)
    inv_rms = lax.rsqrt(jnp.mean(tok32 * tok32, axis=1, keepdims=True) + NORM_EPS)
    normed = (tok32 * inv_rms * norm_gain.astype(jnp.float32)).astype(jnp.bfloat16)
    logits = jnp.dot(normed, w_router, preferred_element_type=jnp.float32)
    router_prob = jax.nn.softmax(logits, axis=1)
    gate_vals = jnp.take_along_axis(router_prob, expert_ids, axis=1)
    flat_ids = expert_ids.reshape(PAIRS)
    sort_order = jnp.argsort(flat_ids, stable=True)
    sorted_ids = flat_ids[sort_order]
    counts = jnp.bincount(flat_ids, length=EXPERTS)
    padded = (counts + BLOCK_ROWS - 1) // BLOCK_ROWS * BLOCK_ROWS
    pad_end = jnp.cumsum(padded)
    group_start = jnp.cumsum(counts) - counts
    slot_sorted = pad_end[sorted_ids] - padded[sorted_ids] + jnp.arange(PAIRS) - group_start[sorted_ids]
    row_buf = jnp.zeros((NUM_BLOCKS * BLOCK_ROWS, D), jnp.bfloat16).at[slot_sorted].set(normed[sort_order // TOP])
    block_expert = jnp.minimum(jnp.searchsorted(pad_end, jnp.arange(NUM_BLOCKS) * BLOCK_ROWS, side='right'), EXPERTS - 1)

    def block_apply(block_args):
        block_rows, expert = block_args
        hidden_gate = jnp.dot(block_rows, w_gate[expert], preferred_element_type=jnp.float32)
        hidden_up = jnp.dot(block_rows, w_up[expert], preferred_element_type=jnp.float32)
        swiglu_out = (jax.nn.silu(hidden_gate) * hidden_up).astype(jnp.bfloat16)
        return jnp.dot(swiglu_out, w_down[expert], preferred_element_type=jnp.float32).astype(jnp.bfloat16)

    block_out = lax.map(block_apply, (row_buf.reshape(NUM_BLOCKS, BLOCK_ROWS, D), block_expert))
    slot_pair = jnp.zeros((PAIRS,), jnp.int32).at[sort_order].set(slot_sorted)
    pair_out = block_out.reshape(NUM_BLOCKS * BLOCK_ROWS, D)[slot_pair].reshape(TOKENS, TOP, D)
    moe_sum = jnp.einsum('nk,nkd->nd', gate_vals, pair_out.astype(jnp.float32))
    return (tok32 + moe_sum).astype(jnp.bfloat16)
```

```python
import functools

import jax
import jax.numpy as jnp
from jax import lax
from jax.experimental import pallas as pl
from jax.experimental.pallas import tpu as pltpu
from jax.sharding import PartitionSpec as P

NORM_EPS = 1e-5
LANES = 128
BM = 256


def rms_norm(tok_rows, norm_gain):
    tok32 = tok_rows.astype(jnp.float32)
    inv_rms = lax.rsqrt(jnp.mean(tok32 * tok32, axis=1, keepdims=True) + NORM_EPS)
    return (tok32 * inv_rms * norm_gain.astype(jnp.float32)).astype(jnp.bfloat16)


def expert_kernel(n_src, sub, cnt, lst, gts, u_hbm, w1, w3, w2, out_hbm, u_vm, acc, xf, xb, hb, o3, sems):
    e = pl.program_id(0)
    n_exp = pl.num_programs(0)

    @pl.when(e == 0)
    def _():
        cp = pltpu.make_async_copy(u_hbm, u_vm, sems.at[0])
        cp.start()

        @pl.loop(0, acc.shape[0] // 256)
        def _(i):
            acc[pl.ds(pl.multiple_of(i * 256, 256), 256), :] = jnp.zeros((256, LANES), jnp.float32)

        cp.wait()

    def block(s0):
        def gather_src(carry):
            s, n = carry
            c = cnt[s, e]
            base = (s * n_exp + e) * LANES

            def row(i, _):
                t = s * LANES + lst[base + i]
                src = u_vm[pl.ds(pl.multiple_of(t * sub, sub), sub), :]
                xf[pl.ds(pl.multiple_of((n + i) * sub, sub), sub), :] = src.astype(jnp.float32)
                return 0

            lax.fori_loop(0, c, row, 0)
            return s + 1, n + c

        def fits(carry):
            s, n = carry
            return jnp.logical_and(s < n_src, n + cnt[jnp.minimum(s, n_src - 1), e] <= BM)

        s1, n_rows = lax.while_loop(fits, gather_src, (s0, jnp.int32(0)))

        @pl.when(n_rows > 0)
        def _():
            for j in range(sub):
                xb[:, j * LANES:(j + 1) * LANES] = xf[pl.ds(j, BM, stride=sub), :].astype(jnp.bfloat16)
            g = jnp.dot(xb[...], w1[0], preferred_element_type=jnp.float32)
            v = jnp.dot(xb[...], w3[0], preferred_element_type=jnp.float32)
            hb[...] = (jax.nn.silu(g) * v).astype(jnp.bfloat16)
            for q in range(sub // 4):
                o = jnp.dot(hb[...], w2[0, :, q * 512:(q + 1) * 512], preferred_element_type=jnp.float32)
                o = o.astype(jnp.bfloat16).astype(jnp.float32)
                for j in range(4):
                    o3[pl.ds(q * 4 + j, BM, stride=sub), :] = o[:, j * LANES:(j + 1) * LANES]

            def scatter_src(s, n):
                c = cnt[s, e]
                base = (s * n_exp + e) * LANES

                def row(i, _):
                    t = s * LANES + lst[base + i]
                    ts = pl.ds(pl.multiple_of(t * sub, sub), sub)
                    acc[ts, :] += gts[base + i] * o3[pl.ds(pl.multiple_of((n + i) * sub, sub), sub), :]
                    return 0

                lax.fori_loop(0, c, row, 0)
                return n + c

            lax.fori_loop(s0, s1, scatter_src, jnp.int32(0))

        return s1

    lax.while_loop(lambda s: s < n_src, block, jnp.int32(0))

    @pl.when(e == n_exp - 1)
    def _():
        cp = pltpu.make_async_copy(acc, out_hbm, sems.at[0])
        cp.start()
        cp.wait()


def experts(n_src, cnt, lst, gts, u_rows, w1, w3, w2):
    n_exp, width, ff = w1.shape
    sub = width // LANES
    n_tok = u_rows.shape[0] // sub
    any_spec = pl.BlockSpec(memory_space=pl.ANY)
    smem = pl.BlockSpec(memory_space=pltpu.SMEM)
    return pl.pallas_call(
        functools.partial(expert_kernel, n_src, sub),
        grid=(n_exp,),
        out_shape=jax.ShapeDtypeStruct((n_tok * sub, LANES), jnp.float32),
        in_specs=[smem, smem, smem, any_spec,
                  pl.BlockSpec((1, width, ff), lambda e: (e, 0, 0)),
                  pl.BlockSpec((1, width, ff), lambda e: (e, 0, 0)),
                  pl.BlockSpec((1, ff, width), lambda e: (e, 0, 0))],
        out_specs=any_spec,
        scratch_shapes=[
            pltpu.VMEM((n_tok * sub, LANES), jnp.bfloat16),
            pltpu.VMEM((n_tok * sub, LANES), jnp.float32),
            pltpu.VMEM((BM * sub, LANES), jnp.float32),
            pltpu.VMEM((BM, width), jnp.bfloat16),
            pltpu.VMEM((BM, ff), jnp.bfloat16),
            pltpu.VMEM((BM * sub, LANES), jnp.float32),
            pltpu.SemaphoreType.DMA((1,)),
        ],
        compiler_params=pltpu.CompilerParams(vmem_limit_bytes=66_000_000, dimension_semantics=("arbitrary",)),
        name="experts",
    )(cnt, lst, gts, u_rows, w1, w3, w2)


def route_lists(expert_ids, router_prob, n_all):
    n_tok = expert_ids.shape[0]
    hit = jnp.any(expert_ids[:, :, None] == jnp.arange(n_all)[None, None, :], axis=1)
    hit_b = hit.astype(jnp.bfloat16)
    tri = (jnp.arange(n_tok)[:, None] > jnp.arange(n_tok)[None, :]).astype(jnp.bfloat16)
    pos = jnp.dot(tri, hit_b, preferred_element_type=jnp.float32).astype(jnp.int32)
    pos = jnp.where(hit, pos, n_tok)
    sel = pos[:, :, None] == jnp.arange(n_tok)[None, None, :]
    tok = jnp.sum(jnp.where(sel, jnp.arange(n_tok, dtype=jnp.float32)[:, None, None], 0.0), axis=0)
    gate = jnp.sum(jnp.where(sel, router_prob[:, :, None], 0.0), axis=0)
    count = jnp.sum(hit.astype(jnp.float32), axis=0)
    return count, tok, gate


def solution(mesh):
    ep_size = mesh.shape['ep']

    def device_step(tokens, expert_ids, norm_gain, w_router, w_gate, w_up, w_down):
        tok_count, width = tokens.shape
        e_local = w_gate.shape[0]
        n_all = ep_size * e_local
        sub = width // LANES
        normed = rms_norm(tokens, norm_gain)
        u_rows = lax.all_gather(normed.reshape(tok_count * sub, LANES), 'ep', axis=0, tiled=True)
        router_prob = jax.nn.softmax(jnp.dot(normed, w_router, preferred_element_type=jnp.float32), axis=1)
        count, tok, gate = route_lists(expert_ids, router_prob, n_all)
        meta = jnp.concatenate([tok.reshape(ep_size, e_local, LANES), gate.reshape(ep_size, e_local, LANES),
                                jnp.broadcast_to(count.reshape(ep_size, e_local, 1), (ep_size, e_local, LANES))], axis=1)
        meta = lax.all_to_all(meta, 'ep', 0, 0, tiled=True)
        lst = meta[:, :e_local].astype(jnp.int32).reshape(-1)
        gts = meta[:, e_local:2 * e_local].reshape(-1)
        cnt = meta[:, 2 * e_local:, 0].astype(jnp.int32)
        part = experts(ep_size, cnt, lst, gts, u_rows, w_gate, w_up, w_down)
        moe_sum = lax.psum_scatter(part, 'ep', scatter_dimension=0, tiled=True)
        return (tokens.astype(jnp.float32) + moe_sum.reshape(tok_count, width)).astype(jnp.bfloat16)

    row_spec = P(('dp', 'ep'), None)
    expert_spec = P('ep', None, None)
    return jax.shard_map(device_step, mesh=mesh, in_specs=(row_spec, row_spec, P(None), P(None, None), expert_spec, expert_spec, expert_spec), out_specs=row_spec, check_vma=False)
```

```python
import functools

import jax
import jax.numpy as jnp
from jax import lax
from jax.experimental import pallas as pl
from jax.experimental.pallas import tpu as pltpu
from jax.sharding import PartitionSpec as P

NORM_EPS = 1e-5
LANES = 128
BM = 256
WIN = 256
TILE = 16
QUAD = 4
PLANES = 4
F32 = jnp.float32
BF16 = jnp.bfloat16


def iota(shape, dim):
    return lax.broadcasted_iota(jnp.int32, shape, dim)


def place():
    me = lax.axis_index('ep')
    return me, me // QUAD, lax.rem(me, QUAD)


def remote(src, dst, send, recv, dev):
    return pltpu.make_async_remote_copy(src_ref=src, dst_ref=dst, send_sem=send, recv_sem=recv,
                                        device_id={'ep': dev}, device_id_type=pl.DeviceIdType.MESH)


def spread_kernel(r_max, x_ref, ids_ref, gain_ref, wr_ref, u_hbm, meta_hbm, ints_hbm,
                  u_all, xs, ub, pos_s, p_s, packet, meta, ints,
                  send_u, recv_u, send_m, recv_m, out_sem):
    n_dev = PLANES * QUAD
    me, z, q = place()
    y, c = q // 2, lax.rem(q, 2)
    half = u_all.shape[1] // 2
    tok = x_ref.shape[0]
    sub = u_all.shape[1] // tok

    barrier = pltpu.get_barrier_semaphore()
    for d in range(1, n_dev):
        pl.semaphore_signal(barrier, inc=1, device_id={'ep': lax.rem(me + d, n_dev)}, device_id_type=pl.DeviceIdType.MESH)

    x32 = x_ref[...].astype(F32)
    inv = lax.rsqrt(jnp.mean(x32 * x32, axis=1, keepdims=True) + NORM_EPS)
    ub[...] = (x32 * inv * gain_ref[...].astype(F32)).astype(BF16)
    for j in range(sub):
        xs[pl.ds(j, tok, stride=sub), :] = ub[:, j * LANES:(j + 1) * LANES].astype(F32)
    u_all[me] = xs[...].astype(BF16)
    pl.semaphore_wait(barrier, n_dev - 1)

    dest = (me + QUAD, me - QUAD, z * QUAD + (1 - y) * 2 + c, z * QUAD + y * 2 + 1 - c)

    def hop(b, h, way):
        rows = u_all.at[b, pl.ds(h * half, half)]
        return remote(rows, rows, send_u.at[b, h, way], recv_u.at[b, h], dest[way])

    def out_copy(b, h):
        rows = pl.ds(h * half, half)
        return pltpu.make_async_copy(u_all.at[b, rows], u_hbm.at[b, rows], out_sem.at[b, h])

    for h in range(2):
        @pl.when(z < PLANES - 1)
        def _():
            hop(me, h, 0).start()

        @pl.when(z > 0)
        def _():
            hop(me, h, 1).start()

        hop(me, h, 2).start()
        hop(me, h, 3).start()
        out_copy(me, h).start()

    logits = jnp.dot(ub[...], wr_ref[...], preferred_element_type=F32)
    top = jnp.max(logits, axis=1, keepdims=True)
    ex = jnp.exp(logits - top)
    p_s[...] = ex / jnp.sum(ex, axis=1, keepdims=True)
    lane = iota((tok, LANES), 1)
    hit = lane < 0
    for k in range(ids_ref.shape[1]):
        hit = jnp.logical_or(hit, ids_ref[:, k:k + 1] == lane)
    hit32 = hit.astype(F32)
    hit_b = hit32.astype(BF16)
    tri = (iota((tok, tok), 0) > iota((tok, tok), 1)).astype(F32).astype(BF16)
    rank = jnp.dot(tri, hit_b, preferred_element_type=F32)
    count = jnp.sum(hit32, axis=0, keepdims=True)
    row_e, col_e = iota((LANES, LANES), 0), iota((LANES, LANES), 1)
    e_loc = LANES // n_dev
    before = jnp.logical_and(row_e < col_e, row_e // e_loc == col_e // e_loc).astype(F32).astype(BF16)
    count8 = jnp.broadcast_to(count, (8, LANES))
    base = jnp.dot(count8.astype(BF16), before, preferred_element_type=F32)[0:1]
    pos_s[...] = jnp.where(hit, base + rank, -1.0)
    t_id = iota((tok, LANES), 0).astype(F32)
    lane_f = lane.astype(F32)

    def pack(zd, _):
        for m in range(QUAD):
            tk = jnp.zeros((tok, LANES), F32)
            gt = jnp.zeros((tok, LANES), F32)
            for ee in range(e_loc):
                col = m * e_loc + ee
                at = pos_s[:, col:col + 1] == lane_f
                tk = jnp.where(at, t_id, tk)
                gt = jnp.where(at, p_s[:, col:col + 1], gt)
            packet[zd, m:m + 1, :] = jnp.sum(tk, axis=0, keepdims=True)
            packet[zd, QUAD + m:QUAD + m + 1, :] = jnp.sum(gt, axis=0, keepdims=True)
        packet[zd, 8:16, :] = count8
        pos_s[...] = pltpu.roll(pos_s[...], LANES - QUAD * e_loc, 1)
        p_s[...] = pltpu.roll(p_s[...], LANES - QUAD * e_loc, 1)
        return 0

    lax.fori_loop(0, PLANES, pack, 0)

    def route_copy(d):
        return remote(packet.at[d // QUAD], meta.at[me], send_m.at[d], recv_m.at[me], d)

    for d in range(n_dev):
        @pl.when(d != me)
        def _():
            route_copy(d).start()

    meta[me] = packet[z]

    def take(b, h, ways):
        hop(b, h, 3).wait_recv()
        out_copy(b, h).start()
        for way in ways:
            hop(b, h, way).start()

    def from_z(d, fn):
        @pl.when(z >= d)
        def _():
            fn(me - QUAD * d, 0, z < PLANES - 1)

        @pl.when(z + d < PLANES)
        def _():
            fn(me + QUAD * d, 1, z > 0)

    def across(zb):
        return zb * QUAD + (1 - y) * 2 + c

    def step_z(d):
        for h in range(2):
            def on(b, way, more):
                hop(b, h, 3).wait_recv()

                @pl.when(more)
                def _():
                    hop(b, h, way).start()

                hop(b, h, 2).start()
                hop(b, h, 3).start()
                out_copy(b, h).start()

            from_z(d, on)

    def step_y(d):
        for h in range(2):
            if d == 0:
                take(across(z), h, (3,))
            else:
                @pl.when(z >= d)
                def _():
                    take(across(z - d), h, (3,))

                @pl.when(z + d < PLANES)
                def _():
                    take(across(z + d), h, (3,))

    step_z(1)
    step_y(0)
    step_z(2)
    step_y(1)
    step_z(3)
    step_y(2)
    step_y(3)
    for b in range(n_dev):
        @pl.when(b % 2 != c)
        def _():
            for h in range(2):
                hop(b, h, 3).wait_recv()
                out_copy(b, h).start()

    for d in range(n_dev):
        @pl.when(d != me)
        def _():
            remote(packet.at[0], meta.at[d], send_m.at[d], recv_m.at[d], d).wait_recv()

    cnt = meta[:, 8, :]
    group = (iota((LANES, LANES), 0) // e_loc == iota((LANES, LANES), 1)).astype(F32).astype(BF16)
    n_rows = jnp.dot(cnt.astype(BF16), group, preferred_element_type=F32)
    ints[0:16, :] = meta[:, pl.ds(q, 1), :].reshape(n_dev, LANES).astype(jnp.int32)
    ints[16:32, :] = cnt.astype(jnp.int32)
    run = jnp.zeros((1, LANES), F32)
    for s in range(n_dev):
        off = run.astype(jnp.int32)
        ints[32 + s:33 + s, :] = off
        ints[48 + s:49 + s, :] = jnp.minimum(off // TILE, (r_max - WIN) // TILE)
        run = run + n_rows[s:s + 1]

    tail = [pltpu.make_async_copy(meta, meta_hbm, out_sem.at[0, 2]), pltpu.make_async_copy(ints, ints_hbm, out_sem.at[1, 2])]
    for cp in tail:
        cp.start()

    for h in range(2):
        def sent(b, way, more):
            @pl.when(more)
            def _():
                hop(b, h, way).wait_send()

            hop(b, h, 2).wait_send()
            hop(b, h, 3).wait_send()

        @pl.when(z < PLANES - 1)
        def _():
            hop(me, h, 0).wait_send()

        @pl.when(z > 0)
        def _():
            hop(me, h, 1).wait_send()

        hop(me, h, 2).wait_send()
        hop(me, h, 3).wait_send()
        for d in range(1, PLANES):
            from_z(d, sent)
        for zb in range(PLANES):
            hop(across(zb), h, 3).wait_send()
        for b in range(n_dev):
            out_copy(b, h).wait()
    for d in range(n_dev):
        @pl.when(d != me)
        def _():
            route_copy(d).wait_send()
    for cp in tail:
        cp.wait()


def spread(r_max, tokens, expert_ids, norm_gain, w_router):
    tok, width = tokens.shape
    n_dev = PLANES * QUAD
    sub = width // LANES
    any_spec = pl.BlockSpec(memory_space=pl.ANY)
    vmem = pl.BlockSpec(memory_space=pltpu.VMEM)
    return pl.pallas_call(
        functools.partial(spread_kernel, r_max),
        out_shape=(jax.ShapeDtypeStruct((n_dev, tok * sub, LANES), BF16),
                   jax.ShapeDtypeStruct((n_dev, 16, LANES), F32),
                   jax.ShapeDtypeStruct((64, LANES), jnp.int32)),
        in_specs=[vmem] * 4,
        out_specs=(any_spec, any_spec, any_spec),
        scratch_shapes=[
            pltpu.VMEM((n_dev, tok * sub, LANES), BF16),
            pltpu.VMEM((tok * sub, LANES), F32),
            pltpu.VMEM((tok, width), BF16),
            pltpu.VMEM((tok, LANES), F32),
            pltpu.VMEM((tok, LANES), F32),
            pltpu.VMEM((PLANES, 16, LANES), F32),
            pltpu.VMEM((n_dev, 16, LANES), F32),
            pltpu.VMEM((64, LANES), jnp.int32),
            pltpu.SemaphoreType.DMA((n_dev, 2, 4)),
            pltpu.SemaphoreType.DMA((n_dev, 2)),
            pltpu.SemaphoreType.DMA((n_dev,)),
            pltpu.SemaphoreType.DMA((n_dev,)),
            pltpu.SemaphoreType.DMA((n_dev, 3)),
        ],
        compiler_params=pltpu.CompilerParams(collective_id=0, has_side_effects=True, vmem_limit_bytes=32 * 2 ** 20),
        name="spread",
    )(tokens, expert_ids, norm_gain.reshape(1, width), w_router)


def expert_kernel(n_src, sub, r_max, ints, meta, u_hbm, w1, w3, w2, o_hbm, win_hbm,
                  u_vm, o_all, xf, xb, hb, o3, ob, win, sems):
    e = pl.program_id(0)
    n_exp = pl.num_programs(0)
    me, z, q = place()

    @pl.when(e == 0)
    def _():
        cp = pltpu.make_async_copy(u_hbm, u_vm, sems.at[0])
        cp.start()

        @pl.loop(0, o_all.shape[0] // 256)
        def _(i):
            o_all[pl.ds(pl.multiple_of(i * 256, 256), 256), :] = jnp.zeros((256, LANES), F32)

        @pl.loop(0, n_src)
        def _(s):
            for m in range(QUAD):
                t = meta[s, m:m + 1, :]
                g = meta[s, QUAD + m:QUAD + m + 1, :]
                hi = g.astype(BF16).astype(F32)
                mid = (g - hi).astype(BF16).astype(F32)
                lo = (g - hi - mid).astype(BF16).astype(F32)
                rows = jnp.concatenate([t, hi, mid, lo, t, t, t, t], axis=0)
                rows = jnp.concatenate([rows, jnp.zeros((8, WIN - LANES), F32)], axis=1)
                r = z * QUAD + m
                win[s * QUAD + m] = pltpu.roll(rows, ints[32 + s, r] - TILE * ints[48 + s, r], 1)

        pltpu.make_async_copy(win, win_hbm, sems.at[1]).start()
        cp.wait()

    lane0 = me * n_exp

    def first(s):
        def add(k, v):
            return v + ints[16 + s, lane0 + k]

        return lax.fori_loop(0, e, add, jnp.int32(0))

    def block(s0):
        def gather_src(carry):
            s, n = carry
            cnt = ints[16 + s, lane0 + e]
            j0 = first(s)

            def row(i, _):
                t = s * LANES + ints[s, j0 + i]
                src = u_vm[pl.ds(pl.multiple_of(t * sub, sub), sub), :]
                xf[pl.ds(pl.multiple_of((n + i) * sub, sub), sub), :] = src.astype(F32)
                return 0

            lax.fori_loop(0, cnt, row, 0)
            return s + 1, n + cnt

        def fits(carry):
            s, n = carry
            return jnp.logical_and(s < n_src, n + ints[16 + jnp.minimum(s, n_src - 1), lane0 + e] <= BM)

        s1, n_rows = lax.while_loop(fits, gather_src, (s0, jnp.int32(0)))

        @pl.when(n_rows > 0)
        def _():
            for j in range(sub):
                xb[:, j * LANES:(j + 1) * LANES] = xf[pl.ds(j, BM, stride=sub), :].astype(BF16)
            g = jnp.dot(xb[...], w1[0], preferred_element_type=F32)
            v = jnp.dot(xb[...], w3[0], preferred_element_type=F32)
            hb[...] = (jax.nn.silu(g) * v).astype(BF16)
            for k in range(sub // 4):
                o = jnp.dot(hb[...], w2[0, :, k * 512:(k + 1) * 512], preferred_element_type=F32)
                for j in range(4):
                    o3[pl.ds(k * 4 + j, BM, stride=sub), :] = o[:, j * LANES:(j + 1) * LANES]

            def scatter_src(s, n):
                cnt = ints[16 + s, lane0 + e]
                slot = ints[32 + s, me] + first(s)

                def row(i, _):
                    o_all[pl.ds(pl.multiple_of((slot + i) * sub, sub), sub), :] = o3[pl.ds(pl.multiple_of((n + i) * sub, sub), sub), :]
                    return 0

                lax.fori_loop(0, cnt, row, 0)
                return n + cnt

            lax.fori_loop(s0, s1, scatter_src, jnp.int32(0))

        return s1

    lax.while_loop(lambda s: s < n_src, block, jnp.int32(0))

    @pl.when(e == n_exp - 1)
    def _():
        def put(j):
            return pltpu.make_async_copy(ob.at[j % 4], o_hbm.at[j], sems.at[2 + j % 4])

        for j in range(sub):
            if j >= 4:
                put(j - 4).wait()
            ob[j % 4] = o_all[pl.ds(j, r_max, stride=sub), :].astype(BF16)
            put(j).start()
        for j in range(sub - 4, sub):
            put(j).wait()
        pltpu.make_async_copy(win, win_hbm, sems.at[1]).wait()


def experts(n_src, r_max, ints, meta, u_rows, w1, w3, w2):
    n_exp, width, ff = w1.shape
    sub = width // LANES
    n_tok = u_rows.shape[0] // sub
    any_spec = pl.BlockSpec(memory_space=pl.ANY)
    smem = pl.BlockSpec(memory_space=pltpu.SMEM)
    return pl.pallas_call(
        functools.partial(expert_kernel, n_src, sub, r_max),
        grid=(n_exp,),
        out_shape=(jax.ShapeDtypeStruct((sub, r_max, LANES), BF16),
                   jax.ShapeDtypeStruct((n_src * QUAD, 8, WIN), F32)),
        in_specs=[smem,
                  pl.BlockSpec((n_src, 16, LANES), lambda e: (0, 0, 0)),
                  any_spec,
                  pl.BlockSpec((1, width, ff), lambda e: (e, 0, 0)),
                  pl.BlockSpec((1, width, ff), lambda e: (e, 0, 0)),
                  pl.BlockSpec((1, ff, width), lambda e: (e, 0, 0))],
        out_specs=(any_spec, any_spec),
        scratch_shapes=[
            pltpu.VMEM((n_tok * sub, LANES), BF16),
            pltpu.VMEM((r_max * sub, LANES), F32),
            pltpu.VMEM((BM * sub, LANES), F32),
            pltpu.VMEM((BM, width), BF16),
            pltpu.VMEM((BM, ff), BF16),
            pltpu.VMEM((BM * sub, LANES), F32),
            pltpu.VMEM((4, r_max, LANES), BF16),
            pltpu.VMEM((n_src * QUAD, 8, WIN), F32),
            pltpu.SemaphoreType.DMA((6,)),
        ],
        compiler_params=pltpu.CompilerParams(vmem_limit_bytes=66_000_000, dimension_semantics=("arbitrary",)),
        name="experts",
    )(ints, meta, u_rows, w1, w3, w2)


def collect_kernel(n_src, steps, ints, win, x_ref, o_hbm, out_ref,
                   mix, part, from_l, from_r, fin,
                   send_q, recv_q, send_z, recv_l, recv_r, send_f, recv_f, *rows):
    me, z, q = place()
    y, c = q // 2, lax.rem(q, 2)
    tok = x_ref.shape[0]
    plane = QUAD * tok
    others = ((1 - y) * 2 + c, (1 - y) * 2 + 1 - c, y * 2 + 1 - c)

    barrier = pltpu.get_barrier_semaphore()

    def hello(dev):
        pl.semaphore_signal(barrier, inc=1, device_id={'ep': dev}, device_id_type=pl.DeviceIdType.MESH)

    for m in others:
        hello(z * QUAD + m)

    @pl.when(z > 0)
    def _():
        hello(me - QUAD)

    @pl.when(z < PLANES - 1)
    def _():
        hello(me + QUAD)

    pl.semaphore_wait(barrier, 4 + (z + PLANES - 1) // PLANES - (z + 1) // PLANES)

    def quad_copy(k, m):
        return remote(o_hbm.at[m * steps + k], rows[k].at[q], send_q.at[k, m], recv_q.at[k, q], z * QUAD + m)

    def quad_wait(k, m):
        remote(o_hbm.at[0], rows[k].at[m], send_q.at[k, m], recv_q.at[k, m], z * QUAD + m).wait_recv()

    def own_copy(k):
        return pltpu.make_async_copy(o_hbm.at[q * steps + k], rows[k].at[q], recv_q.at[k, q])

    for k in range(steps):
        for m in others:
            quad_copy(k, m).start()
        own_copy(k).start()

    row_id = iota((tok, WIN), 0).astype(F32)

    def build(i, _):
        w = win[i]
        at = w[0:1] == row_id
        for part_i in range(3):
            mix[i, part_i * tok:(part_i + 1) * tok, :] = jnp.where(at, w[1 + part_i:2 + part_i], 0.0).astype(BF16)
        return 0

    lax.fori_loop(0, n_src * QUAD, build, 0)

    def combine(k):
        own_copy(k).wait()
        for m in others:
            quad_wait(k, m)

        def token_block(s, _):
            acc = jnp.zeros((3 * tok, LANES), F32)
            for m in range(QUAD):
                start = ints[48 + s, z * QUAD + m]
                span = jnp.concatenate([rows[k][m, start + i] for i in range(WIN // TILE)], axis=0)
                acc += jnp.dot(mix[s * QUAD + m], span, preferred_element_type=F32)
            part[k, s // QUAD, pl.ds(pl.multiple_of(lax.rem(s, QUAD) * tok, tok), tok), :] = acc[0:tok] + acc[tok:2 * tok] + acc[2 * tok:]
            return 0

        lax.fori_loop(0, n_src, token_block, 0)

    def right(k, zd):
        return remote(part.at[k, zd], from_l.at[k, zd], send_z.at[k, zd], recv_l.at[k, zd], me + QUAD)

    def left(k, zd):
        return remote(part.at[k, zd], from_r.at[k, zd], send_z.at[k, zd], recv_r.at[k, zd], me - QUAD)

    def forward(k):
        for i in range(PLANES - 1):
            for to_right in (True, False):
                zd = PLANES - 1 - i if to_right else i
                box = from_l if to_right else from_r
                go = right if to_right else left

                @pl.when(z < zd if to_right else z > zd)
                def _():
                    @pl.when(z > 0 if to_right else z < PLANES - 1)
                    def _():
                        go(k, zd).wait_recv()
                        part[k, zd] += box[k, zd]

                    go(k, zd).start()

    def final_copy(k, m):
        src = part.at[k, z, pl.ds(m * tok, tok)]
        return remote(src, fin.at[k, q], send_f.at[k, m], recv_f.at[k, q], z * QUAD + m)

    def finish(k):
        @pl.when(z > 0)
        def _():
            right(k, z).wait_recv()
            part[k, z] += from_l[k, z]

        @pl.when(z < PLANES - 1)
        def _():
            left(k, z).wait_recv()
            part[k, z] += from_r[k, z]

        for m in others:
            final_copy(k, m).start()
        fin[k, q] = part[k, z, pl.ds(pl.multiple_of(q * tok, tok), tok), :]

    for k in range(steps):
        combine(k)
        forward(k)
        if k > 0:
            finish(k - 1)
    finish(steps - 1)

    for k in range(steps):
        for m in others:
            remote(part.at[k, z, pl.ds(0, tok)], fin.at[k, m], send_f.at[k, m], recv_f.at[k, m], z * QUAD + m).wait_recv()
        for m in range(QUAD):
            cols = pl.ds((m * steps + k) * LANES, LANES)
            out_ref[:, cols] = (x_ref[:, cols].astype(F32) + fin[k, m]).astype(BF16)

    for k in range(steps):
        for m in others:
            quad_copy(k, m).wait_send()
            final_copy(k, m).wait_send()
        for zd in range(PLANES):
            @pl.when(z < zd)
            def _():
                right(k, zd).wait_send()

            @pl.when(z > zd)
            def _():
                left(k, zd).wait_send()


def collect(ints, win, tokens, o_rows):
    tok, width = tokens.shape
    sub, r_tiles = o_rows.shape[:2]
    n_src = PLANES * QUAD
    steps = sub // QUAD
    vmem = pl.BlockSpec(memory_space=pltpu.VMEM)
    return pl.pallas_call(
        functools.partial(collect_kernel, n_src, steps),
        out_shape=jax.ShapeDtypeStruct((tok, width), BF16),
        in_specs=[pl.BlockSpec(memory_space=pltpu.SMEM), vmem, vmem, pl.BlockSpec(memory_space=pl.ANY)],
        out_specs=vmem,
        scratch_shapes=[
            pltpu.VMEM((n_src * QUAD, 3 * tok, WIN), BF16),
            pltpu.VMEM((steps, PLANES, QUAD * tok, LANES), F32),
            pltpu.VMEM((steps, PLANES, QUAD * tok, LANES), F32),
            pltpu.VMEM((steps, PLANES, QUAD * tok, LANES), F32),
            pltpu.VMEM((steps, QUAD, tok, LANES), F32),
            pltpu.SemaphoreType.DMA((steps, QUAD)),
            pltpu.SemaphoreType.DMA((steps, QUAD)),
            pltpu.SemaphoreType.DMA((steps, PLANES)),
            pltpu.SemaphoreType.DMA((steps, PLANES)),
            pltpu.SemaphoreType.DMA((steps, PLANES)),
            pltpu.SemaphoreType.DMA((steps, QUAD)),
            pltpu.SemaphoreType.DMA((steps, QUAD)),
        ] + [pltpu.VMEM((QUAD, r_tiles, TILE, LANES), BF16)] * steps,
        compiler_params=pltpu.CompilerParams(collective_id=1, has_side_effects=True, vmem_limit_bytes=56 * 2 ** 20),
        name="collect",
    )(ints, win, tokens, o_rows)


def solution(mesh):
    ep_size = mesh.shape['ep']

    def device_step(tokens, expert_ids, norm_gain, w_router, w_gate, w_up, w_down):
        pairs = expert_ids.shape[0] * expert_ids.shape[1]
        r_max = 3 * pairs // 2
        u_rows, meta, ints = spread(r_max, tokens, expert_ids, norm_gain, w_router)
        u_rows = u_rows.reshape(-1, LANES)
        o_rows, win = experts(ep_size, r_max, ints, meta, u_rows, w_gate, w_up, w_down)
        return collect(ints, win, tokens, o_rows.reshape(-1, r_max // TILE, TILE, LANES))

    row_spec = P(('dp', 'ep'), None)
    expert_spec = P('ep', None, None)
    return jax.shard_map(device_step, mesh=mesh, in_specs=(row_spec, row_spec, P(None), P(None, None), expert_spec, expert_spec, expert_spec), out_specs=row_spec, check_vma=False)
```

```python
import functools

import jax
import jax.numpy as jnp
from jax import lax
from jax.experimental import pallas as pl
from jax.experimental.pallas import tpu as pltpu
from jax.sharding import PartitionSpec as P

NORM_EPS = 1e-5
LANES = 128
BM = 256
WIN = 256
TILE = 16
PITCH = 17
STEP = 8
QUAD = 4
PLANES = 4
F32 = jnp.float32
BF16 = jnp.bfloat16


def iota(shape, dim):
    return lax.broadcasted_iota(jnp.int32, shape, dim)


def place():
    me = lax.axis_index('ep')
    return me, me // QUAD, lax.rem(me, QUAD)


def remote(src, dst, send, recv, dev):
    return pltpu.make_async_remote_copy(src_ref=src, dst_ref=dst, send_sem=send, recv_sem=recv,
                                        device_id={'ep': dev}, device_id_type=pl.DeviceIdType.MESH)


def spread_kernel(r_max, x_ref, ids_ref, gain_ref, wr_ref, u_hbm, meta_hbm, ints_hbm,
                  u_all, xs, ub, pos_s, p_s, packet, meta, ints,
                  send_u, recv_u, send_m, recv_m, out_sem):
    n_dev = PLANES * QUAD
    me, z, q = place()
    y, c = q // 2, lax.rem(q, 2)
    half = u_all.shape[1] // 2
    tok = x_ref.shape[0]
    sub = u_all.shape[1] // tok

    barrier = pltpu.get_barrier_semaphore()
    for d in range(1, n_dev):
        pl.semaphore_signal(barrier, inc=1, device_id={'ep': lax.rem(me + d, n_dev)}, device_id_type=pl.DeviceIdType.MESH)

    x32 = x_ref[...].astype(F32)
    inv = lax.rsqrt(jnp.mean(x32 * x32, axis=1, keepdims=True) + NORM_EPS)
    ub[...] = (x32 * inv * gain_ref[...].astype(F32)).astype(BF16)
    for j in range(sub):
        xs[pl.ds(j, tok, stride=sub), :] = ub[:, j * LANES:(j + 1) * LANES].astype(F32)
    u_all[me] = xs[...].astype(BF16)
    pl.semaphore_wait(barrier, n_dev - 1)

    dest = (me + QUAD, me - QUAD, z * QUAD + (1 - y) * 2 + c, z * QUAD + y * 2 + 1 - c)

    def hop(b, h, way):
        rows = u_all.at[b, pl.ds(h * half, half)]
        return remote(rows, rows, send_u.at[b, h, way], recv_u.at[b, h], dest[way])

    def out_copy(b, h):
        rows = pl.ds(h * half, half)
        return pltpu.make_async_copy(u_all.at[b, rows], u_hbm.at[b, rows], out_sem.at[b, h])

    for h in range(2):
        @pl.when(z < PLANES - 1)
        def _():
            hop(me, h, 0).start()

        @pl.when(z > 0)
        def _():
            hop(me, h, 1).start()

        hop(me, h, 2).start()
        hop(me, h, 3).start()
        out_copy(me, h).start()

    logits = jnp.dot(ub[...], wr_ref[...], preferred_element_type=F32)
    top = jnp.max(logits, axis=1, keepdims=True)
    ex = jnp.exp(logits - top)
    p_s[...] = ex / jnp.sum(ex, axis=1, keepdims=True)
    lane = iota((tok, LANES), 1)
    hit = lane < 0
    for k in range(ids_ref.shape[1]):
        hit = jnp.logical_or(hit, ids_ref[:, k:k + 1] == lane)
    hit32 = hit.astype(F32)
    hit_b = hit32.astype(BF16)
    tri = (iota((tok, tok), 0) > iota((tok, tok), 1)).astype(F32).astype(BF16)
    rank = jnp.dot(tri, hit_b, preferred_element_type=F32)
    count = jnp.sum(hit32, axis=0, keepdims=True)
    row_e, col_e = iota((LANES, LANES), 0), iota((LANES, LANES), 1)
    e_loc = LANES // n_dev
    before = jnp.logical_and(row_e < col_e, row_e // e_loc == col_e // e_loc).astype(F32).astype(BF16)
    count8 = jnp.broadcast_to(count, (8, LANES))
    base = jnp.dot(count8.astype(BF16), before, preferred_element_type=F32)[0:1]
    pos_s[...] = jnp.where(hit, base + rank, -1.0)
    t_id = iota((tok, LANES), 0).astype(F32)
    lane_f = lane.astype(F32)

    def pack(zd, _):
        for m in range(QUAD):
            tk = jnp.zeros((tok, LANES), F32)
            gt = jnp.zeros((tok, LANES), F32)
            for ee in range(e_loc):
                col = m * e_loc + ee
                at = pos_s[:, col:col + 1] == lane_f
                tk = jnp.where(at, t_id, tk)
                gt = jnp.where(at, p_s[:, col:col + 1], gt)
            packet[zd, m:m + 1, :] = jnp.sum(tk, axis=0, keepdims=True)
            packet[zd, QUAD + m:QUAD + m + 1, :] = jnp.sum(gt, axis=0, keepdims=True)
        packet[zd, 8:16, :] = count8
        pos_s[...] = pltpu.roll(pos_s[...], LANES - QUAD * e_loc, 1)
        p_s[...] = pltpu.roll(p_s[...], LANES - QUAD * e_loc, 1)
        return 0

    lax.fori_loop(0, PLANES, pack, 0)

    def route_copy(d):
        return remote(packet.at[d // QUAD], meta.at[me], send_m.at[d], recv_m.at[me], d)

    for d in range(n_dev):
        @pl.when(d != me)
        def _():
            route_copy(d).start()

    meta[me] = packet[z]

    def take(b, h, ways):
        hop(b, h, 3).wait_recv()
        out_copy(b, h).start()
        for way in ways:
            hop(b, h, way).start()

    def from_z(d, fn):
        @pl.when(z >= d)
        def _():
            fn(me - QUAD * d, 0, z < PLANES - 1)

        @pl.when(z + d < PLANES)
        def _():
            fn(me + QUAD * d, 1, z > 0)

    def across(zb):
        return zb * QUAD + (1 - y) * 2 + c

    def step_z(d):
        for h in range(2):
            def on(b, way, more):
                hop(b, h, 3).wait_recv()

                @pl.when(more)
                def _():
                    hop(b, h, way).start()

                hop(b, h, 2).start()
                hop(b, h, 3).start()
                out_copy(b, h).start()

            from_z(d, on)

    def step_y(d):
        for h in range(2):
            if d == 0:
                take(across(z), h, (3,))
            else:
                @pl.when(z >= d)
                def _():
                    take(across(z - d), h, (3,))

                @pl.when(z + d < PLANES)
                def _():
                    take(across(z + d), h, (3,))

    step_z(1)
    step_y(0)
    step_z(2)
    step_y(1)
    step_z(3)
    step_y(2)
    step_y(3)
    for b in range(n_dev):
        @pl.when(b % 2 != c)
        def _():
            for h in range(2):
                hop(b, h, 3).wait_recv()
                out_copy(b, h).start()

    for d in range(n_dev):
        @pl.when(d != me)
        def _():
            remote(packet.at[0], meta.at[d], send_m.at[d], recv_m.at[d], d).wait_recv()

    cnt = meta[:, 8, :]
    group = (iota((LANES, LANES), 0) // e_loc == iota((LANES, LANES), 1)).astype(F32).astype(BF16)
    n_rows = jnp.dot(cnt.astype(BF16), group, preferred_element_type=F32)
    ints[0:16, LANES:] = jnp.zeros((16, LANES), jnp.int32)
    ints[0:16, :LANES] = meta[:, pl.ds(q, 1), :].reshape(n_dev, LANES).astype(jnp.int32)
    ints[16:32, :LANES] = cnt.astype(jnp.int32)
    run = jnp.zeros((1, LANES), F32)
    for s in range(n_dev):
        off = run.astype(jnp.int32)
        ints[32 + s:33 + s, :LANES] = off
        ints[48 + s:49 + s, :LANES] = jnp.minimum(off // TILE, (r_max - WIN) // TILE)
        run = run + n_rows[s:s + 1]

    tail = [pltpu.make_async_copy(meta, meta_hbm, out_sem.at[0, 2]), pltpu.make_async_copy(ints, ints_hbm, out_sem.at[1, 2])]
    for cp in tail:
        cp.start()

    for h in range(2):
        def sent(b, way, more):
            @pl.when(more)
            def _():
                hop(b, h, way).wait_send()

            hop(b, h, 2).wait_send()
            hop(b, h, 3).wait_send()

        @pl.when(z < PLANES - 1)
        def _():
            hop(me, h, 0).wait_send()

        @pl.when(z > 0)
        def _():
            hop(me, h, 1).wait_send()

        hop(me, h, 2).wait_send()
        hop(me, h, 3).wait_send()
        for d in range(1, PLANES):
            from_z(d, sent)
        for zb in range(PLANES):
            hop(across(zb), h, 3).wait_send()
        for b in range(n_dev):
            out_copy(b, h).wait()
    for d in range(n_dev):
        @pl.when(d != me)
        def _():
            route_copy(d).wait_send()
    for cp in tail:
        cp.wait()


def spread(r_max, tokens, expert_ids, norm_gain, w_router):
    tok, width = tokens.shape
    n_dev = PLANES * QUAD
    sub = width // LANES
    hbm = pl.BlockSpec(memory_space=pltpu.HBM)
    vmem = pl.BlockSpec(memory_space=pltpu.VMEM)
    return pl.pallas_call(
        functools.partial(spread_kernel, r_max),
        out_shape=(jax.ShapeDtypeStruct((n_dev, tok * sub, LANES), BF16),
                   jax.ShapeDtypeStruct((n_dev, 16, LANES), F32),
                   jax.ShapeDtypeStruct((64, 2 * LANES), jnp.int32)),
        in_specs=[vmem] * 4,
        out_specs=(hbm, hbm, hbm),
        scratch_shapes=[
            pltpu.VMEM((n_dev, tok * sub, LANES), BF16),
            pltpu.VMEM((tok * sub, LANES), F32),
            pltpu.VMEM((tok, width), BF16),
            pltpu.VMEM((tok, LANES), F32),
            pltpu.VMEM((tok, LANES), F32),
            pltpu.VMEM((PLANES, 16, LANES), F32),
            pltpu.VMEM((n_dev, 16, LANES), F32),
            pltpu.VMEM((64, 2 * LANES), jnp.int32),
            pltpu.SemaphoreType.DMA((n_dev, 2, 4)),
            pltpu.SemaphoreType.DMA((n_dev, 2)),
            pltpu.SemaphoreType.DMA((n_dev,)),
            pltpu.SemaphoreType.DMA((n_dev,)),
            pltpu.SemaphoreType.DMA((n_dev, 3)),
        ],
        compiler_params=pltpu.CompilerParams(collective_id=0, has_side_effects=True, vmem_limit_bytes=66_000_000),
        name="spread",
    )(tokens, expert_ids, norm_gain.reshape(1, width), w_router)


def expert_kernel(n_src, sub, r_max, ints, meta, u_hbm, w1, w3, w2, o_hbm, win_hbm,
                  u_vm, o_all, xf, xb, hb, ob, win, pre, sems):
    e = pl.program_id(0)
    n_exp = pl.num_programs(0)
    me, z, q = place()
    lane0 = me * n_exp

    @pl.when(e == 0)
    def _():
        cp = pltpu.make_async_copy(u_hbm, u_vm, sems.at[0])
        cp.start()
        for s in range(n_src):
            pre[s] = 0

        @pl.loop(0, r_max * PITCH // 256)
        def _(i):
            o_all[pl.ds(pl.multiple_of(i * 256, 256), 256), :] = jnp.zeros((256, LANES), F32)

        @pl.loop(0, n_src)
        def _(s):
            for m in range(QUAD):
                t = meta[s, m:m + 1, :]
                g = meta[s, QUAD + m:QUAD + m + 1, :]
                hi = g.astype(BF16).astype(F32)
                mid = (g - hi).astype(BF16).astype(F32)
                lo = (g - hi - mid).astype(BF16).astype(F32)
                rows = jnp.concatenate([t, hi, mid, lo, t, t, t, t], axis=0)
                rows = jnp.concatenate([rows, jnp.zeros((8, WIN - LANES), F32)], axis=1)
                r = z * QUAD + m
                win[s * QUAD + m] = pltpu.roll(rows, ints[32 + s, r] - TILE * ints[48 + s, r], 1)

        pltpu.make_async_copy(win, win_hbm, sems.at[1]).start()
        cp.wait()

    def take(s, j0, n, i):
        t = s * LANES + ints[s, j0 + i]
        src = u_vm[pl.ds(pl.multiple_of(t * sub, sub), sub), :]
        xf[pl.ds((n + i) * PITCH, sub), :] = src.astype(F32)

    n = jnp.int32(0)
    top = jnp.int32(0)
    for s in range(n_src):
        cnt = ints[16 + s, lane0 + e]
        j0 = pre[s]
        for i in range(STEP):
            take(s, j0, n, i)
        n = n + cnt
        top = jnp.maximum(top, cnt)

    def rest(body):
        @pl.when(top > STEP)
        def _():
            def source(s, n):
                cnt = ints[16 + s, lane0 + e]

                def row(i, _):
                    body(s, pre[s], n, i)
                    return 0

                lax.fori_loop(STEP, cnt, row, 0)
                return n + cnt

            lax.fori_loop(0, n_src, source, jnp.int32(0))

    rest(take)

    def block(b, _):
        r0 = b * (BM * PITCH)
        for j in range(sub):
            xb[:, j * LANES:(j + 1) * LANES] = xf[pl.ds(r0 + j, BM, stride=PITCH), :].astype(BF16)
        g = jnp.dot(xb[...], w1[0], preferred_element_type=F32)
        v = jnp.dot(xb[...], w3[0], preferred_element_type=F32)
        hb[...] = (jax.nn.silu(g) * v).astype(BF16)
        for k in range(sub // 4):
            o = jnp.dot(hb[...], w2[0, :, k * 512:(k + 1) * 512], preferred_element_type=F32)
            for j in range(4):
                xf[pl.ds(r0 + k * 4 + j, BM, stride=PITCH), :] = o[:, j * LANES:(j + 1) * LANES]
        return 0

    lax.fori_loop(0, (n + BM - 1) // BM, block, 0)

    def give(s, slot, n, i):
        o_all[pl.ds(slot * PITCH, sub), :] = xf[pl.ds((n + i) * PITCH, sub), :]

    n = jnp.int32(0)
    for s in range(n_src):
        cnt = ints[16 + s, lane0 + e]
        slot = ints[32 + s, me] + pre[s]
        for i in range(STEP):
            give(s, jnp.where(i < cnt, slot + i, r_max), n, i)
        n = n + cnt
    rest(lambda s, j0, n, i: give(s, ints[32 + s, me] + j0 + i, n, i))
    for s in range(n_src):
        pre[s] = pre[s] + ints[16 + s, lane0 + e]

    @pl.when(e == n_exp - 1)
    def _():
        def put(j):
            return pltpu.make_async_copy(ob.at[j % 4], o_hbm.at[j], sems.at[2 + j % 4])

        for j in range(sub):
            if j >= 4:
                put(j - 4).wait()
            ob[j % 4] = o_all[pl.ds(j, r_max, stride=PITCH), :].astype(BF16)
            put(j).start()
        for j in range(sub - 4, sub):
            put(j).wait()
        pltpu.make_async_copy(win, win_hbm, sems.at[1]).wait()


def experts(n_src, r_max, ints, meta, u_rows, w1, w3, w2):
    n_exp, width, ff = w1.shape
    sub = width // LANES
    n_tok = u_rows.shape[0] // sub
    hbm = pl.BlockSpec(memory_space=pltpu.HBM)
    smem = pl.BlockSpec(memory_space=pltpu.SMEM)
    return pl.pallas_call(
        functools.partial(expert_kernel, n_src, sub, r_max),
        grid=(n_exp,),
        out_shape=(jax.ShapeDtypeStruct((sub, r_max, LANES), BF16),
                   jax.ShapeDtypeStruct((n_src * QUAD, 8, WIN), F32)),
        in_specs=[smem,
                  pl.BlockSpec((n_src, 16, LANES), lambda e: (0, 0, 0)),
                  hbm,
                  pl.BlockSpec((1, width, ff), lambda e: (e, 0, 0)),
                  pl.BlockSpec((1, width, ff), lambda e: (e, 0, 0)),
                  pl.BlockSpec((1, ff, width), lambda e: (e, 0, 0))],
        out_specs=(hbm, hbm),
        scratch_shapes=[
            pltpu.VMEM((n_tok * sub, LANES), BF16),
            pltpu.VMEM(((r_max + 8) * PITCH, LANES), F32),
            pltpu.VMEM(((r_max + 2 * STEP) * PITCH, LANES), F32),
            pltpu.VMEM((BM, width), BF16),
            pltpu.VMEM((BM, ff), BF16),
            pltpu.VMEM((4, r_max, LANES), BF16),
            pltpu.VMEM((n_src * QUAD, 8, WIN), F32),
            pltpu.SMEM((n_src,), jnp.int32),
            pltpu.SemaphoreType.DMA((6,)),
        ],
        compiler_params=pltpu.CompilerParams(vmem_limit_bytes=66_000_000, dimension_semantics=("arbitrary",)),
        name="experts",
    )(ints, meta, u_rows, w1, w3, w2)


def collect_kernel(n_src, steps, ints, win, x_ref, o_hbm, out_ref,
                   mix, part, from_l, from_r, fin,
                   send_q, recv_q, send_z, recv_l, recv_r, send_f, recv_f, *rows):
    me, z, q = place()
    y, c = q // 2, lax.rem(q, 2)
    tok = x_ref.shape[0]
    plane = QUAD * tok
    others = ((1 - y) * 2 + c, (1 - y) * 2 + 1 - c, y * 2 + 1 - c)

    barrier = pltpu.get_barrier_semaphore()

    def hello(dev):
        pl.semaphore_signal(barrier, inc=1, device_id={'ep': dev}, device_id_type=pl.DeviceIdType.MESH)

    for m in others:
        hello(z * QUAD + m)

    @pl.when(z > 0)
    def _():
        hello(me - QUAD)

    @pl.when(z < PLANES - 1)
    def _():
        hello(me + QUAD)

    pl.semaphore_wait(barrier, 4 + (z + PLANES - 1) // PLANES - (z + 1) // PLANES)

    def quad_copy(k, m):
        return remote(o_hbm.at[m * steps + k], rows[k].at[q], send_q.at[k, m], recv_q.at[k, q], z * QUAD + m)

    def quad_wait(k, m):
        remote(o_hbm.at[0], rows[k].at[m], send_q.at[k, m], recv_q.at[k, m], z * QUAD + m).wait_recv()

    def own_copy(k):
        return pltpu.make_async_copy(o_hbm.at[q * steps + k], rows[k].at[q], recv_q.at[k, q])

    for k in range(steps):
        for m in others:
            quad_copy(k, m).start()
        own_copy(k).start()

    row_id = iota((tok, WIN), 0).astype(F32)

    def build(i, _):
        w = win[i]
        at = w[0:1] == row_id
        for part_i in range(3):
            mix[i, part_i * tok:(part_i + 1) * tok, :] = jnp.where(at, w[1 + part_i:2 + part_i], 0.0).astype(BF16)
        return 0

    lax.fori_loop(0, n_src * QUAD, build, 0)

    def combine(k):
        own_copy(k).wait()
        for m in others:
            quad_wait(k, m)

        def token_block(s, _):
            acc = jnp.zeros((3 * tok, LANES), F32)
            for m in range(QUAD):
                start = ints[48 + s, z * QUAD + m]
                span = jnp.concatenate([rows[k][m, start + i] for i in range(WIN // TILE)], axis=0)
                acc += jnp.dot(mix[s * QUAD + m], span, preferred_element_type=F32)
            part[k, s // QUAD, pl.ds(pl.multiple_of(lax.rem(s, QUAD) * tok, tok), tok), :] = acc[0:tok] + acc[tok:2 * tok] + acc[2 * tok:]
            return 0

        lax.fori_loop(0, n_src, token_block, 0)

    def right(k, zd):
        return remote(part.at[k, zd], from_l.at[k, zd], send_z.at[k, zd], recv_l.at[k, zd], me + QUAD)

    def left(k, zd):
        return remote(part.at[k, zd], from_r.at[k, zd], send_z.at[k, zd], recv_r.at[k, zd], me - QUAD)

    def forward(k):
        for i in range(PLANES - 1):
            for to_right in (True, False):
                zd = PLANES - 1 - i if to_right else i
                box = from_l if to_right else from_r
                go = right if to_right else left

                @pl.when(z < zd if to_right else z > zd)
                def _():
                    @pl.when(z > 0 if to_right else z < PLANES - 1)
                    def _():
                        go(k, zd).wait_recv()
                        part[k, zd] += box[k, zd]

                    go(k, zd).start()

    def final_copy(k, m):
        src = part.at[k, z, pl.ds(m * tok, tok)]
        return remote(src, fin.at[k, q], send_f.at[k, m], recv_f.at[k, q], z * QUAD + m)

    def finish(k):
        @pl.when(z > 0)
        def _():
            right(k, z).wait_recv()
            part[k, z] += from_l[k, z]

        @pl.when(z < PLANES - 1)
        def _():
            left(k, z).wait_recv()
            part[k, z] += from_r[k, z]

        for m in others:
            final_copy(k, m).start()
        fin[k, q] = part[k, z, pl.ds(pl.multiple_of(q * tok, tok), tok), :]

    for k in range(steps):
        combine(k)
        forward(k)
        if k > 0:
            finish(k - 1)
    finish(steps - 1)

    for k in range(steps):
        for m in others:
            remote(part.at[k, z, pl.ds(0, tok)], fin.at[k, m], send_f.at[k, m], recv_f.at[k, m], z * QUAD + m).wait_recv()
        for m in range(QUAD):
            cols = pl.ds((m * steps + k) * LANES, LANES)
            out_ref[:, cols] = (x_ref[:, cols].astype(F32) + fin[k, m]).astype(BF16)

    for k in range(steps):
        for m in others:
            quad_copy(k, m).wait_send()
            final_copy(k, m).wait_send()
        for zd in range(PLANES):
            @pl.when(z < zd)
            def _():
                right(k, zd).wait_send()

            @pl.when(z > zd)
            def _():
                left(k, zd).wait_send()


def collect(ints, win, tokens, o_rows):
    tok, width = tokens.shape
    sub, r_tiles = o_rows.shape[:2]
    n_src = PLANES * QUAD
    steps = sub // QUAD
    vmem = pl.BlockSpec(memory_space=pltpu.VMEM)
    return pl.pallas_call(
        functools.partial(collect_kernel, n_src, steps),
        out_shape=jax.ShapeDtypeStruct((tok, width), BF16),
        in_specs=[pl.BlockSpec(memory_space=pltpu.SMEM), vmem, vmem, pl.BlockSpec(memory_space=pltpu.HBM)],
        out_specs=vmem,
        scratch_shapes=[
            pltpu.VMEM((n_src * QUAD, 3 * tok, WIN), BF16),
            pltpu.VMEM((steps, PLANES, QUAD * tok, LANES), F32),
            pltpu.VMEM((steps, PLANES, QUAD * tok, LANES), F32),
            pltpu.VMEM((steps, PLANES, QUAD * tok, LANES), F32),
            pltpu.VMEM((steps, QUAD, tok, LANES), F32),
            pltpu.SemaphoreType.DMA((steps, QUAD)),
            pltpu.SemaphoreType.DMA((steps, QUAD)),
            pltpu.SemaphoreType.DMA((steps, PLANES)),
            pltpu.SemaphoreType.DMA((steps, PLANES)),
            pltpu.SemaphoreType.DMA((steps, PLANES)),
            pltpu.SemaphoreType.DMA((steps, QUAD)),
            pltpu.SemaphoreType.DMA((steps, QUAD)),
        ] + [pltpu.VMEM((QUAD, r_tiles, TILE, LANES), BF16)] * steps,
        compiler_params=pltpu.CompilerParams(collective_id=1, has_side_effects=True, vmem_limit_bytes=56 * 2 ** 20),
        name="collect",
    )(ints, win, tokens, o_rows)


def solution(mesh):
    ep_size = mesh.shape['ep']

    def device_step(tokens, expert_ids, norm_gain, w_router, w_gate, w_up, w_down):
        pairs = expert_ids.shape[0] * expert_ids.shape[1]
        r_max = 3 * pairs // 2
        u_rows, meta, ints = spread(r_max, tokens, expert_ids, norm_gain, w_router)
        u_rows = u_rows.reshape(-1, LANES)
        o_rows, win = experts(ep_size, r_max, ints, meta, u_rows, w_gate, w_up, w_down)
        return collect(ints, win, tokens, o_rows.reshape(-1, r_max // TILE, TILE, LANES))

    row_spec = P(('dp', 'ep'), None)
    expert_spec = P('ep', None, None)
    return jax.shard_map(device_step, mesh=mesh, in_specs=(row_spec, row_spec, P(None), P(None, None), expert_spec, expert_spec, expert_spec), out_specs=row_spec, check_vma=False)
```

```python
import functools

import jax
import jax.numpy as jnp
from jax import lax
from jax.experimental import pallas as pl
from jax.experimental.pallas import tpu as pltpu
from jax.sharding import PartitionSpec as P

NORM_EPS = 1e-5
LANES = 128
BM = 128
WIN = 256
TILE = 16
PITCH = 17
STEP = 8
PIECES = 4
QUAD = 4
PLANES = 4
F32 = jnp.float32
BF16 = jnp.bfloat16


def iota(shape, dim):
    return lax.broadcasted_iota(jnp.int32, shape, dim)


def place():
    me = lax.axis_index('ep')
    return me, me // QUAD, lax.rem(me, QUAD)


def remote(src, dst, send, recv, dev):
    return pltpu.make_async_remote_copy(src_ref=src, dst_ref=dst, send_sem=send, recv_sem=recv,
                                        device_id={'ep': dev}, device_id_type=pl.DeviceIdType.MESH)


def spread_kernel(r_max, x_ref, ids_ref, gain_ref, wr_ref, u_hbm, meta_hbm, ints_hbm,
                  u_all, xs, ub, pos_s, p_s, packet, meta, ints,
                  send_u, recv_u, send_m, recv_m, out_sem):
    n_dev = PLANES * QUAD
    me, z, q = place()
    y, c = q // 2, lax.rem(q, 2)
    half = u_all.shape[1] // 2
    tok = x_ref.shape[0]
    sub = u_all.shape[1] // tok

    barrier = pltpu.get_barrier_semaphore()
    for d in range(1, n_dev):
        pl.semaphore_signal(barrier, inc=1, device_id={'ep': lax.rem(me + d, n_dev)}, device_id_type=pl.DeviceIdType.MESH)

    x32 = x_ref[...].astype(F32)
    inv = lax.rsqrt(jnp.mean(x32 * x32, axis=1, keepdims=True) + NORM_EPS)
    ub[...] = (x32 * inv * gain_ref[...].astype(F32)).astype(BF16)
    for j in range(sub):
        xs[pl.ds(j, tok, stride=sub), :] = ub[:, j * LANES:(j + 1) * LANES].astype(F32)
    u_all[me] = xs[...].astype(BF16)
    pl.semaphore_wait(barrier, n_dev - 1)

    dest = (me + QUAD, me - QUAD, z * QUAD + (1 - y) * 2 + c, z * QUAD + y * 2 + 1 - c)

    def hop(b, h, way):
        rows = u_all.at[b, pl.ds(h * half, half)]
        return remote(rows, rows, send_u.at[b, h, way], recv_u.at[b, h], dest[way])

    def out_copy(b, h):
        rows = pl.ds(h * half, half)
        return pltpu.make_async_copy(u_all.at[b, rows], u_hbm.at[b, rows], out_sem.at[b, h])

    for h in range(2):
        @pl.when(z < PLANES - 1)
        def _():
            hop(me, h, 0).start()

        @pl.when(z > 0)
        def _():
            hop(me, h, 1).start()

        hop(me, h, 2).start()
        hop(me, h, 3).start()
        out_copy(me, h).start()

    logits = jnp.dot(ub[...], wr_ref[...], preferred_element_type=F32)
    top = jnp.max(logits, axis=1, keepdims=True)
    ex = jnp.exp(logits - top)
    p_s[...] = ex / jnp.sum(ex, axis=1, keepdims=True)
    lane = iota((tok, LANES), 1)
    hit = lane < 0
    for k in range(ids_ref.shape[1]):
        hit = jnp.logical_or(hit, ids_ref[:, k:k + 1] == lane)
    hit32 = hit.astype(F32)
    hit_b = hit32.astype(BF16)
    tri = (iota((tok, tok), 0) > iota((tok, tok), 1)).astype(F32).astype(BF16)
    rank = jnp.dot(tri, hit_b, preferred_element_type=F32)
    count = jnp.sum(hit32, axis=0, keepdims=True)
    row_e, col_e = iota((LANES, LANES), 0), iota((LANES, LANES), 1)
    e_loc = LANES // n_dev
    before = jnp.logical_and(row_e < col_e, row_e // e_loc == col_e // e_loc).astype(F32).astype(BF16)
    count8 = jnp.broadcast_to(count, (8, LANES))
    base = jnp.dot(count8.astype(BF16), before, preferred_element_type=F32)[0:1]
    pos_s[...] = jnp.where(hit, base + rank, -1.0)
    t_id = iota((tok, LANES), 0).astype(F32)
    lane_f = lane.astype(F32)

    def pack(zd, _):
        for m in range(QUAD):
            tk = jnp.zeros((tok, LANES), F32)
            gt = jnp.zeros((tok, LANES), F32)
            for ee in range(e_loc):
                col = m * e_loc + ee
                at = pos_s[:, col:col + 1] == lane_f
                tk = jnp.where(at, t_id, tk)
                gt = jnp.where(at, p_s[:, col:col + 1], gt)
            packet[zd, m:m + 1, :] = jnp.sum(tk, axis=0, keepdims=True)
            packet[zd, QUAD + m:QUAD + m + 1, :] = jnp.sum(gt, axis=0, keepdims=True)
        packet[zd, 8:16, :] = count8
        pos_s[...] = pltpu.roll(pos_s[...], LANES - QUAD * e_loc, 1)
        p_s[...] = pltpu.roll(p_s[...], LANES - QUAD * e_loc, 1)
        return 0

    lax.fori_loop(0, PLANES, pack, 0)

    def route_copy(d):
        return remote(packet.at[d // QUAD], meta.at[me], send_m.at[d], recv_m.at[me], d)

    for d in range(n_dev):
        @pl.when(d != me)
        def _():
            route_copy(d).start()

    meta[me] = packet[z]

    def take(b, h, ways):
        hop(b, h, 3).wait_recv()
        out_copy(b, h).start()
        for way in ways:
            hop(b, h, way).start()

    def from_z(d, fn):
        @pl.when(z >= d)
        def _():
            fn(me - QUAD * d, 0, z < PLANES - 1)

        @pl.when(z + d < PLANES)
        def _():
            fn(me + QUAD * d, 1, z > 0)

    def across(zb):
        return zb * QUAD + (1 - y) * 2 + c

    def step_z(d):
        for h in range(2):
            def on(b, way, more):
                hop(b, h, 3).wait_recv()

                @pl.when(more)
                def _():
                    hop(b, h, way).start()

                hop(b, h, 2).start()
                hop(b, h, 3).start()
                out_copy(b, h).start()

            from_z(d, on)

    def step_y(d):
        for h in range(2):
            if d == 0:
                take(across(z), h, (3,))
            else:
                @pl.when(z >= d)
                def _():
                    take(across(z - d), h, (3,))

                @pl.when(z + d < PLANES)
                def _():
                    take(across(z + d), h, (3,))

    step_z(1)
    step_y(0)
    step_z(2)
    step_y(1)
    step_z(3)
    step_y(2)
    step_y(3)
    for b in range(n_dev):
        @pl.when(b % 2 != c)
        def _():
            for h in range(2):
                hop(b, h, 3).wait_recv()
                out_copy(b, h).start()

    for d in range(n_dev):
        @pl.when(d != me)
        def _():
            remote(packet.at[0], meta.at[d], send_m.at[d], recv_m.at[d], d).wait_recv()

    cnt = meta[:, 8, :]
    group = (iota((LANES, LANES), 0) // e_loc == iota((LANES, LANES), 1)).astype(F32).astype(BF16)
    n_rows = jnp.dot(cnt.astype(BF16), group, preferred_element_type=F32)
    ints[0:16, LANES:] = jnp.zeros((16, LANES), jnp.int32)
    ints[0:16, :LANES] = meta[:, pl.ds(q, 1), :].reshape(n_dev, LANES).astype(jnp.int32)
    ints[16:32, :LANES] = cnt.astype(jnp.int32)
    run = jnp.zeros((1, LANES), F32)
    for s in range(n_dev):
        off = run.astype(jnp.int32)
        ints[32 + s:33 + s, :LANES] = off
        ints[48 + s:49 + s, :LANES] = jnp.minimum(off // TILE, (r_max - WIN) // TILE)
        run = run + n_rows[s:s + 1]

    tail = [pltpu.make_async_copy(meta, meta_hbm, out_sem.at[0, 2]), pltpu.make_async_copy(ints, ints_hbm, out_sem.at[1, 2])]
    for cp in tail:
        cp.start()

    for h in range(2):
        def sent(b, way, more):
            @pl.when(more)
            def _():
                hop(b, h, way).wait_send()

            hop(b, h, 2).wait_send()
            hop(b, h, 3).wait_send()

        @pl.when(z < PLANES - 1)
        def _():
            hop(me, h, 0).wait_send()

        @pl.when(z > 0)
        def _():
            hop(me, h, 1).wait_send()

        hop(me, h, 2).wait_send()
        hop(me, h, 3).wait_send()
        for d in range(1, PLANES):
            from_z(d, sent)
        for zb in range(PLANES):
            hop(across(zb), h, 3).wait_send()
        for b in range(n_dev):
            out_copy(b, h).wait()
    for d in range(n_dev):
        @pl.when(d != me)
        def _():
            route_copy(d).wait_send()
    for cp in tail:
        cp.wait()


def spread(r_max, tokens, expert_ids, norm_gain, w_router):
    tok, width = tokens.shape
    n_dev = PLANES * QUAD
    sub = width // LANES
    hbm = pl.BlockSpec(memory_space=pltpu.HBM)
    vmem = pl.BlockSpec(memory_space=pltpu.VMEM)
    return pl.pallas_call(
        functools.partial(spread_kernel, r_max),
        out_shape=(jax.ShapeDtypeStruct((n_dev, tok * sub, LANES), BF16),
                   jax.ShapeDtypeStruct((n_dev, 16, LANES), F32),
                   jax.ShapeDtypeStruct((64, 2 * LANES), jnp.int32)),
        in_specs=[vmem] * 4,
        out_specs=(hbm, hbm, hbm),
        scratch_shapes=[
            pltpu.VMEM((n_dev, tok * sub, LANES), BF16),
            pltpu.VMEM((tok * sub, LANES), F32),
            pltpu.VMEM((tok, width), BF16),
            pltpu.VMEM((tok, LANES), F32),
            pltpu.VMEM((tok, LANES), F32),
            pltpu.VMEM((PLANES, 16, LANES), F32),
            pltpu.VMEM((n_dev, 16, LANES), F32),
            pltpu.VMEM((64, 2 * LANES), jnp.int32),
            pltpu.SemaphoreType.DMA((n_dev, 2, 4)),
            pltpu.SemaphoreType.DMA((n_dev, 2)),
            pltpu.SemaphoreType.DMA((n_dev,)),
            pltpu.SemaphoreType.DMA((n_dev,)),
            pltpu.SemaphoreType.DMA((n_dev, 3)),
        ],
        compiler_params=pltpu.CompilerParams(collective_id=0, has_side_effects=True, vmem_limit_bytes=66_000_000),
        name="spread",
    )(tokens, expert_ids, norm_gain.reshape(1, width), w_router)


def expert_kernel(n_src, sub, r_max, ints, meta, u_hbm, w1_hbm, w3_hbm, w2_hbm, o_hbm, win_hbm,
                  u_vm, o_all, xf, xb, hb, ob, win, w1, w3, w2, pre, sems, sem_w):
    n_exp = w1_hbm.shape[0]
    me, z, q = place()
    lane0 = me * n_exp

    def load(e, names):
        slot = lax.rem(e, 2)
        copies = []
        for i, (src, dst) in enumerate(((w1_hbm, w1), (w3_hbm, w3), (w2_hbm, w2))):
            if i in names:
                size = src.shape[1] // PIECES
                for p in range(PIECES):
                    part = pl.ds(p * size, size)
                    copies.append(pltpu.make_async_copy(src.at[e, part], dst.at[slot, part], sem_w.at[slot, i, p]))
        return copies

    def begin():
        cp = pltpu.make_async_copy(u_hbm, u_vm, sems.at[0])
        cp.start()
        for e in range(2):
            for w in load(e, (0, 1, 2)):
                w.start()
        for s in range(n_src):
            pre[s] = 0

        @pl.loop(0, r_max * PITCH // 256)
        def _(i):
            o_all[pl.ds(pl.multiple_of(i * 256, 256), 256), :] = jnp.zeros((256, LANES), F32)

        @pl.loop(0, n_src)
        def _(s):
            for m in range(QUAD):
                t = meta[s, m:m + 1, :]
                g = meta[s, QUAD + m:QUAD + m + 1, :]
                hi = g.astype(BF16).astype(F32)
                mid = (g - hi).astype(BF16).astype(F32)
                lo = (g - hi - mid).astype(BF16).astype(F32)
                rows = jnp.concatenate([t, hi, mid, lo, t, t, t, t], axis=0)
                rows = jnp.concatenate([rows, jnp.zeros((8, WIN - LANES), F32)], axis=1)
                r = z * QUAD + m
                win[s * QUAD + m] = pltpu.roll(rows, ints[32 + s, r] - TILE * ints[48 + s, r], 1)

        pltpu.make_async_copy(win, win_hbm, sems.at[1]).start()
        cp.wait()

    begin()

    def expert(e, _):
        slot = lax.rem(e, 2)
        def take(s, j0, n, i):
            t = s * LANES + ints[s, j0 + i]
            src = u_vm[pl.ds(pl.multiple_of(t * sub, sub), sub), :]
            xf[pl.ds((n + i) * PITCH, sub), :] = src.astype(F32)

        n = jnp.int32(0)
        top = jnp.int32(0)
        for s in range(n_src):
            cnt = ints[16 + s, lane0 + e]
            j0 = pre[s]
            for i in range(STEP):
                take(s, j0, n, i)
            n = n + cnt
            top = jnp.maximum(top, cnt)

        def rest(body):
            @pl.when(top > STEP)
            def _():
                def source(s, n):
                    cnt = ints[16 + s, lane0 + e]

                    def row(i, _):
                        body(s, pre[s], n, i)
                        return 0

                    lax.fori_loop(STEP, cnt, row, 0)
                    return n + cnt

                lax.fori_loop(0, n_src, source, jnp.int32(0))

        rest(take)

        for w in load(e, (0, 1, 2)):
            w.wait()

        def block(b, _):
            r0 = b * (BM * PITCH)
            for j in range(sub):
                xb[:, j * LANES:(j + 1) * LANES] = xf[pl.ds(r0 + j, BM, stride=PITCH), :].astype(BF16)
            g = jnp.dot(xb[...], w1[slot], preferred_element_type=F32)
            v = jnp.dot(xb[...], w3[slot], preferred_element_type=F32)
            hb[...] = (jax.nn.silu(g) * v).astype(BF16)
            for k in range(sub // 4):
                o = jnp.dot(hb[...], w2[slot, :, k * 512:(k + 1) * 512], preferred_element_type=F32)
                for j in range(4):
                    xf[pl.ds(r0 + k * 4 + j, BM, stride=PITCH), :] = o[:, j * LANES:(j + 1) * LANES]
            return 0

        lax.fori_loop(0, (n + BM - 1) // BM, block, 0)

        def give(s, slot, n, i):
            o_all[pl.ds(slot * PITCH, sub), :] = xf[pl.ds((n + i) * PITCH, sub), :]

        n = jnp.int32(0)
        for s in range(n_src):
            cnt = ints[16 + s, lane0 + e]
            slot = ints[32 + s, me] + pre[s]
            for i in range(STEP):
                give(s, jnp.where(i < cnt, slot + i, r_max), n, i)
            n = n + cnt
        rest(lambda s, j0, n, i: give(s, ints[32 + s, me] + j0 + i, n, i))
        for s in range(n_src):
            pre[s] = pre[s] + ints[16 + s, lane0 + e]

        @pl.when(e + 2 < n_exp)
        def _():
            for w in load(e + 2, (0, 1, 2)):
                w.start()

        return 0

    lax.fori_loop(0, n_exp, expert, 0)

    def put(j):
        return pltpu.make_async_copy(ob.at[j % 4], o_hbm.at[j], sems.at[2 + j % 4])

    for j in range(sub):
        if j >= 4:
            put(j - 4).wait()
        ob[j % 4] = o_all[pl.ds(j, r_max, stride=PITCH), :].astype(BF16)
        put(j).start()
    for j in range(sub - 4, sub):
        put(j).wait()
    pltpu.make_async_copy(win, win_hbm, sems.at[1]).wait()


def experts(n_src, r_max, ints, meta, u_rows, w1, w3, w2):
    n_exp, width, ff = w1.shape
    sub = width // LANES
    n_tok = u_rows.shape[0] // sub
    hbm = pl.BlockSpec(memory_space=pltpu.HBM)
    smem = pl.BlockSpec(memory_space=pltpu.SMEM)
    return pl.pallas_call(
        functools.partial(expert_kernel, n_src, sub, r_max),
        out_shape=(jax.ShapeDtypeStruct((sub, r_max, LANES), BF16),
                   jax.ShapeDtypeStruct((n_src * QUAD, 8, WIN), F32)),
        in_specs=[smem, pl.BlockSpec(memory_space=pltpu.VMEM), hbm, hbm, hbm, hbm],
        out_specs=(hbm, hbm),
        scratch_shapes=[
            pltpu.VMEM((n_tok * sub, LANES), BF16),
            pltpu.VMEM(((r_max + 8) * PITCH, LANES), F32),
            pltpu.VMEM(((r_max + 2 * STEP) * PITCH, LANES), F32),
            pltpu.VMEM((BM, width), BF16),
            pltpu.VMEM((BM, ff), BF16),
            pltpu.VMEM((4, r_max, LANES), BF16),
            pltpu.VMEM((n_src * QUAD, 8, WIN), F32),
            pltpu.VMEM((2, width, ff), BF16),
            pltpu.VMEM((2, width, ff), BF16),
            pltpu.VMEM((2, ff, width), BF16),
            pltpu.SMEM((n_src,), jnp.int32),
            pltpu.SemaphoreType.DMA((6,)),
            pltpu.SemaphoreType.DMA((2, 3, PIECES)),
        ],
        compiler_params=pltpu.CompilerParams(vmem_limit_bytes=66_000_000),
        name="experts",
    )(ints, meta, u_rows, w1, w3, w2)


def collect_kernel(n_src, steps, ints, win, x_ref, o_hbm, out_ref,
                   mix, part, from_l, from_r, fin,
                   send_q, recv_q, send_z, recv_l, recv_r, send_f, recv_f, *rows):
    me, z, q = place()
    y, c = q // 2, lax.rem(q, 2)
    tok = x_ref.shape[0]
    plane = QUAD * tok
    others = ((1 - y) * 2 + c, (1 - y) * 2 + 1 - c, y * 2 + 1 - c)

    barrier = pltpu.get_barrier_semaphore()

    def hello(dev):
        pl.semaphore_signal(barrier, inc=1, device_id={'ep': dev}, device_id_type=pl.DeviceIdType.MESH)

    for m in others:
        hello(z * QUAD + m)

    @pl.when(z > 0)
    def _():
        hello(me - QUAD)

    @pl.when(z < PLANES - 1)
    def _():
        hello(me + QUAD)

    pl.semaphore_wait(barrier, 4 + (z + PLANES - 1) // PLANES - (z + 1) // PLANES)

    def quad_copy(k, m):
        return remote(o_hbm.at[m * steps + k], rows[k].at[q], send_q.at[k, m], recv_q.at[k, q], z * QUAD + m)

    def quad_wait(k, m):
        remote(o_hbm.at[0], rows[k].at[m], send_q.at[k, m], recv_q.at[k, m], z * QUAD + m).wait_recv()

    def own_copy(k):
        return pltpu.make_async_copy(o_hbm.at[q * steps + k], rows[k].at[q], recv_q.at[k, q])

    for k in range(steps):
        for m in others:
            quad_copy(k, m).start()
        own_copy(k).start()

    row_id = iota((tok, WIN), 0).astype(F32)

    def build(i, _):
        w = win[i]
        at = w[0:1] == row_id
        for part_i in range(3):
            mix[i, part_i * tok:(part_i + 1) * tok, :] = jnp.where(at, w[1 + part_i:2 + part_i], 0.0).astype(BF16)
        return 0

    lax.fori_loop(0, n_src * QUAD, build, 0)

    def combine(k):
        own_copy(k).wait()
        for m in others:
            quad_wait(k, m)

        def token_block(s):
            acc = jnp.zeros((3 * tok, LANES), F32)
            for m in range(QUAD):
                start = ints[48 + s, z * QUAD + m]
                span = jnp.concatenate([rows[k][m, start + i] for i in range(WIN // TILE)], axis=0)
                acc += jnp.dot(mix[s * QUAD + m], span, preferred_element_type=F32)
            part[k, s // QUAD, pl.ds(pl.multiple_of(lax.rem(s, QUAD) * tok, tok), tok), :] = acc[0:tok] + acc[tok:2 * tok] + acc[2 * tok:]

        def token_blocks(i, _):
            token_block(2 * i)
            token_block(2 * i + 1)
            return 0

        lax.fori_loop(0, n_src // 2, token_blocks, 0)

    def right(k, zd):
        return remote(part.at[k, zd], from_l.at[k, zd], send_z.at[k, zd], recv_l.at[k, zd], me + QUAD)

    def left(k, zd):
        return remote(part.at[k, zd], from_r.at[k, zd], send_z.at[k, zd], recv_r.at[k, zd], me - QUAD)

    def forward(k):
        for i in range(PLANES - 1):
            for to_right in (True, False):
                zd = PLANES - 1 - i if to_right else i
                box = from_l if to_right else from_r
                go = right if to_right else left

                @pl.when(z < zd if to_right else z > zd)
                def _():
                    @pl.when(z > 0 if to_right else z < PLANES - 1)
                    def _():
                        go(k, zd).wait_recv()
                        part[k, zd] += box[k, zd]

                    go(k, zd).start()

    def final_copy(k, m):
        src = part.at[k, z, pl.ds(m * tok, tok)]
        return remote(src, fin.at[k, q], send_f.at[k, m], recv_f.at[k, q], z * QUAD + m)

    def finish(k):
        @pl.when(z > 0)
        def _():
            right(k, z).wait_recv()
            part[k, z] += from_l[k, z]

        @pl.when(z < PLANES - 1)
        def _():
            left(k, z).wait_recv()
            part[k, z] += from_r[k, z]

        for m in others:
            final_copy(k, m).start()
        fin[k, q] = part[k, z, pl.ds(pl.multiple_of(q * tok, tok), tok), :]

    for k in range(steps):
        combine(k)
        forward(k)
        if k > 0:
            finish(k - 1)
    finish(steps - 1)

    for k in range(steps):
        for m in others:
            remote(part.at[k, z, pl.ds(0, tok)], fin.at[k, m], send_f.at[k, m], recv_f.at[k, m], z * QUAD + m).wait_recv()
        for m in range(QUAD):
            cols = pl.ds((m * steps + k) * LANES, LANES)
            out_ref[:, cols] = (x_ref[:, cols].astype(F32) + fin[k, m]).astype(BF16)

    for k in range(steps):
        for m in others:
            quad_copy(k, m).wait_send()
            final_copy(k, m).wait_send()
        for zd in range(PLANES):
            @pl.when(z < zd)
            def _():
                right(k, zd).wait_send()

            @pl.when(z > zd)
            def _():
                left(k, zd).wait_send()


def collect(ints, win, tokens, o_rows):
    tok, width = tokens.shape
    sub, r_tiles = o_rows.shape[:2]
    n_src = PLANES * QUAD
    steps = sub // QUAD
    vmem = pl.BlockSpec(memory_space=pltpu.VMEM)
    return pl.pallas_call(
        functools.partial(collect_kernel, n_src, steps),
        out_shape=jax.ShapeDtypeStruct((tok, width), BF16),
        in_specs=[pl.BlockSpec(memory_space=pltpu.SMEM), vmem, vmem, pl.BlockSpec(memory_space=pltpu.HBM)],
        out_specs=vmem,
        scratch_shapes=[
            pltpu.VMEM((n_src * QUAD, 3 * tok, WIN), BF16),
            pltpu.VMEM((steps, PLANES, QUAD * tok, LANES), F32),
            pltpu.VMEM((steps, PLANES, QUAD * tok, LANES), F32),
            pltpu.VMEM((steps, PLANES, QUAD * tok, LANES), F32),
            pltpu.VMEM((steps, QUAD, tok, LANES), F32),
            pltpu.SemaphoreType.DMA((steps, QUAD)),
            pltpu.SemaphoreType.DMA((steps, QUAD)),
            pltpu.SemaphoreType.DMA((steps, PLANES)),
            pltpu.SemaphoreType.DMA((steps, PLANES)),
            pltpu.SemaphoreType.DMA((steps, PLANES)),
            pltpu.SemaphoreType.DMA((steps, QUAD)),
            pltpu.SemaphoreType.DMA((steps, QUAD)),
        ] + [pltpu.VMEM((QUAD, r_tiles, TILE, LANES), BF16)] * steps,
        compiler_params=pltpu.CompilerParams(collective_id=1, has_side_effects=True, vmem_limit_bytes=56 * 2 ** 20),
        name="collect",
    )(ints, win, tokens, o_rows)


def solution(mesh):
    ep_size = mesh.shape['ep']

    def device_step(tokens, expert_ids, norm_gain, w_router, w_gate, w_up, w_down):
        pairs = expert_ids.shape[0] * expert_ids.shape[1]
        r_max = 3 * pairs // 2
        u_rows, meta, ints = spread(r_max, tokens, expert_ids, norm_gain, w_router)
        u_rows = u_rows.reshape(-1, LANES)
        o_rows, win = experts(ep_size, r_max, ints, meta, u_rows, w_gate, w_up, w_down)
        return collect(ints, win, tokens, o_rows.reshape(-1, r_max // TILE, TILE, LANES))

    row_spec = P(('dp', 'ep'), None)
    expert_spec = P('ep', None, None)
    return jax.shard_map(device_step, mesh=mesh, in_specs=(row_spec, row_spec, P(None), P(None, None), expert_spec, expert_spec, expert_spec), out_specs=row_spec, check_vma=False)
```

```python
import functools

import jax
import jax.numpy as jnp
from jax import lax
from jax.experimental import pallas as pl
from jax.experimental.pallas import tpu as pltpu
from jax.sharding import PartitionSpec as P

NORM_EPS = 1e-5
LANES = 128
BM = 128
WIN = 256
CUTS = 2
TILE = 16
PITCH = 17
STEP = 8
MORE = 8
PIECES = 4
QUAD = 4
PLANES = 4
F32 = jnp.float32
BF16 = jnp.bfloat16


def iota(shape, dim):
    return lax.broadcasted_iota(jnp.int32, shape, dim)


def place():
    me = lax.axis_index('ep')
    return me, me // QUAD, lax.rem(me, QUAD)


def remote(src, dst, send, recv, dev):
    return pltpu.make_async_remote_copy(src_ref=src, dst_ref=dst, send_sem=send, recv_sem=recv,
                                        device_id={'ep': dev}, device_id_type=pl.DeviceIdType.MESH)


def spread_kernel(r_max, x_ref, ids_ref, gain_ref, wr_ref, u_hbm, meta_hbm, ints_hbm,
                  u_all, xs, ub, pos_s, p_s, packet, meta, ints,
                  send_u, recv_u, send_m, recv_m, out_sem):
    n_dev = PLANES * QUAD
    me, z, q = place()
    y, c = q // 2, lax.rem(q, 2)
    half = u_all.shape[1] // 2
    tok = x_ref.shape[0]
    sub = u_all.shape[1] // tok

    barrier = pltpu.get_barrier_semaphore()
    for d in range(1, n_dev):
        pl.semaphore_signal(barrier, inc=1, device_id={'ep': lax.rem(me + d, n_dev)}, device_id_type=pl.DeviceIdType.MESH)

    x32 = x_ref[...].astype(F32)
    inv = lax.rsqrt(jnp.mean(x32 * x32, axis=1, keepdims=True) + NORM_EPS)
    ub[...] = (x32 * inv * gain_ref[...].astype(F32)).astype(BF16)
    for j in range(sub):
        xs[pl.ds(j, tok, stride=sub), :] = ub[:, j * LANES:(j + 1) * LANES].astype(F32)
    u_all[me] = xs[...].astype(BF16)
    pl.semaphore_wait(barrier, n_dev - 1)

    dest = (me + QUAD, me - QUAD, z * QUAD + (1 - y) * 2 + c, z * QUAD + y * 2 + 1 - c)

    def hop(b, h, way):
        rows = u_all.at[b, pl.ds(h * half, half)]
        return remote(rows, rows, send_u.at[b, h, way], recv_u.at[b, h], dest[way])

    def out_copy(b, h):
        rows = pl.ds(h * half, half)
        return pltpu.make_async_copy(u_all.at[b, rows], u_hbm.at[b, rows], out_sem.at[b, h])

    for h in range(2):
        @pl.when(z < PLANES - 1)
        def _():
            hop(me, h, 0).start()

        @pl.when(z > 0)
        def _():
            hop(me, h, 1).start()

        hop(me, h, 2).start()
        hop(me, h, 3).start()
        out_copy(me, h).start()

    logits = jnp.dot(ub[...], wr_ref[...], preferred_element_type=F32)
    top = jnp.max(logits, axis=1, keepdims=True)
    ex = jnp.exp(logits - top)
    p_s[...] = ex / jnp.sum(ex, axis=1, keepdims=True)
    lane = iota((tok, LANES), 1)
    hit = lane < 0
    ids = ids_ref[...].T
    for k in range(ids.shape[1]):
        hit = jnp.logical_or(hit, ids[:, k:k + 1] == lane)
    hit32 = hit.astype(F32)
    hit_b = hit32.astype(BF16)
    tri = (iota((tok, tok), 0) > iota((tok, tok), 1)).astype(F32).astype(BF16)
    rank = jnp.dot(tri, hit_b, preferred_element_type=F32)
    count = jnp.sum(hit32, axis=0, keepdims=True)
    row_e, col_e = iota((LANES, LANES), 0), iota((LANES, LANES), 1)
    e_loc = LANES // n_dev
    before = jnp.logical_and(row_e < col_e, row_e // e_loc == col_e // e_loc).astype(F32).astype(BF16)
    count8 = jnp.broadcast_to(count, (8, LANES))
    base = jnp.dot(count8.astype(BF16), before, preferred_element_type=F32)[0:1]
    pos_s[...] = jnp.where(hit, base + rank, -1.0)
    t_id = iota((tok, LANES), 0).astype(F32)
    lane_f = lane.astype(F32)

    def pack(zd, _):
        for m in range(QUAD):
            tk = jnp.zeros((tok, LANES), F32)
            gt = jnp.zeros((tok, LANES), F32)
            for ee in range(e_loc):
                col = m * e_loc + ee
                at = pos_s[:, col:col + 1] == lane_f
                tk = jnp.where(at, t_id, tk)
                gt = jnp.where(at, p_s[:, col:col + 1], gt)
            packet[zd, m:m + 1, :] = jnp.sum(tk, axis=0, keepdims=True)
            packet[zd, QUAD + m:QUAD + m + 1, :] = jnp.sum(gt, axis=0, keepdims=True)
        packet[zd, 8:16, :] = count8
        pos_s[...] = pltpu.roll(pos_s[...], LANES - QUAD * e_loc, 1)
        p_s[...] = pltpu.roll(p_s[...], LANES - QUAD * e_loc, 1)
        return 0

    lax.fori_loop(0, PLANES, pack, 0)

    def route_copy(d):
        return remote(packet.at[d // QUAD], meta.at[me], send_m.at[d], recv_m.at[me], d)

    for d in range(n_dev):
        @pl.when(d != me)
        def _():
            route_copy(d).start()

    meta[me] = packet[z]

    def take(b, h, ways):
        hop(b, h, 3).wait_recv()
        out_copy(b, h).start()
        for way in ways:
            hop(b, h, way).start()

    def from_z(d, fn):
        @pl.when(z >= d)
        def _():
            fn(me - QUAD * d, 0, z < PLANES - 1)

        @pl.when(z + d < PLANES)
        def _():
            fn(me + QUAD * d, 1, z > 0)

    def across(zb):
        return zb * QUAD + (1 - y) * 2 + c

    def step_z(d):
        for h in range(2):
            def on(b, way, more):
                hop(b, h, 3).wait_recv()

                @pl.when(more)
                def _():
                    hop(b, h, way).start()

                hop(b, h, 2).start()
                hop(b, h, 3).start()
                out_copy(b, h).start()

            from_z(d, on)

    def step_y(d):
        for h in range(2):
            if d == 0:
                take(across(z), h, (3,))
            else:
                @pl.when(z >= d)
                def _():
                    take(across(z - d), h, (3,))

                @pl.when(z + d < PLANES)
                def _():
                    take(across(z + d), h, (3,))

    step_z(1)
    step_y(0)
    step_z(2)
    step_y(1)
    step_z(3)
    step_y(2)
    step_y(3)
    for b in range(n_dev):
        @pl.when(b % 2 != c)
        def _():
            for h in range(2):
                hop(b, h, 3).wait_recv()
                out_copy(b, h).start()

    for d in range(n_dev):
        @pl.when(d != me)
        def _():
            remote(packet.at[0], meta.at[d], send_m.at[d], recv_m.at[d], d).wait_recv()

    cnt = meta[:, 8, :]
    group = (iota((LANES, LANES), 0) // e_loc == iota((LANES, LANES), 1)).astype(F32).astype(BF16)
    n_rows = jnp.dot(cnt.astype(BF16), group, preferred_element_type=F32)
    ints[0:16, LANES:] = jnp.zeros((16, LANES), jnp.int32)
    ints[0:16, :LANES] = meta[:, pl.ds(q, 1), :].reshape(n_dev, LANES).astype(jnp.int32)
    ints[16:32, :LANES] = cnt.astype(jnp.int32)
    run = jnp.zeros((1, LANES), F32)
    for s in range(n_dev):
        off = run.astype(jnp.int32)
        ints[32 + s:33 + s, :LANES] = off
        ints[48 + s:49 + s, :LANES] = jnp.minimum(off // TILE, (r_max - WIN) // TILE)
        run = run + n_rows[s:s + 1]

    tail = [pltpu.make_async_copy(meta, meta_hbm, out_sem.at[0, 2]), pltpu.make_async_copy(ints, ints_hbm, out_sem.at[1, 2])]
    for cp in tail:
        cp.start()

    for h in range(2):
        def sent(b, way, more):
            @pl.when(more)
            def _():
                hop(b, h, way).wait_send()

            hop(b, h, 2).wait_send()
            hop(b, h, 3).wait_send()

        @pl.when(z < PLANES - 1)
        def _():
            hop(me, h, 0).wait_send()

        @pl.when(z > 0)
        def _():
            hop(me, h, 1).wait_send()

        hop(me, h, 2).wait_send()
        hop(me, h, 3).wait_send()
        for d in range(1, PLANES):
            from_z(d, sent)
        for zb in range(PLANES):
            hop(across(zb), h, 3).wait_send()
        for b in range(n_dev):
            out_copy(b, h).wait()
    for d in range(n_dev):
        @pl.when(d != me)
        def _():
            route_copy(d).wait_send()
    for cp in tail:
        cp.wait()


def spread(r_max, tokens, expert_ids, norm_gain, w_router):
    tok, width = tokens.shape
    n_dev = PLANES * QUAD
    sub = width // LANES
    hbm = pl.BlockSpec(memory_space=pltpu.HBM)
    vmem = pl.BlockSpec(memory_space=pltpu.VMEM)
    return pl.pallas_call(
        functools.partial(spread_kernel, r_max),
        out_shape=(jax.ShapeDtypeStruct((n_dev, tok * sub, LANES), BF16),
                   jax.ShapeDtypeStruct((n_dev, 16, LANES), F32),
                   jax.ShapeDtypeStruct((64, 2 * LANES), jnp.int32)),
        in_specs=[vmem] * 4,
        out_specs=(hbm, hbm, hbm),
        scratch_shapes=[
            pltpu.VMEM((n_dev, tok * sub, LANES), BF16),
            pltpu.VMEM((tok * sub, LANES), F32),
            pltpu.VMEM((tok, width), BF16),
            pltpu.VMEM((tok, LANES), F32),
            pltpu.VMEM((tok, LANES), F32),
            pltpu.VMEM((PLANES, 16, LANES), F32),
            pltpu.VMEM((n_dev, 16, LANES), F32),
            pltpu.VMEM((64, 2 * LANES), jnp.int32),
            pltpu.SemaphoreType.DMA((n_dev, 2, 4)),
            pltpu.SemaphoreType.DMA((n_dev, 2)),
            pltpu.SemaphoreType.DMA((n_dev,)),
            pltpu.SemaphoreType.DMA((n_dev,)),
            pltpu.SemaphoreType.DMA((n_dev, 3)),
        ],
        compiler_params=pltpu.CompilerParams(collective_id=0, has_side_effects=True, vmem_limit_bytes=66_000_000),
        name="spread",
    )(tokens, expert_ids.T, norm_gain.reshape(1, width), w_router)


def expert_kernel(n_src, sub, r_max, ints, meta, u_hbm, w1_hbm, w3_hbm, w2_hbm, o_hbm, win_hbm,
                  u_vm, o_all, xf, xb, hb, ob, win, w1, w3, w2, pre, sems, sem_w):
    n_exp = w1_hbm.shape[0]
    me, z, q = place()
    lane0 = me * n_exp

    def load(e, names):
        slot = lax.rem(e, 2)
        copies = []
        for i, (src, dst) in enumerate(((w1_hbm, w1), (w3_hbm, w3), (w2_hbm, w2))):
            if i in names:
                size = src.shape[1] // PIECES
                for p in range(PIECES):
                    part = pl.ds(p * size, size)
                    copies.append(pltpu.make_async_copy(src.at[e, part], dst.at[slot, part], sem_w.at[slot, i, p]))
        return copies

    def begin():
        cp = pltpu.make_async_copy(u_hbm, u_vm, sems.at[0])
        cp.start()
        for e in range(2):
            for w in load(e, (0, 1, 2)):
                w.start()
        for s in range(n_src):
            pre[s] = 0

        @pl.loop(0, r_max * PITCH // 256)
        def _(i):
            o_all[pl.ds(pl.multiple_of(i * 256, 256), 256), :] = jnp.zeros((256, LANES), F32)

        @pl.loop(0, n_src)
        def _(s):
            for m in range(QUAD):
                t = meta[s, m:m + 1, :]
                g = meta[s, QUAD + m:QUAD + m + 1, :]
                hi = g.astype(BF16).astype(F32)
                mid = (g - hi).astype(BF16).astype(F32)
                lo = (g - hi - mid).astype(BF16).astype(F32)
                rows = jnp.concatenate([t, hi, mid, lo, t, t, t, t], axis=0)
                rows = jnp.concatenate([rows, jnp.zeros((8, WIN - LANES), F32)], axis=1)
                r = z * QUAD + m
                win[s * QUAD + m] = pltpu.roll(rows, ints[32 + s, r] - TILE * ints[48 + s, r], 1)

        pltpu.make_async_copy(win, win_hbm, sems.at[1]).start()
        cp.wait()

    begin()

    def expert(e, _):
        slot = lax.rem(e, 2)
        def take(s, j0, n, i, at):
            t = s * LANES + ints[s, j0 + i]
            src = u_vm[pl.ds(pl.multiple_of(t * sub, sub), sub), :]
            xf[pl.ds(at * PITCH, sub), :] = src.astype(F32)

        def give(s, j0, n, i, at):
            o_all[pl.ds(at * PITCH, sub), :] = xf[pl.ds((n + i) * PITCH, sub), :]

        def sweep(body, target, spare):
            n = jnp.int32(0)
            top = jnp.int32(0)
            starts = []
            for s in range(n_src):
                cnt = ints[16 + s, lane0 + e]
                to = target(s, n)
                for i in range(STEP):
                    at = to + i if target is by_row else jnp.where(i < cnt, to + i, spare)
                    body(s, pre[s], n, i, at)
                starts.append(n)
                n = n + cnt
                top = jnp.maximum(top, cnt)
            for s in range(n_src):
                cnt = ints[16 + s, lane0 + e]

                @pl.when(cnt > STEP)
                def _():
                    to = target(s, starts[s])
                    for i in range(STEP, STEP + MORE):
                        body(s, pre[s], starts[s], i, jnp.where(i < cnt, to + i, spare))

            @pl.when(top > STEP + MORE)
            def _():
                def source(s, n):
                    cnt = ints[16 + s, lane0 + e]

                    def row(i, _):
                        body(s, pre[s], n, i, target(s, n) + i)
                        return 0

                    lax.fori_loop(STEP + MORE, cnt, row, 0)
                    return n + cnt

                lax.fori_loop(0, n_src, source, jnp.int32(0))

            return n

        def by_row(s, n):
            return n

        def by_slot(s, n):
            return ints[32 + s, me] + pre[s]

        n = sweep(take, by_row, r_max + 2 * STEP)

        for w in load(e, (0, 1, 2)):
            w.wait()

        def block(b, _):
            r0 = b * (BM * PITCH)
            for j in range(sub):
                xb[:, j * LANES:(j + 1) * LANES] = xf[pl.ds(r0 + j, BM, stride=PITCH), :].astype(BF16)
            g = jnp.dot(xb[...], w1[slot], preferred_element_type=F32)
            v = jnp.dot(xb[...], w3[slot], preferred_element_type=F32)
            hb[...] = (jax.nn.silu(g) * v).astype(BF16)
            for k in range(sub // 4):
                o = jnp.dot(hb[...], w2[slot, :, k * 512:(k + 1) * 512], preferred_element_type=F32)
                for j in range(4):
                    xf[pl.ds(r0 + k * 4 + j, BM, stride=PITCH), :] = o[:, j * LANES:(j + 1) * LANES]
            return 0

        lax.fori_loop(0, (n + BM - 1) // BM, block, 0)

        sweep(give, by_slot, r_max)
        for s in range(n_src):
            pre[s] = pre[s] + ints[16 + s, lane0 + e]

        @pl.when(e + 2 < n_exp)
        def _():
            for w in load(e + 2, (0, 1, 2)):
                w.start()

        return 0

    lax.fori_loop(0, n_exp, expert, 0)

    def put(j):
        return pltpu.make_async_copy(ob.at[j % 4], o_hbm.at[j], sems.at[2 + j % 4])

    for j in range(sub):
        if j >= 4:
            put(j - 4).wait()
        ob[j % 4] = o_all[pl.ds(j, r_max, stride=PITCH), :].astype(BF16)
        put(j).start()
    for j in range(sub - 4, sub):
        put(j).wait()
    pltpu.make_async_copy(win, win_hbm, sems.at[1]).wait()


def experts(n_src, r_max, ints, meta, u_rows, w1, w3, w2):
    n_exp, width, ff = w1.shape
    sub = width // LANES
    n_tok = u_rows.shape[0] // sub
    hbm = pl.BlockSpec(memory_space=pltpu.HBM)
    smem = pl.BlockSpec(memory_space=pltpu.SMEM)
    return pl.pallas_call(
        functools.partial(expert_kernel, n_src, sub, r_max),
        out_shape=(jax.ShapeDtypeStruct((sub, r_max, LANES), BF16),
                   jax.ShapeDtypeStruct((n_src * QUAD, 8, WIN), F32)),
        in_specs=[smem, pl.BlockSpec(memory_space=pltpu.VMEM), hbm, hbm, hbm, hbm],
        out_specs=(hbm, hbm),
        scratch_shapes=[
            pltpu.VMEM((n_tok * sub, LANES), BF16),
            pltpu.VMEM(((r_max + 8) * PITCH, LANES), F32),
            pltpu.VMEM(((r_max + 2 * STEP + 8) * PITCH, LANES), F32),
            pltpu.VMEM((BM, width), BF16),
            pltpu.VMEM((BM, ff), BF16),
            pltpu.VMEM((4, r_max, LANES), BF16),
            pltpu.VMEM((n_src * QUAD, 8, WIN), F32),
            pltpu.VMEM((2, width, ff), BF16),
            pltpu.VMEM((2, width, ff), BF16),
            pltpu.VMEM((2, ff, width), BF16),
            pltpu.SMEM((n_src,), jnp.int32),
            pltpu.SemaphoreType.DMA((6,)),
            pltpu.SemaphoreType.DMA((2, 3, PIECES)),
        ],
        compiler_params=pltpu.CompilerParams(vmem_limit_bytes=66_000_000),
        name="experts",
    )(ints, meta, u_rows, w1, w3, w2)


def collect_kernel(n_src, steps, ints, win, x_ref, o_hbm, out_ref,
                   mix, part, from_l, from_r, fin,
                   send_q, recv_q, send_z, recv_l, recv_r, send_f, recv_f, *rows):
    me, z, q = place()
    y, c = q // 2, lax.rem(q, 2)
    tok = x_ref.shape[0]
    plane = QUAD * tok
    others = ((1 - y) * 2 + c, (1 - y) * 2 + 1 - c, y * 2 + 1 - c)

    barrier = pltpu.get_barrier_semaphore()

    def hello(dev):
        pl.semaphore_signal(barrier, inc=1, device_id={'ep': dev}, device_id_type=pl.DeviceIdType.MESH)

    for m in others:
        hello(z * QUAD + m)

    @pl.when(z > 0)
    def _():
        hello(me - QUAD)

    @pl.when(z < PLANES - 1)
    def _():
        hello(me + QUAD)

    pl.semaphore_wait(barrier, 4 + (z + PLANES - 1) // PLANES - (z + 1) // PLANES)

    def quad_copy(k, m):
        return remote(o_hbm.at[m * steps + k], rows[k].at[q], send_q.at[k, m], recv_q.at[k, q], z * QUAD + m)

    def quad_wait(k, m):
        remote(o_hbm.at[0], rows[k].at[m], send_q.at[k, m], recv_q.at[k, m], z * QUAD + m).wait_recv()

    def own_copy(k):
        return pltpu.make_async_copy(o_hbm.at[q * steps + k], rows[k].at[q], recv_q.at[k, q])

    for k in range(steps):
        for m in others:
            quad_copy(k, m).start()
        own_copy(k).start()

    row_id = iota((tok, WIN), 0).astype(F32)

    def build(i, _):
        w = win[i]
        at = w[0:1] == row_id
        for part_i in range(3):
            mix[i, part_i * tok:(part_i + 1) * tok, :] = jnp.where(at, w[1 + part_i:2 + part_i], 0.0).astype(BF16)
        return 0

    lax.fori_loop(0, n_src * QUAD, build, 0)

    def combine(k):
        own_copy(k).wait()
        for m in others:
            quad_wait(k, m)

        def token_block(s, _):
            acc = jnp.zeros((3 * tok, LANES), F32)
            for m in range(QUAD):
                start = ints[48 + s, z * QUAD + m]
                span = jnp.concatenate([rows[k][m, start + i] for i in range(WIN // TILE)], axis=0)
                acc += jnp.dot(mix[s * QUAD + m], span, preferred_element_type=F32)
            part[k, s // QUAD, pl.ds(pl.multiple_of(lax.rem(s, QUAD) * tok, tok), tok), :] = acc[0:tok] + acc[tok:2 * tok] + acc[2 * tok:]

            return 0

        lax.fori_loop(0, n_src, token_block, 0)

    bit = plane // CUTS

    def right(k, zd, h):
        part_h = pl.ds(h * bit, bit)
        return remote(part.at[k, zd, part_h], from_l.at[k, zd, part_h], send_z.at[k, zd, h], recv_l.at[k, zd, h], me + QUAD)

    def left(k, zd, h):
        part_h = pl.ds(h * bit, bit)
        return remote(part.at[k, zd, part_h], from_r.at[k, zd, part_h], send_z.at[k, zd, h], recv_r.at[k, zd, h], me - QUAD)

    def forward(k):
        for i, h in [(i, h) for i in range(PLANES - 1) for h in range(CUTS)]:
            for to_right in (True, False):
                zd = PLANES - 1 - i if to_right else i
                box = from_l if to_right else from_r
                go = right if to_right else left
                rows_h = pl.ds(h * bit, bit)

                @pl.when(z < zd if to_right else z > zd)
                def _():
                    @pl.when(z > 0 if to_right else z < PLANES - 1)
                    def _():
                        go(k, zd, h).wait_recv()
                        part[k, zd, rows_h] += box[k, zd, rows_h]

                    go(k, zd, h).start()

    def final_copy(k, m):
        src = part.at[k, z, pl.ds(m * tok, tok)]
        return remote(src, fin.at[k, q], send_f.at[k, m], recv_f.at[k, q], z * QUAD + m)

    def finish(k):
        @pl.when(z > 0)
        def _():
            for h in range(CUTS):
                right(k, z, h).wait_recv()
            part[k, z] += from_l[k, z]

        @pl.when(z < PLANES - 1)
        def _():
            for h in range(CUTS):
                left(k, z, h).wait_recv()
            part[k, z] += from_r[k, z]

        for m in others:
            final_copy(k, m).start()
        fin[k, q] = part[k, z, pl.ds(pl.multiple_of(q * tok, tok), tok), :]

    for k in range(steps):
        combine(k)
        forward(k)
        if k > 0:
            finish(k - 1)
    finish(steps - 1)

    for k in range(steps):
        for m in others:
            remote(part.at[k, z, pl.ds(0, tok)], fin.at[k, m], send_f.at[k, m], recv_f.at[k, m], z * QUAD + m).wait_recv()
        for m in range(QUAD):
            cols = pl.ds((m * steps + k) * LANES, LANES)
            out_ref[:, cols] = (x_ref[:, cols].astype(F32) + fin[k, m]).astype(BF16)

    for k in range(steps):
        for m in others:
            quad_copy(k, m).wait_send()
            final_copy(k, m).wait_send()
        for zd in range(PLANES):
            @pl.when(z < zd)
            def _():
                for h in range(CUTS):
                    right(k, zd, h).wait_send()

            @pl.when(z > zd)
            def _():
                for h in range(CUTS):
                    left(k, zd, h).wait_send()


def collect(ints, win, tokens, o_rows):
    tok, width = tokens.shape
    sub, r_tiles = o_rows.shape[:2]
    n_src = PLANES * QUAD
    steps = sub // QUAD
    vmem = pl.BlockSpec(memory_space=pltpu.VMEM)
    return pl.pallas_call(
        functools.partial(collect_kernel, n_src, steps),
        out_shape=jax.ShapeDtypeStruct((tok, width), BF16),
        in_specs=[pl.BlockSpec(memory_space=pltpu.SMEM), vmem, vmem, pl.BlockSpec(memory_space=pltpu.HBM)],
        out_specs=vmem,
        scratch_shapes=[
            pltpu.VMEM((n_src * QUAD, 3 * tok, WIN), BF16),
            pltpu.VMEM((steps, PLANES, QUAD * tok, LANES), F32),
            pltpu.VMEM((steps, PLANES, QUAD * tok, LANES), F32),
            pltpu.VMEM((steps, PLANES, QUAD * tok, LANES), F32),
            pltpu.VMEM((steps, QUAD, tok, LANES), F32),
            pltpu.SemaphoreType.DMA((steps, QUAD)),
            pltpu.SemaphoreType.DMA((steps, QUAD)),
            pltpu.SemaphoreType.DMA((steps, PLANES, CUTS)),
            pltpu.SemaphoreType.DMA((steps, PLANES, CUTS)),
            pltpu.SemaphoreType.DMA((steps, PLANES, CUTS)),
            pltpu.SemaphoreType.DMA((steps, QUAD)),
            pltpu.SemaphoreType.DMA((steps, QUAD)),
        ] + [pltpu.VMEM((QUAD, r_tiles, TILE, LANES), BF16)] * steps,
        compiler_params=pltpu.CompilerParams(collective_id=1, has_side_effects=True, vmem_limit_bytes=56 * 2 ** 20),
        name="collect",
    )(ints, win, tokens, o_rows)


def solution(mesh):
    ep_size = mesh.shape['ep']

    def device_step(tokens, expert_ids, norm_gain, w_router, w_gate, w_up, w_down):
        pairs = expert_ids.shape[0] * expert_ids.shape[1]
        r_max = 3 * pairs // 2
        u_rows, meta, ints = spread(r_max, tokens, expert_ids, norm_gain, w_router)
        u_rows = u_rows.reshape(-1, LANES)
        o_rows, win = experts(ep_size, r_max, ints, meta, u_rows, w_gate, w_up, w_down)
        return collect(ints, win, tokens, o_rows.reshape(-1, r_max // TILE, TILE, LANES))

    row_spec = P(('dp', 'ep'), None)
    expert_spec = P('ep', None, None)
    return jax.shard_map(device_step, mesh=mesh, in_specs=(row_spec, row_spec, P(None), P(None, None), expert_spec, expert_spec, expert_spec), out_specs=row_spec, check_vma=False)
```

```python
import functools

import jax
import jax.numpy as jnp
from jax import lax
from jax.experimental import pallas as pl
from jax.experimental.pallas import tpu as pltpu
from jax.sharding import PartitionSpec as P

NORM_EPS = 1e-5
LANES = 128
BM = 128
WIN = 256
CUTS = 1
TILE = 16
PITCH = 17
STEP = 8
MORE = 8
PIECES = 4
QUAD = 4
PLANES = 4
F32 = jnp.float32
BF16 = jnp.bfloat16


def iota(shape, dim):
    return lax.broadcasted_iota(jnp.int32, shape, dim)


def place():
    me = lax.axis_index('ep')
    return me, me // QUAD, lax.rem(me, QUAD)


def remote(src, dst, send, recv, dev):
    return pltpu.make_async_remote_copy(src_ref=src, dst_ref=dst, send_sem=send, recv_sem=recv,
                                        device_id={'ep': dev}, device_id_type=pl.DeviceIdType.MESH)


def spread_kernel(r_max, x_ref, ids_ref, gain_ref, wr_ref, u_hbm, meta_hbm, ints_hbm,
                  u_all, xs, ub, pos_s, p_s, packet, meta, ints,
                  send_u, recv_u, send_m, recv_m, out_sem):
    n_dev = PLANES * QUAD
    me, z, q = place()
    y, c = q // 2, lax.rem(q, 2)
    half = u_all.shape[1] // 2
    tok = x_ref.shape[0]
    sub = u_all.shape[1] // tok

    barrier = pltpu.get_barrier_semaphore()
    for d in range(1, n_dev):
        pl.semaphore_signal(barrier, inc=1, device_id={'ep': lax.rem(me + d, n_dev)}, device_id_type=pl.DeviceIdType.MESH)

    x32 = x_ref[...].astype(F32)
    inv = lax.rsqrt(jnp.mean(x32 * x32, axis=1, keepdims=True) + NORM_EPS)
    ub[...] = (x32 * inv * gain_ref[...].astype(F32)).astype(BF16)
    for j in range(sub):
        xs[pl.ds(j, tok, stride=sub), :] = ub[:, j * LANES:(j + 1) * LANES].astype(F32)
    u_all[me] = xs[...].astype(BF16)
    pl.semaphore_wait(barrier, n_dev - 1)

    dest = (me + QUAD, me - QUAD, z * QUAD + (1 - y) * 2 + c, z * QUAD + y * 2 + 1 - c)

    def hop(b, h, way):
        rows = u_all.at[b, pl.ds(h * half, half)]
        return remote(rows, rows, send_u.at[b, h, way], recv_u.at[b, h], dest[way])

    def out_copy(b, h):
        rows = pl.ds(h * half, half)
        return pltpu.make_async_copy(u_all.at[b, rows], u_hbm.at[b, rows], out_sem.at[b, h])

    for h in range(2):
        @pl.when(z < PLANES - 1)
        def _():
            hop(me, h, 0).start()

        @pl.when(z > 0)
        def _():
            hop(me, h, 1).start()

        hop(me, h, 2).start()
        hop(me, h, 3).start()
        out_copy(me, h).start()

    logits = jnp.dot(ub[...], wr_ref[...], preferred_element_type=F32)
    top = jnp.max(logits, axis=1, keepdims=True)
    ex = jnp.exp(logits - top)
    p_s[...] = ex / jnp.sum(ex, axis=1, keepdims=True)
    lane = iota((tok, LANES), 1)
    hit = lane < 0
    ids = ids_ref[...].T
    for k in range(ids.shape[1]):
        hit = jnp.logical_or(hit, ids[:, k:k + 1] == lane)
    hit32 = hit.astype(F32)
    hit_b = hit32.astype(BF16)
    tri = (iota((tok, tok), 0) > iota((tok, tok), 1)).astype(F32).astype(BF16)
    rank = jnp.dot(tri, hit_b, preferred_element_type=F32)
    count = jnp.sum(hit32, axis=0, keepdims=True)
    row_e, col_e = iota((LANES, LANES), 0), iota((LANES, LANES), 1)
    e_loc = LANES // n_dev
    before = jnp.logical_and(row_e < col_e, row_e // e_loc == col_e // e_loc).astype(F32).astype(BF16)
    count8 = jnp.broadcast_to(count, (8, LANES))
    base = jnp.dot(count8.astype(BF16), before, preferred_element_type=F32)[0:1]
    pos_s[...] = jnp.where(hit, base + rank, -1.0)
    t_id = iota((tok, LANES), 0).astype(F32)
    lane_f = lane.astype(F32)

    def pack(zd, _):
        for m in range(QUAD):
            tk = jnp.zeros((tok, LANES), F32)
            gt = jnp.zeros((tok, LANES), F32)
            for ee in range(e_loc):
                col = m * e_loc + ee
                at = pos_s[:, col:col + 1] == lane_f
                tk = jnp.where(at, t_id, tk)
                gt = jnp.where(at, p_s[:, col:col + 1], gt)
            packet[zd, m:m + 1, :] = jnp.sum(tk, axis=0, keepdims=True)
            packet[zd, QUAD + m:QUAD + m + 1, :] = jnp.sum(gt, axis=0, keepdims=True)
        packet[zd, 8:16, :] = count8
        pos_s[...] = pltpu.roll(pos_s[...], LANES - QUAD * e_loc, 1)
        p_s[...] = pltpu.roll(p_s[...], LANES - QUAD * e_loc, 1)
        return 0

    lax.fori_loop(0, PLANES, pack, 0)

    def route_copy(d):
        return remote(packet.at[d // QUAD], meta.at[me], send_m.at[d], recv_m.at[me], d)

    for d in range(n_dev):
        @pl.when(d != me)
        def _():
            route_copy(d).start()

    meta[me] = packet[z]

    def take(b, h, ways):
        hop(b, h, 3).wait_recv()
        out_copy(b, h).start()
        for way in ways:
            hop(b, h, way).start()

    def from_z(d, fn):
        @pl.when(z >= d)
        def _():
            fn(me - QUAD * d, 0, z < PLANES - 1)

        @pl.when(z + d < PLANES)
        def _():
            fn(me + QUAD * d, 1, z > 0)

    def across(zb):
        return zb * QUAD + (1 - y) * 2 + c

    def step_z(d):
        for h in range(2):
            def on(b, way, more):
                hop(b, h, 3).wait_recv()

                @pl.when(more)
                def _():
                    hop(b, h, way).start()

                hop(b, h, 2).start()
                hop(b, h, 3).start()
                out_copy(b, h).start()

            from_z(d, on)

    def step_y(d):
        for h in range(2):
            if d == 0:
                take(across(z), h, (3,))
            else:
                @pl.when(z >= d)
                def _():
                    take(across(z - d), h, (3,))

                @pl.when(z + d < PLANES)
                def _():
                    take(across(z + d), h, (3,))

    step_z(1)
    step_y(0)
    step_z(2)
    step_y(1)
    step_z(3)
    step_y(2)
    step_y(3)
    for b in range(n_dev):
        @pl.when(b % 2 != c)
        def _():
            for h in range(2):
                hop(b, h, 3).wait_recv()
                out_copy(b, h).start()

    for d in range(n_dev):
        @pl.when(d != me)
        def _():
            remote(packet.at[0], meta.at[d], send_m.at[d], recv_m.at[d], d).wait_recv()

    cnt = meta[:, 8, :]
    group = (iota((LANES, LANES), 0) // e_loc == iota((LANES, LANES), 1)).astype(F32).astype(BF16)
    n_rows = jnp.dot(cnt.astype(BF16), group, preferred_element_type=F32)
    ints[0:16, LANES:] = jnp.zeros((16, LANES), jnp.int32)
    ints[0:16, :LANES] = meta[:, pl.ds(q, 1), :].reshape(n_dev, LANES).astype(jnp.int32)
    ints[16:32, :LANES] = cnt.astype(jnp.int32)
    run = jnp.zeros((1, LANES), F32)
    for s in range(n_dev):
        off = run.astype(jnp.int32)
        ints[32 + s:33 + s, :LANES] = off
        ints[48 + s:49 + s, :LANES] = jnp.minimum(off // TILE, (r_max - WIN) // TILE)
        run = run + n_rows[s:s + 1]

    tail = [pltpu.make_async_copy(meta, meta_hbm, out_sem.at[0, 2]), pltpu.make_async_copy(ints, ints_hbm, out_sem.at[1, 2])]
    for cp in tail:
        cp.start()

    for h in range(2):
        def sent(b, way, more):
            @pl.when(more)
            def _():
                hop(b, h, way).wait_send()

            hop(b, h, 2).wait_send()
            hop(b, h, 3).wait_send()

        @pl.when(z < PLANES - 1)
        def _():
            hop(me, h, 0).wait_send()

        @pl.when(z > 0)
        def _():
            hop(me, h, 1).wait_send()

        hop(me, h, 2).wait_send()
        hop(me, h, 3).wait_send()
        for d in range(1, PLANES):
            from_z(d, sent)
        for zb in range(PLANES):
            hop(across(zb), h, 3).wait_send()
        for b in range(n_dev):
            out_copy(b, h).wait()
    for d in range(n_dev):
        @pl.when(d != me)
        def _():
            route_copy(d).wait_send()
    for cp in tail:
        cp.wait()


def spread(r_max, tokens, expert_ids, norm_gain, w_router):
    tok, width = tokens.shape
    n_dev = PLANES * QUAD
    sub = width // LANES
    hbm = pl.BlockSpec(memory_space=pltpu.HBM)
    vmem = pl.BlockSpec(memory_space=pltpu.VMEM)
    return pl.pallas_call(
        functools.partial(spread_kernel, r_max),
        out_shape=(jax.ShapeDtypeStruct((n_dev, tok * sub, LANES), BF16),
                   jax.ShapeDtypeStruct((n_dev, 16, LANES), F32),
                   jax.ShapeDtypeStruct((64, 2 * LANES), jnp.int32)),
        in_specs=[vmem] * 4,
        out_specs=(hbm, hbm, hbm),
        scratch_shapes=[
            pltpu.VMEM((n_dev, tok * sub, LANES), BF16),
            pltpu.VMEM((tok * sub, LANES), F32),
            pltpu.VMEM((tok, width), BF16),
            pltpu.VMEM((tok, LANES), F32),
            pltpu.VMEM((tok, LANES), F32),
            pltpu.VMEM((PLANES, 16, LANES), F32),
            pltpu.VMEM((n_dev, 16, LANES), F32),
            pltpu.VMEM((64, 2 * LANES), jnp.int32),
            pltpu.SemaphoreType.DMA((n_dev, 2, 4)),
            pltpu.SemaphoreType.DMA((n_dev, 2)),
            pltpu.SemaphoreType.DMA((n_dev,)),
            pltpu.SemaphoreType.DMA((n_dev,)),
            pltpu.SemaphoreType.DMA((n_dev, 3)),
        ],
        compiler_params=pltpu.CompilerParams(collective_id=0, has_side_effects=True, vmem_limit_bytes=66_000_000),
        name="spread",
    )(tokens, expert_ids.T, norm_gain.reshape(1, width), w_router)


def expert_kernel(n_src, sub, r_max, ints, meta, u_hbm, w1_hbm, w3_hbm, w2_hbm, o_hbm, win_hbm,
                  u_vm, o_all, xf, xb, hb, ob, win, w1, w3, w2, pre, sems, sem_w):
    n_exp = w1_hbm.shape[0]
    me, z, q = place()
    lane0 = me * n_exp

    def load(e, names):
        slot = lax.rem(e, 2)
        copies = []
        for i, (src, dst) in enumerate(((w1_hbm, w1), (w3_hbm, w3), (w2_hbm, w2))):
            if i in names:
                size = src.shape[1] // PIECES
                for p in range(PIECES):
                    part = pl.ds(p * size, size)
                    copies.append(pltpu.make_async_copy(src.at[e, part], dst.at[slot, part], sem_w.at[slot, i, p]))
        return copies

    def start(copies):
        for i, w in enumerate(copies):
            w.start(priority=i % 2)

    def begin():
        cp = pltpu.make_async_copy(u_hbm, u_vm, sems.at[0])
        cp.start()
        for e in range(2):
            start(load(e, (0, 1, 2)))
        for s in range(n_src):
            pre[s] = 0

        @pl.loop(0, r_max * PITCH // 256)
        def _(i):
            o_all[pl.ds(pl.multiple_of(i * 256, 256), 256), :] = jnp.zeros((256, LANES), F32)

        @pl.loop(0, n_src)
        def _(s):
            for m in range(QUAD):
                t = meta[s, m:m + 1, :]
                g = meta[s, QUAD + m:QUAD + m + 1, :]
                hi = g.astype(BF16).astype(F32)
                mid = (g - hi).astype(BF16).astype(F32)
                lo = (g - hi - mid).astype(BF16).astype(F32)
                rows = jnp.concatenate([t, hi, mid, lo, t, t, t, t], axis=0)
                rows = jnp.concatenate([rows, jnp.zeros((8, WIN - LANES), F32)], axis=1)
                r = z * QUAD + m
                win[s * QUAD + m] = pltpu.roll(rows, ints[32 + s, r] - TILE * ints[48 + s, r], 1)

        pltpu.make_async_copy(win, win_hbm, sems.at[1]).start()
        cp.wait()

    begin()

    def expert(e, _):
        slot = lax.rem(e, 2)
        def take(s, j0, n, i, at):
            t = s * LANES + ints[s, j0 + i]
            src = u_vm[pl.ds(pl.multiple_of(t * sub, sub), sub), :]
            xf[pl.ds(at * PITCH, sub), :] = src.astype(F32)

        def give(s, j0, n, i, at):
            o_all[pl.ds(at * PITCH, sub), :] = xf[pl.ds((n + i) * PITCH, sub), :]

        def sweep(body, target, spare):
            n = jnp.int32(0)
            top = jnp.int32(0)
            starts = []
            for s in range(n_src):
                cnt = ints[16 + s, lane0 + e]
                to = target(s, n)
                for i in range(STEP):
                    at = to + i if target is by_row else jnp.where(i < cnt, to + i, spare)
                    body(s, pre[s], n, i, at)
                starts.append(n)
                n = n + cnt
                top = jnp.maximum(top, cnt)
            for s in range(n_src):
                cnt = ints[16 + s, lane0 + e]

                @pl.when(cnt > STEP)
                def _():
                    to = target(s, starts[s])
                    for i in range(STEP, STEP + MORE):
                        body(s, pre[s], starts[s], i, jnp.where(i < cnt, to + i, spare))

            @pl.when(top > STEP + MORE)
            def _():
                def source(s, n):
                    cnt = ints[16 + s, lane0 + e]

                    def row(i, _):
                        body(s, pre[s], n, i, target(s, n) + i)
                        return 0

                    lax.fori_loop(STEP + MORE, cnt, row, 0)
                    return n + cnt

                lax.fori_loop(0, n_src, source, jnp.int32(0))

            return n

        def by_row(s, n):
            return n

        def by_slot(s, n):
            return ints[32 + s, me] + pre[s]

        n = sweep(take, by_row, r_max + 2 * STEP)

        for w in load(e, (0, 1, 2)):
            w.wait()

        def block(b, _):
            r0 = b * (BM * PITCH)
            for j in range(sub):
                xb[:, j * LANES:(j + 1) * LANES] = xf[pl.ds(r0 + j, BM, stride=PITCH), :].astype(BF16)
            g = jnp.dot(xb[...], w1[slot], preferred_element_type=F32)
            v = jnp.dot(xb[...], w3[slot], preferred_element_type=F32)
            hb[...] = (jax.nn.silu(g) * v).astype(BF16)
            for k in range(sub // 4):
                o = jnp.dot(hb[...], w2[slot, :, k * 512:(k + 1) * 512], preferred_element_type=F32)
                for j in range(4):
                    xf[pl.ds(r0 + k * 4 + j, BM, stride=PITCH), :] = o[:, j * LANES:(j + 1) * LANES]
            return 0

        lax.fori_loop(0, (n + BM - 1) // BM, block, 0)

        sweep(give, by_slot, r_max)
        for s in range(n_src):
            pre[s] = pre[s] + ints[16 + s, lane0 + e]

        @pl.when(e + 2 < n_exp)
        def _():
            start(load(e + 2, (0, 1, 2)))

        return 0

    lax.fori_loop(0, n_exp, expert, 0)

    def put(j):
        return pltpu.make_async_copy(ob.at[j % 4], o_hbm.at[j], sems.at[2 + j % 4])

    for j in range(sub):
        if j >= 4:
            put(j - 4).wait()
        ob[j % 4] = o_all[pl.ds(j, r_max, stride=PITCH), :].astype(BF16)
        put(j).start()
    for j in range(sub - 4, sub):
        put(j).wait()
    pltpu.make_async_copy(win, win_hbm, sems.at[1]).wait()


def experts(n_src, r_max, ints, meta, u_rows, w1, w3, w2):
    n_exp, width, ff = w1.shape
    sub = width // LANES
    n_tok = u_rows.shape[0] // sub
    hbm = pl.BlockSpec(memory_space=pltpu.HBM)
    smem = pl.BlockSpec(memory_space=pltpu.SMEM)
    return pl.pallas_call(
        functools.partial(expert_kernel, n_src, sub, r_max),
        out_shape=(jax.ShapeDtypeStruct((sub, r_max, LANES), BF16),
                   jax.ShapeDtypeStruct((n_src * QUAD, 8, WIN), F32)),
        in_specs=[smem, pl.BlockSpec(memory_space=pltpu.VMEM), hbm, hbm, hbm, hbm],
        out_specs=(hbm, hbm),
        scratch_shapes=[
            pltpu.VMEM((n_tok * sub, LANES), BF16),
            pltpu.VMEM(((r_max + 8) * PITCH, LANES), F32),
            pltpu.VMEM(((r_max + 2 * STEP + 8) * PITCH, LANES), F32),
            pltpu.VMEM((BM, width), BF16),
            pltpu.VMEM((BM, ff), BF16),
            pltpu.VMEM((4, r_max, LANES), BF16),
            pltpu.VMEM((n_src * QUAD, 8, WIN), F32),
            pltpu.VMEM((2, width, ff), BF16),
            pltpu.VMEM((2, width, ff), BF16),
            pltpu.VMEM((2, ff, width), BF16),
            pltpu.SMEM((n_src,), jnp.int32),
            pltpu.SemaphoreType.DMA((6,)),
            pltpu.SemaphoreType.DMA((2, 3, PIECES)),
        ],
        compiler_params=pltpu.CompilerParams(vmem_limit_bytes=66_000_000),
        name="experts",
    )(ints, meta, u_rows, w1, w3, w2)


def collect_kernel(n_src, steps, ints, win, x_ref, o_hbm, out_ref,
                   mix, part, from_l, from_r, fin,
                   send_q, recv_q, send_z, recv_l, recv_r, send_f, recv_f, stage, stage_sem, *rows):
    me, z, q = place()
    y, c = q // 2, lax.rem(q, 2)
    tok = x_ref.shape[0]
    plane = QUAD * tok
    others = ((1 - y) * 2 + c, (1 - y) * 2 + 1 - c, y * 2 + 1 - c)

    barrier = pltpu.get_barrier_semaphore()

    def hello(dev):
        pl.semaphore_signal(barrier, inc=1, device_id={'ep': dev}, device_id_type=pl.DeviceIdType.MESH)

    def stage_copy(k, m):
        return pltpu.make_async_copy(o_hbm.at[m * steps + k], stage.at[k, m], stage_sem.at[k, m])

    def own_copy(k):
        return pltpu.make_async_copy(o_hbm.at[q * steps + k], rows[k].at[q], recv_q.at[k, q])

    for k in range(steps):
        for m in others:
            stage_copy(k, m).start()
        own_copy(k).start()

    for m in others:
        hello(z * QUAD + m)

    @pl.when(z > 0)
    def _():
        hello(me - QUAD)

    @pl.when(z < PLANES - 1)
    def _():
        hello(me + QUAD)

    pl.semaphore_wait(barrier, 4 + (z + PLANES - 1) // PLANES - (z + 1) // PLANES)

    def quad_copy(k, m):
        return remote(stage.at[k, m], rows[k].at[q], send_q.at[k, m], recv_q.at[k, q], z * QUAD + m)

    def quad_wait(k, m):
        remote(stage.at[k, m], rows[k].at[m], send_q.at[k, m], recv_q.at[k, m], z * QUAD + m).wait_recv()

    for k in range(steps):
        for m in others:
            stage_copy(k, m).wait()
            quad_copy(k, m).start()

    row_id = iota((tok, WIN), 0).astype(F32)

    def build(i, _):
        w = win[i]
        at = w[0:1] == row_id
        for part_i in range(3):
            mix[i, part_i * tok:(part_i + 1) * tok, :] = jnp.where(at, w[1 + part_i:2 + part_i], 0.0).astype(BF16)
        return 0

    lax.fori_loop(0, n_src * QUAD, build, 0)

    def combine(k):
        own_copy(k).wait()
        for m in others:
            quad_wait(k, m)

        def token_block(s, _):
            acc = jnp.zeros((3 * tok, LANES), F32)
            for m in range(QUAD):
                start = ints[48 + s, z * QUAD + m]
                span = jnp.concatenate([rows[k][m, start + i] for i in range(WIN // TILE)], axis=0)
                acc += jnp.dot(mix[s * QUAD + m], span, preferred_element_type=F32)
            part[k, s // QUAD, pl.ds(pl.multiple_of(lax.rem(s, QUAD) * tok, tok), tok), :] = acc[0:tok] + acc[tok:2 * tok] + acc[2 * tok:]

            return 0

        lax.fori_loop(0, n_src, token_block, 0)

    bit = plane // CUTS

    def right(k, zd, h):
        part_h = pl.ds(h * bit, bit)
        return remote(part.at[k, zd, part_h], from_l.at[k, zd, part_h], send_z.at[k, zd, h], recv_l.at[k, zd, h], me + QUAD)

    def left(k, zd, h):
        part_h = pl.ds(h * bit, bit)
        return remote(part.at[k, zd, part_h], from_r.at[k, zd, part_h], send_z.at[k, zd, h], recv_r.at[k, zd, h], me - QUAD)

    def forward(k):
        for i, h in [(i, h) for i in range(PLANES - 1) for h in range(CUTS)]:
            for to_right in (True, False):
                zd = PLANES - 1 - i if to_right else i
                box = from_l if to_right else from_r
                go = right if to_right else left
                rows_h = pl.ds(h * bit, bit)

                @pl.when(z < zd if to_right else z > zd)
                def _():
                    @pl.when(z > 0 if to_right else z < PLANES - 1)
                    def _():
                        go(k, zd, h).wait_recv()
                        part[k, zd, rows_h] += box[k, zd, rows_h]

                    go(k, zd, h).start()

    def final_copy(k, m):
        src = part.at[k, z, pl.ds(m * tok, tok)]
        return remote(src, fin.at[k, q], send_f.at[k, m], recv_f.at[k, q], z * QUAD + m)

    def finish(k):
        @pl.when(z > 0)
        def _():
            for h in range(CUTS):
                right(k, z, h).wait_recv()
            part[k, z] += from_l[k, z]

        @pl.when(z < PLANES - 1)
        def _():
            for h in range(CUTS):
                left(k, z, h).wait_recv()
            part[k, z] += from_r[k, z]

        for m in others:
            final_copy(k, m).start()
        fin[k, q] = part[k, z, pl.ds(pl.multiple_of(q * tok, tok), tok), :]

    for k in range(steps):
        combine(k)
        forward(k)
        if k > 0:
            finish(k - 1)
    finish(steps - 1)

    for k in range(steps):
        for m in others:
            remote(part.at[k, z, pl.ds(0, tok)], fin.at[k, m], send_f.at[k, m], recv_f.at[k, m], z * QUAD + m).wait_recv()
        for m in range(QUAD):
            cols = pl.ds((m * steps + k) * LANES, LANES)
            out_ref[:, cols] = (x_ref[:, cols].astype(F32) + fin[k, m]).astype(BF16)

    for k in range(steps):
        for m in others:
            quad_copy(k, m).wait_send()
            final_copy(k, m).wait_send()
        for zd in range(PLANES):
            @pl.when(z < zd)
            def _():
                for h in range(CUTS):
                    right(k, zd, h).wait_send()

            @pl.when(z > zd)
            def _():
                for h in range(CUTS):
                    left(k, zd, h).wait_send()


def collect(ints, win, tokens, o_rows):
    tok, width = tokens.shape
    sub, r_tiles = o_rows.shape[:2]
    n_src = PLANES * QUAD
    steps = sub // QUAD
    vmem = pl.BlockSpec(memory_space=pltpu.VMEM)
    return pl.pallas_call(
        functools.partial(collect_kernel, n_src, steps),
        out_shape=jax.ShapeDtypeStruct((tok, width), BF16),
        in_specs=[pl.BlockSpec(memory_space=pltpu.SMEM), vmem, vmem, pl.BlockSpec(memory_space=pltpu.HBM)],
        out_specs=vmem,
        scratch_shapes=[
            pltpu.VMEM((n_src * QUAD, 3 * tok, WIN), BF16),
            pltpu.VMEM((steps, PLANES, QUAD * tok, LANES), F32),
            pltpu.VMEM((steps, PLANES, QUAD * tok, LANES), F32),
            pltpu.VMEM((steps, PLANES, QUAD * tok, LANES), F32),
            pltpu.VMEM((steps, QUAD, tok, LANES), F32),
            pltpu.SemaphoreType.DMA((steps, QUAD)),
            pltpu.SemaphoreType.DMA((steps, QUAD)),
            pltpu.SemaphoreType.DMA((steps, PLANES, CUTS)),
            pltpu.SemaphoreType.DMA((steps, PLANES, CUTS)),
            pltpu.SemaphoreType.DMA((steps, PLANES, CUTS)),
            pltpu.SemaphoreType.DMA((steps, QUAD)),
            pltpu.SemaphoreType.DMA((steps, QUAD)),
            pltpu.VMEM((steps, QUAD, r_tiles, TILE, LANES), BF16),
            pltpu.SemaphoreType.DMA((steps, QUAD)),
        ] + [pltpu.VMEM((QUAD, r_tiles, TILE, LANES), BF16)] * steps,
        compiler_params=pltpu.CompilerParams(collective_id=1, has_side_effects=True, vmem_limit_bytes=56 * 2 ** 20),
        name="collect",
    )(ints, win, tokens, o_rows)


def solution(mesh):
    ep_size = mesh.shape['ep']

    def device_step(tokens, expert_ids, norm_gain, w_router, w_gate, w_up, w_down):
        pairs = expert_ids.shape[0] * expert_ids.shape[1]
        r_max = 3 * pairs // 2
        u_rows, meta, ints = spread(r_max, tokens, expert_ids, norm_gain, w_router)
        u_rows = u_rows.reshape(-1, LANES)
        o_rows, win = experts(ep_size, r_max, ints, meta, u_rows, w_gate, w_up, w_down)
        return collect(ints, win, tokens, o_rows.reshape(-1, r_max // TILE, TILE, LANES))

    row_spec = P(('dp', 'ep'), None)
    expert_spec = P('ep', None, None)
    return jax.shard_map(device_step, mesh=mesh, in_specs=(row_spec, row_spec, P(None), P(None, None), expert_spec, expert_spec, expert_spec), out_specs=row_spec, check_vma=False)
```

```python
import functools

import jax
import jax.numpy as jnp
from jax import lax
from jax.experimental import pallas as pl
from jax.experimental.pallas import tpu as pltpu
from jax.sharding import PartitionSpec as P

NORM_EPS = 1e-5
LANES = 128
BM = 128
WIN = 256
CUTS = 2
TILE = 16
PITCH = 17
STEP = 8
MORE = 8
PIECES = 4
QUAD = 4
PLANES = 4
F32 = jnp.float32
BF16 = jnp.bfloat16


def iota(shape, dim):
    return lax.broadcasted_iota(jnp.int32, shape, dim)


def place():
    me = lax.axis_index('ep')
    return me, me // QUAD, lax.rem(me, QUAD)


def remote(src, dst, send, recv, dev):
    return pltpu.make_async_remote_copy(src_ref=src, dst_ref=dst, send_sem=send, recv_sem=recv,
                                        device_id={'ep': dev}, device_id_type=pl.DeviceIdType.MESH)


def spread_kernel(r_max, x_ref, ids_ref, gain_ref, wr_ref, u_hbm, meta_hbm, ints_hbm,
                  u_all, xs, ub, pos_s, p_s, packet, meta, ints,
                  send_u, recv_u, send_m, recv_m, out_sem):
    n_dev = PLANES * QUAD
    me, z, q = place()
    y, c = q // 2, lax.rem(q, 2)
    half = u_all.shape[1] // 2
    tok = x_ref.shape[0]
    sub = u_all.shape[1] // tok

    barrier = pltpu.get_barrier_semaphore()
    for d in range(1, n_dev):
        pl.semaphore_signal(barrier, inc=1, device_id={'ep': lax.rem(me + d, n_dev)}, device_id_type=pl.DeviceIdType.MESH)

    x32 = x_ref[...].astype(F32)
    inv = lax.rsqrt(jnp.mean(x32 * x32, axis=1, keepdims=True) + NORM_EPS)
    ub[...] = (x32 * inv * gain_ref[...].astype(F32)).astype(BF16)
    for j in range(sub):
        xs[pl.ds(j, tok, stride=sub), :] = ub[:, j * LANES:(j + 1) * LANES].astype(F32)
    u_all[me] = xs[...].astype(BF16)
    pl.semaphore_wait(barrier, n_dev - 1)

    dest = (me + QUAD, me - QUAD, z * QUAD + (1 - y) * 2 + c, z * QUAD + y * 2 + 1 - c)

    def hop(b, h, way):
        rows = u_all.at[b, pl.ds(h * half, half)]
        return remote(rows, rows, send_u.at[b, h, way], recv_u.at[b, h], dest[way])

    def out_copy(b, h):
        rows = pl.ds(h * half, half)
        return pltpu.make_async_copy(u_all.at[b, rows], u_hbm.at[b, rows], out_sem.at[b, h])

    def own_sends():
        for h in range(2):
            @pl.when(z < PLANES - 1)
            def _():
                hop(me, h, 0).start()

            @pl.when(z > 0)
            def _():
                hop(me, h, 1).start()

            hop(me, h, 2).start()
            hop(me, h, 3).start()
            out_copy(me, h).start()

    @pl.when(c == 0)
    def _():
        own_sends()

    logits = jnp.dot(ub[...], wr_ref[...], preferred_element_type=F32)
    top = jnp.max(logits, axis=1, keepdims=True)
    ex = jnp.exp(logits - top)
    p_s[...] = ex / jnp.sum(ex, axis=1, keepdims=True)
    lane = iota((tok, LANES), 1)
    hit = lane < 0
    ids = ids_ref[...].T
    for k in range(ids.shape[1]):
        hit = jnp.logical_or(hit, ids[:, k:k + 1] == lane)
    hit32 = hit.astype(F32)
    hit_b = hit32.astype(BF16)
    tri = (iota((tok, tok), 0) > iota((tok, tok), 1)).astype(F32).astype(BF16)
    rank = jnp.dot(tri, hit_b, preferred_element_type=F32)
    count = jnp.sum(hit32, axis=0, keepdims=True)
    row_e, col_e = iota((LANES, LANES), 0), iota((LANES, LANES), 1)
    e_loc = LANES // n_dev
    before = jnp.logical_and(row_e < col_e, row_e // e_loc == col_e // e_loc).astype(F32).astype(BF16)
    count8 = jnp.broadcast_to(count, (8, LANES))
    base = jnp.dot(count8.astype(BF16), before, preferred_element_type=F32)[0:1]
    pos_s[...] = jnp.where(hit, base + rank, -1.0)
    t_id = iota((tok, LANES), 0).astype(F32)
    lane_f = lane.astype(F32)

    @pl.when(c == 1)
    def _():
        own_sends()

    def pack(zd, _):
        for m in range(QUAD):
            tk = jnp.zeros((tok, LANES), F32)
            gt = jnp.zeros((tok, LANES), F32)
            for ee in range(e_loc):
                col = m * e_loc + ee
                at = pos_s[:, col:col + 1] == lane_f
                tk = jnp.where(at, t_id, tk)
                gt = jnp.where(at, p_s[:, col:col + 1], gt)
            packet[zd, m:m + 1, :] = jnp.sum(tk, axis=0, keepdims=True)
            packet[zd, QUAD + m:QUAD + m + 1, :] = jnp.sum(gt, axis=0, keepdims=True)
        packet[zd, 8:16, :] = count8
        pos_s[...] = pltpu.roll(pos_s[...], LANES - QUAD * e_loc, 1)
        p_s[...] = pltpu.roll(p_s[...], LANES - QUAD * e_loc, 1)
        return 0

    lax.fori_loop(0, PLANES, pack, 0)

    def route_copy(d):
        return remote(packet.at[d // QUAD], meta.at[me], send_m.at[d], recv_m.at[me], d)

    for d in range(n_dev):
        @pl.when(d != me)
        def _():
            route_copy(d).start()

    meta[me] = packet[z]

    def take(b, h, ways):
        hop(b, h, 3).wait_recv()
        out_copy(b, h).start()
        for way in ways:
            hop(b, h, way).start()

    def from_z(d, fn):
        @pl.when(z >= d)
        def _():
            fn(me - QUAD * d, 0, z < PLANES - 1)

        @pl.when(z + d < PLANES)
        def _():
            fn(me + QUAD * d, 1, z > 0)

    def across(zb):
        return zb * QUAD + (1 - y) * 2 + c

    def step_z(d):
        for h in range(2):
            def on(b, way, more):
                hop(b, h, 3).wait_recv()

                @pl.when(more)
                def _():
                    hop(b, h, way).start()

                hop(b, h, 2).start()
                hop(b, h, 3).start()
                out_copy(b, h).start()

            from_z(d, on)

    def step_y(d):
        for h in range(2):
            if d == 0:
                take(across(z), h, (3,))
            else:
                @pl.when(z >= d)
                def _():
                    take(across(z - d), h, (3,))

                @pl.when(z + d < PLANES)
                def _():
                    take(across(z + d), h, (3,))

    step_z(1)
    step_y(0)
    step_z(2)
    step_y(1)
    step_z(3)
    step_y(2)
    step_y(3)
    for b in range(n_dev):
        @pl.when(b % 2 != c)
        def _():
            for h in range(2):
                hop(b, h, 3).wait_recv()
                out_copy(b, h).start()

    for d in range(n_dev):
        @pl.when(d != me)
        def _():
            remote(packet.at[0], meta.at[d], send_m.at[d], recv_m.at[d], d).wait_recv()

    cnt = meta[:, 8, :]
    group = (iota((LANES, LANES), 0) // e_loc == iota((LANES, LANES), 1)).astype(F32).astype(BF16)
    n_rows = jnp.dot(cnt.astype(BF16), group, preferred_element_type=F32)
    ints[0:16, LANES:] = jnp.zeros((16, LANES), jnp.int32)
    ints[0:16, :LANES] = meta[:, pl.ds(q, 1), :].reshape(n_dev, LANES).astype(jnp.int32)
    ints[16:32, :LANES] = cnt.astype(jnp.int32)
    run = jnp.zeros((1, LANES), F32)
    for s in range(n_dev):
        off = run.astype(jnp.int32)
        ints[32 + s:33 + s, :LANES] = off
        ints[48 + s:49 + s, :LANES] = jnp.minimum(off // TILE, (r_max - WIN) // TILE)
        run = run + n_rows[s:s + 1]

    tail = [pltpu.make_async_copy(meta, meta_hbm, out_sem.at[0, 2]), pltpu.make_async_copy(ints, ints_hbm, out_sem.at[1, 2])]
    for cp in tail:
        cp.start()

    for h in range(2):
        def sent(b, way, more):
            @pl.when(more)
            def _():
                hop(b, h, way).wait_send()

            hop(b, h, 2).wait_send()
            hop(b, h, 3).wait_send()

        @pl.when(z < PLANES - 1)
        def _():
            hop(me, h, 0).wait_send()

        @pl.when(z > 0)
        def _():
            hop(me, h, 1).wait_send()

        hop(me, h, 2).wait_send()
        hop(me, h, 3).wait_send()
        for d in range(1, PLANES):
            from_z(d, sent)
        for zb in range(PLANES):
            hop(across(zb), h, 3).wait_send()
        for b in range(n_dev):
            out_copy(b, h).wait()
    for d in range(n_dev):
        @pl.when(d != me)
        def _():
            route_copy(d).wait_send()
    for cp in tail:
        cp.wait()


def spread(r_max, tokens, expert_ids, norm_gain, w_router):
    tok, width = tokens.shape
    n_dev = PLANES * QUAD
    sub = width // LANES
    hbm = pl.BlockSpec(memory_space=pltpu.HBM)
    vmem = pl.BlockSpec(memory_space=pltpu.VMEM)
    return pl.pallas_call(
        functools.partial(spread_kernel, r_max),
        out_shape=(jax.ShapeDtypeStruct((n_dev, tok * sub, LANES), BF16),
                   jax.ShapeDtypeStruct((n_dev, 16, LANES), F32),
                   jax.ShapeDtypeStruct((64, 2 * LANES), jnp.int32)),
        in_specs=[vmem] * 4,
        out_specs=(hbm, hbm, hbm),
        scratch_shapes=[
            pltpu.VMEM((n_dev, tok * sub, LANES), BF16),
            pltpu.VMEM((tok * sub, LANES), F32),
            pltpu.VMEM((tok, width), BF16),
            pltpu.VMEM((tok, LANES), F32),
            pltpu.VMEM((tok, LANES), F32),
            pltpu.VMEM((PLANES, 16, LANES), F32),
            pltpu.VMEM((n_dev, 16, LANES), F32),
            pltpu.VMEM((64, 2 * LANES), jnp.int32),
            pltpu.SemaphoreType.DMA((n_dev, 2, 4)),
            pltpu.SemaphoreType.DMA((n_dev, 2)),
            pltpu.SemaphoreType.DMA((n_dev,)),
            pltpu.SemaphoreType.DMA((n_dev,)),
            pltpu.SemaphoreType.DMA((n_dev, 3)),
        ],
        compiler_params=pltpu.CompilerParams(collective_id=0, has_side_effects=True, vmem_limit_bytes=66_000_000),
        name="spread",
    )(tokens, expert_ids.T, norm_gain.reshape(1, width), w_router)


def expert_kernel(n_src, sub, r_max, ints, meta, u_hbm, w1_hbm, w3_hbm, w2_hbm, o_hbm, win_hbm,
                  u_vm, o_all, xf, xb, hb, ob, win, w1, w3, w2, pre, sems, sem_w):
    n_exp = w1_hbm.shape[0]
    me, z, q = place()
    lane0 = me * n_exp

    def load(e, names):
        slot = lax.rem(e, 2)
        copies = []
        for i, (src, dst) in enumerate(((w1_hbm, w1), (w3_hbm, w3), (w2_hbm, w2))):
            if i in names:
                size = src.shape[1] // PIECES
                for p in range(PIECES):
                    part = pl.ds(p * size, size)
                    copies.append(pltpu.make_async_copy(src.at[e, part], dst.at[slot, part], sem_w.at[slot, i, p]))
        return copies

    def start(copies):
        for i, w in enumerate(copies):
            w.start(priority=i % 2)

    def begin():
        cp = pltpu.make_async_copy(u_hbm, u_vm, sems.at[0])
        cp.start()
        for e in range(2):
            start(load(e, (0, 1, 2)))
        for s in range(n_src):
            pre[s] = 0

        @pl.loop(0, r_max * PITCH // 256)
        def _(i):
            o_all[pl.ds(pl.multiple_of(i * 256, 256), 256), :] = jnp.zeros((256, LANES), F32)

        @pl.loop(0, n_src)
        def _(s):
            for m in range(QUAD):
                t = meta[s, m:m + 1, :]
                g = meta[s, QUAD + m:QUAD + m + 1, :]
                hi = g.astype(BF16).astype(F32)
                mid = (g - hi).astype(BF16).astype(F32)
                lo = (g - hi - mid).astype(BF16).astype(F32)
                rows = jnp.concatenate([t, hi, mid, lo, t, t, t, t], axis=0)
                rows = jnp.concatenate([rows, jnp.zeros((8, WIN - LANES), F32)], axis=1)
                r = z * QUAD + m
                win[s * QUAD + m] = pltpu.roll(rows, ints[32 + s, r] - TILE * ints[48 + s, r], 1)

        pltpu.make_async_copy(win, win_hbm, sems.at[1]).start()
        cp.wait()

    begin()

    def expert(e, _):
        slot = lax.rem(e, 2)
        def take(s, j0, n, i, at):
            t = s * LANES + ints[s, j0 + i]
            src = u_vm[pl.ds(pl.multiple_of(t * sub, sub), sub), :]
            xf[pl.ds(at * PITCH, sub), :] = src.astype(F32)

        def give(s, j0, n, i, at):
            o_all[pl.ds(at * PITCH, sub), :] = xf[pl.ds((n + i) * PITCH, sub), :]

        def sweep(body, target, spare):
            n = jnp.int32(0)
            top = jnp.int32(0)
            starts = []
            for s in range(n_src):
                cnt = ints[16 + s, lane0 + e]
                to = target(s, n)
                for i in range(STEP):
                    at = to + i if target is by_row else jnp.where(i < cnt, to + i, spare)
                    body(s, pre[s], n, i, at)
                starts.append(n)
                n = n + cnt
                top = jnp.maximum(top, cnt)
            for s in range(n_src):
                cnt = ints[16 + s, lane0 + e]

                @pl.when(cnt > STEP)
                def _():
                    to = target(s, starts[s])
                    for i in range(STEP, STEP + MORE):
                        body(s, pre[s], starts[s], i, jnp.where(i < cnt, to + i, spare))

            @pl.when(top > STEP + MORE)
            def _():
                def source(s, n):
                    cnt = ints[16 + s, lane0 + e]

                    def row(i, _):
                        body(s, pre[s], n, i, target(s, n) + i)
                        return 0

                    lax.fori_loop(STEP + MORE, cnt, row, 0)
                    return n + cnt

                lax.fori_loop(0, n_src, source, jnp.int32(0))

            return n

        def by_row(s, n):
            return n

        def by_slot(s, n):
            return ints[32 + s, me] + pre[s]

        n = sweep(take, by_row, r_max + 2 * STEP)

        for w in load(e, (0, 1, 2)):
            w.wait()

        def block(b, _):
            r0 = b * (BM * PITCH)
            for j in range(sub):
                xb[:, j * LANES:(j + 1) * LANES] = xf[pl.ds(r0 + j, BM, stride=PITCH), :].astype(BF16)
            g = jnp.dot(xb[...], w1[slot], preferred_element_type=F32)
            v = jnp.dot(xb[...], w3[slot], preferred_element_type=F32)
            hb[...] = (jax.nn.silu(g) * v).astype(BF16)
            for k in range(sub // 4):
                o = jnp.dot(hb[...], w2[slot, :, k * 512:(k + 1) * 512], preferred_element_type=F32)
                for j in range(4):
                    xf[pl.ds(r0 + k * 4 + j, BM, stride=PITCH), :] = o[:, j * LANES:(j + 1) * LANES]
            return 0

        lax.fori_loop(0, (n + BM - 1) // BM, block, 0)

        sweep(give, by_slot, r_max)
        for s in range(n_src):
            pre[s] = pre[s] + ints[16 + s, lane0 + e]

        @pl.when(e + 2 < n_exp)
        def _():
            start(load(e + 2, (0, 1, 2)))

        return 0

    lax.fori_loop(0, n_exp, expert, 0)

    def put(j):
        return pltpu.make_async_copy(ob.at[j % 4], o_hbm.at[j], sems.at[2 + j % 4])

    for j in range(sub):
        if j >= 4:
            put(j - 4).wait()
        ob[j % 4] = o_all[pl.ds(j, r_max, stride=PITCH), :].astype(BF16)
        put(j).start()
    for j in range(sub - 4, sub):
        put(j).wait()
    pltpu.make_async_copy(win, win_hbm, sems.at[1]).wait()


def experts(n_src, r_max, ints, meta, u_rows, w1, w3, w2):
    n_exp, width, ff = w1.shape
    sub = width // LANES
    n_tok = u_rows.shape[0] // sub
    hbm = pl.BlockSpec(memory_space=pltpu.HBM)
    smem = pl.BlockSpec(memory_space=pltpu.SMEM)
    return pl.pallas_call(
        functools.partial(expert_kernel, n_src, sub, r_max),
        out_shape=(jax.ShapeDtypeStruct((sub, r_max, LANES), BF16),
                   jax.ShapeDtypeStruct((n_src * QUAD, 8, WIN), F32)),
        in_specs=[smem, pl.BlockSpec(memory_space=pltpu.VMEM), hbm, hbm, hbm, hbm],
        out_specs=(hbm, hbm),
        scratch_shapes=[
            pltpu.VMEM((n_tok * sub, LANES), BF16),
            pltpu.VMEM(((r_max + 8) * PITCH, LANES), F32),
            pltpu.VMEM(((r_max + 2 * STEP + 8) * PITCH, LANES), F32),
            pltpu.VMEM((BM, width), BF16),
            pltpu.VMEM((BM, ff), BF16),
            pltpu.VMEM((4, r_max, LANES), BF16),
            pltpu.VMEM((n_src * QUAD, 8, WIN), F32),
            pltpu.VMEM((2, width, ff), BF16),
            pltpu.VMEM((2, width, ff), BF16),
            pltpu.VMEM((2, ff, width), BF16),
            pltpu.SMEM((n_src,), jnp.int32),
            pltpu.SemaphoreType.DMA((6,)),
            pltpu.SemaphoreType.DMA((2, 3, PIECES)),
        ],
        compiler_params=pltpu.CompilerParams(vmem_limit_bytes=66_000_000),
        name="experts",
    )(ints, meta, u_rows, w1, w3, w2)


def collect_kernel(n_src, steps, ints, win, x_ref, o_hbm, out_ref,
                   mix, part, from_l, from_r, fin,
                   send_q, recv_q, send_z, recv_l, recv_r, send_f, recv_f, stage, stage_sem, *rows):
    me, z, q = place()
    y, c = q // 2, lax.rem(q, 2)
    tok = x_ref.shape[0]
    plane = QUAD * tok
    others = ((1 - y) * 2 + c, (1 - y) * 2 + 1 - c, y * 2 + 1 - c)

    barrier = pltpu.get_barrier_semaphore()

    def hello(dev):
        pl.semaphore_signal(barrier, inc=1, device_id={'ep': dev}, device_id_type=pl.DeviceIdType.MESH)

    def stage_copy(k, m):
        return pltpu.make_async_copy(o_hbm.at[m * steps + k], stage.at[k, m], stage_sem.at[k, m])

    def own_copy(k):
        return pltpu.make_async_copy(o_hbm.at[q * steps + k], rows[k].at[q], recv_q.at[k, q])

    for k in range(steps):
        for m in others:
            stage_copy(k, m).start()
        own_copy(k).start()

    for m in others:
        hello(z * QUAD + m)

    @pl.when(z > 0)
    def _():
        hello(me - QUAD)

    @pl.when(z < PLANES - 1)
    def _():
        hello(me + QUAD)

    pl.semaphore_wait(barrier, 4 + (z + PLANES - 1) // PLANES - (z + 1) // PLANES)

    def quad_copy(k, m):
        return remote(stage.at[k, m], rows[k].at[q], send_q.at[k, m], recv_q.at[k, q], z * QUAD + m)

    def quad_wait(k, m):
        remote(stage.at[k, m], rows[k].at[m], send_q.at[k, m], recv_q.at[k, m], z * QUAD + m).wait_recv()

    def quad_sends():
        for k in range(steps):
            for m in others:
                stage_copy(k, m).wait()
                quad_copy(k, m).start()

    @pl.when(c == 0)
    def _():
        quad_sends()

    row_id = iota((tok, WIN), 0).astype(F32)

    def build(i, _):
        w = win[i]
        at = w[0:1] == row_id
        for part_i in range(3):
            mix[i, part_i * tok:(part_i + 1) * tok, :] = jnp.where(at, w[1 + part_i:2 + part_i], 0.0).astype(BF16)
        return 0

    lax.fori_loop(0, n_src * QUAD, build, 0)

    @pl.when(c == 1)
    def _():
        quad_sends()

    def right(k, zd, h, n):
        rows_h = pl.ds(h * (plane // n), plane // n)
        return remote(part.at[k, zd, rows_h], from_l.at[k, zd, rows_h], send_z.at[k, zd, h], recv_l.at[k, zd, h], me + QUAD)

    def left(k, zd, h, n):
        rows_h = pl.ds(h * (plane // n), plane // n)
        return remote(part.at[k, zd, rows_h], from_r.at[k, zd, rows_h], send_z.at[k, zd, h], recv_r.at[k, zd, h], me - QUAD)

    def cut(k, farthest, body):
        if k == 0 and farthest:
            @pl.when(c == 0)
            def _():
                body(1)

            @pl.when(c == 1)
            def _():
                body(2)
        else:
            body(1)

    def combine(k):
        own_copy(k).wait()
        for m in others:
            quad_wait(k, m)

        def token_block(s):
            acc = jnp.zeros((3 * tok, LANES), F32)
            for m in range(QUAD):
                start = ints[48 + s, z * QUAD + m]
                span = jnp.concatenate([rows[k][m, start + i] for i in range(WIN // TILE)], axis=0)
                acc += jnp.dot(mix[s * QUAD + m], span, preferred_element_type=F32)
            part[k, s // QUAD, pl.ds(pl.multiple_of(lax.rem(s, QUAD) * tok, tok), tok), :] = acc[0:tok] + acc[tok:2 * tok] + acc[2 * tok:]

        def one_plane(i, _):
            zd = (PLANES - 1 - i) * (1 - z // 2) + i * (z // 2)

            def one_block(m, _):
                token_block(zd * QUAD + m)
                return 0

            lax.fori_loop(0, QUAD, one_block, 0)

            for j in range(PLANES - 1):
                @pl.when(i == j)
                def _():
                    def to_right(n):
                        for h in range(n):
                            right(k, PLANES - 1 - j, h, n).start()

                    def to_left(n):
                        for h in range(n):
                            left(k, j, h, n).start()

                    @pl.when(z == 0)
                    def _():
                        cut(k, j == 0, to_right)

                    @pl.when(z == PLANES - 1)
                    def _():
                        cut(k, j == 0, to_left)

            return 0

        lax.fori_loop(0, PLANES, one_plane, 0)

    def forward(k):
        for i in range(PLANES - 1):
            for to_right in (True, False):
                zd = PLANES - 1 - i if to_right else i
                box = from_l if to_right else from_r
                go = right if to_right else left

                def relay(n):
                    for h in range(n):
                        rows_h = pl.ds(h * (plane // n), plane // n)
                        go(k, zd, h, n).wait_recv()
                        part[k, zd, rows_h] += box[k, zd, rows_h]
                        go(k, zd, h, n).start()

                @pl.when(z < zd if to_right else z > zd)
                def _():
                    @pl.when(z > 0 if to_right else z < PLANES - 1)
                    def _():
                        cut(k, i == 0, relay)

    def final_copy(k, m):
        src = part.at[k, z, pl.ds(m * tok, tok)]
        return remote(src, fin.at[k, q], send_f.at[k, m], recv_f.at[k, q], z * QUAD + m)

    def finish(k):
        for zd in range(PLANES):
            @pl.when(z == zd)
            def _():
                def from_left(n):
                    for h in range(n):
                        right(k, zd, h, n).wait_recv()

                def from_right(n):
                    for h in range(n):
                        left(k, zd, h, n).wait_recv()

                if zd > 0:
                    cut(k, zd == PLANES - 1, from_left)
                    part[k, zd] += from_l[k, zd]
                if zd < PLANES - 1:
                    cut(k, zd == 0, from_right)
                    part[k, zd] += from_r[k, zd]

        for m in others:
            final_copy(k, m).start()
        fin[k, q] = part[k, z, pl.ds(pl.multiple_of(q * tok, tok), tok), :]

    for k in range(steps):
        combine(k)
        forward(k)
        if k > 0:
            finish(k - 1)
    finish(steps - 1)

    for k in range(steps):
        for m in others:
            remote(part.at[k, z, pl.ds(0, tok)], fin.at[k, m], send_f.at[k, m], recv_f.at[k, m], z * QUAD + m).wait_recv()
        for m in range(QUAD):
            cols = pl.ds((m * steps + k) * LANES, LANES)
            out_ref[:, cols] = (x_ref[:, cols].astype(F32) + fin[k, m]).astype(BF16)

    for k in range(steps):
        for m in others:
            quad_copy(k, m).wait_send()
            final_copy(k, m).wait_send()
        for zd in range(PLANES):
            @pl.when(z < zd)
            def _():
                def done(n):
                    for h in range(n):
                        right(k, zd, h, n).wait_send()

                cut(k, zd == PLANES - 1, done)

            @pl.when(z > zd)
            def _():
                def done(n):
                    for h in range(n):
                        left(k, zd, h, n).wait_send()

                cut(k, zd == 0, done)


def collect(ints, win, tokens, o_rows):
    tok, width = tokens.shape
    sub, r_tiles = o_rows.shape[:2]
    n_src = PLANES * QUAD
    steps = sub // QUAD
    vmem = pl.BlockSpec(memory_space=pltpu.VMEM)
    return pl.pallas_call(
        functools.partial(collect_kernel, n_src, steps),
        out_shape=jax.ShapeDtypeStruct((tok, width), BF16),
        in_specs=[pl.BlockSpec(memory_space=pltpu.SMEM), vmem, vmem, pl.BlockSpec(memory_space=pltpu.HBM)],
        out_specs=vmem,
        scratch_shapes=[
            pltpu.VMEM((n_src * QUAD, 3 * tok, WIN), BF16),
            pltpu.VMEM((steps, PLANES, QUAD * tok, LANES), F32),
            pltpu.VMEM((steps, PLANES, QUAD * tok, LANES), F32),
            pltpu.VMEM((steps, PLANES, QUAD * tok, LANES), F32),
            pltpu.VMEM((steps, QUAD, tok, LANES), F32),
            pltpu.SemaphoreType.DMA((steps, QUAD)),
            pltpu.SemaphoreType.DMA((steps, QUAD)),
            pltpu.SemaphoreType.DMA((steps, PLANES, CUTS)),
            pltpu.SemaphoreType.DMA((steps, PLANES, CUTS)),
            pltpu.SemaphoreType.DMA((steps, PLANES, CUTS)),
            pltpu.SemaphoreType.DMA((steps, QUAD)),
            pltpu.SemaphoreType.DMA((steps, QUAD)),
            pltpu.VMEM((steps, QUAD, r_tiles, TILE, LANES), BF16),
            pltpu.SemaphoreType.DMA((steps, QUAD)),
        ] + [pltpu.VMEM((QUAD, r_tiles, TILE, LANES), BF16)] * steps,
        compiler_params=pltpu.CompilerParams(collective_id=1, has_side_effects=True, vmem_limit_bytes=56 * 2 ** 20),
        name="collect",
    )(ints, win, tokens, o_rows)


def solution(mesh):
    ep_size = mesh.shape['ep']

    def device_step(tokens, expert_ids, norm_gain, w_router, w_gate, w_up, w_down):
        pairs = expert_ids.shape[0] * expert_ids.shape[1]
        r_max = 3 * pairs // 2
        u_rows, meta, ints = spread(r_max, tokens, expert_ids, norm_gain, w_router)
        u_rows = u_rows.reshape(-1, LANES)
        o_rows, win = experts(ep_size, r_max, ints, meta, u_rows, w_gate, w_up, w_down)
        return collect(ints, win, tokens, o_rows.reshape(-1, r_max // TILE, TILE, LANES))

    row_spec = P(('dp', 'ep'), None)
    expert_spec = P('ep', None, None)
    return jax.shard_map(device_step, mesh=mesh, in_specs=(row_spec, row_spec, P(None), P(None, None), expert_spec, expert_spec, expert_spec), out_specs=row_spec, check_vma=False)
```

```python
import functools

import jax
import jax.numpy as jnp
from jax import lax
from jax.experimental import pallas as pl
from jax.experimental.pallas import tpu as pltpu
from jax.sharding import PartitionSpec as P

NORM_EPS = 1e-5
LANES = 128
BM = 128
WIN = 256
CUTS = 2
TILE = 16
PITCH = 17
STEP = 8
MORE = 8
PIECES = 4
QUAD = 4
PLANES = 4
F32 = jnp.float32
BF16 = jnp.bfloat16


def iota(shape, dim):
    return lax.broadcasted_iota(jnp.int32, shape, dim)


def place():
    me = lax.axis_index('ep')
    return me, me // QUAD, lax.rem(me, QUAD)


def remote(src, dst, send, recv, dev):
    return pltpu.make_async_remote_copy(src_ref=src, dst_ref=dst, send_sem=send, recv_sem=recv,
                                        device_id={'ep': dev}, device_id_type=pl.DeviceIdType.MESH)


def spread_kernel(r_max, x_ref, ids_ref, gain_ref, wr_ref, u_hbm, meta_hbm, ints_hbm,
                  u_all, xs, ub, pos_s, p_s, packet, meta, ints,
                  send_u, recv_u, send_m, recv_m, out_sem):
    n_dev = PLANES * QUAD
    me, z, q = place()
    y, c = q // 2, lax.rem(q, 2)
    half = u_all.shape[1] // 2
    tok = x_ref.shape[0]
    sub = u_all.shape[1] // tok

    barrier = pltpu.get_barrier_semaphore()
    for d in range(1, n_dev):
        pl.semaphore_signal(barrier, inc=1, device_id={'ep': lax.rem(me + d, n_dev)}, device_id_type=pl.DeviceIdType.MESH)

    x32 = x_ref[...].astype(F32)
    inv = lax.rsqrt(jnp.mean(x32 * x32, axis=1, keepdims=True) + NORM_EPS)
    ub[...] = (x32 * inv * gain_ref[...].astype(F32)).astype(BF16)
    for j in range(sub):
        xs[pl.ds(j, tok, stride=sub), :] = ub[:, j * LANES:(j + 1) * LANES].astype(F32)
    u_all[me] = xs[...].astype(BF16)
    pl.semaphore_wait(barrier, n_dev - 1)

    dest = (me + QUAD, me - QUAD, z * QUAD + (1 - y) * 2 + c, z * QUAD + y * 2 + 1 - c)

    def hop(b, h, way):
        rows = u_all.at[b, pl.ds(h * half, half)]
        return remote(rows, rows, send_u.at[b, h, way], recv_u.at[b, h], dest[way])

    def out_copy(b, h):
        rows = pl.ds(h * half, half)
        return pltpu.make_async_copy(u_all.at[b, rows], u_hbm.at[b, rows], out_sem.at[b, h])

    def own_sends():
        for h in range(2):
            @pl.when(z < PLANES - 1)
            def _():
                hop(me, h, 0).start()

            @pl.when(z > 0)
            def _():
                hop(me, h, 1).start()

            hop(me, h, 2).start()
            hop(me, h, 3).start()
            out_copy(me, h).start()

    @pl.when(c == 0)
    def _():
        own_sends()

    logits = jnp.dot(ub[...], wr_ref[...], preferred_element_type=F32)
    top = jnp.max(logits, axis=1, keepdims=True)
    ex = jnp.exp(logits - top)
    p_s[...] = ex / jnp.sum(ex, axis=1, keepdims=True)
    lane = iota((tok, LANES), 1)
    hit = lane < 0
    ids = ids_ref[...].T
    for k in range(ids.shape[1]):
        hit = jnp.logical_or(hit, ids[:, k:k + 1] == lane)
    hit32 = hit.astype(F32)
    hit_b = hit32.astype(BF16)
    tri = (iota((tok, tok), 0) > iota((tok, tok), 1)).astype(F32).astype(BF16)
    rank = jnp.dot(tri, hit_b, preferred_element_type=F32)
    count = jnp.sum(hit32, axis=0, keepdims=True)
    row_e, col_e = iota((LANES, LANES), 0), iota((LANES, LANES), 1)
    e_loc = LANES // n_dev
    before = jnp.logical_and(row_e < col_e, row_e // e_loc == col_e // e_loc).astype(F32).astype(BF16)
    count8 = jnp.broadcast_to(count, (8, LANES))
    base = jnp.dot(count8.astype(BF16), before, preferred_element_type=F32)[0:1]
    pos_s[...] = jnp.where(hit, base + rank, -1.0)
    t_id = iota((tok, LANES), 0).astype(F32)
    lane_f = lane.astype(F32)

    @pl.when(c == 1)
    def _():
        own_sends()

    def pack(zd, _):
        for m in range(QUAD):
            tk = jnp.zeros((tok, LANES), F32)
            gt = jnp.zeros((tok, LANES), F32)
            for ee in range(e_loc):
                col = m * e_loc + ee
                at = pos_s[:, col:col + 1] == lane_f
                tk = jnp.where(at, t_id, tk)
                gt = jnp.where(at, p_s[:, col:col + 1], gt)
            packet[zd, m:m + 1, :] = jnp.sum(tk, axis=0, keepdims=True)
            packet[zd, QUAD + m:QUAD + m + 1, :] = jnp.sum(gt, axis=0, keepdims=True)
        packet[zd, 8:16, :] = count8
        pos_s[...] = pltpu.roll(pos_s[...], LANES - QUAD * e_loc, 1)
        p_s[...] = pltpu.roll(p_s[...], LANES - QUAD * e_loc, 1)
        return 0

    lax.fori_loop(0, PLANES, pack, 0)

    def route_copy(d):
        return remote(packet.at[d // QUAD], meta.at[me], send_m.at[d], recv_m.at[me], d)

    for d in range(n_dev):
        @pl.when(d != me)
        def _():
            route_copy(d).start()

    meta[me] = packet[z]

    def take(b, h, ways):
        hop(b, h, 3).wait_recv()
        out_copy(b, h).start()
        for way in ways:
            hop(b, h, way).start()

    def from_z(d, fn):
        @pl.when(z >= d)
        def _():
            fn(me - QUAD * d, 0, z < PLANES - 1)

        @pl.when(z + d < PLANES)
        def _():
            fn(me + QUAD * d, 1, z > 0)

    def across(zb):
        return zb * QUAD + (1 - y) * 2 + c

    def step_z(d):
        for h in range(2):
            def on(b, way, more):
                hop(b, h, 3).wait_recv()

                @pl.when(more)
                def _():
                    hop(b, h, way).start()

                hop(b, h, 2).start()
                hop(b, h, 3).start()
                out_copy(b, h).start()

            from_z(d, on)

    def step_y(d):
        for h in range(2):
            if d == 0:
                take(across(z), h, (3,))
            else:
                @pl.when(z >= d)
                def _():
                    take(across(z - d), h, (3,))

                @pl.when(z + d < PLANES)
                def _():
                    take(across(z + d), h, (3,))

    step_z(1)
    step_y(0)
    step_z(2)
    step_y(1)
    step_z(3)
    step_y(2)
    step_y(3)
    for b in range(n_dev):
        @pl.when(b % 2 != c)
        def _():
            for h in range(2):
                hop(b, h, 3).wait_recv()
                out_copy(b, h).start()

    for d in range(n_dev):
        @pl.when(d != me)
        def _():
            remote(packet.at[0], meta.at[d], send_m.at[d], recv_m.at[d], d).wait_recv()

    cnt = meta[:, 8, :]
    group = (iota((LANES, LANES), 0) // e_loc == iota((LANES, LANES), 1)).astype(F32).astype(BF16)
    n_rows = jnp.dot(cnt.astype(BF16), group, preferred_element_type=F32)
    ints[0:16, LANES:] = jnp.zeros((16, LANES), jnp.int32)
    ints[0:16, :LANES] = (meta[:, pl.ds(q, 1), :].reshape(n_dev, LANES).astype(jnp.int32) + iota((n_dev, LANES), 0) * tok) * sub
    ints[16:32, :LANES] = cnt.astype(jnp.int32)
    run = jnp.zeros((1, LANES), F32)
    for s in range(n_dev):
        off = run.astype(jnp.int32)
        ints[32 + s:33 + s, :LANES] = off
        ints[48 + s:49 + s, :LANES] = jnp.minimum(off // TILE, (r_max - WIN) // TILE)
        run = run + n_rows[s:s + 1]

    tail = [pltpu.make_async_copy(meta, meta_hbm, out_sem.at[0, 2]), pltpu.make_async_copy(ints, ints_hbm, out_sem.at[1, 2])]
    for cp in tail:
        cp.start()

    for h in range(2):
        def sent(b, way, more):
            @pl.when(more)
            def _():
                hop(b, h, way).wait_send()

            hop(b, h, 2).wait_send()
            hop(b, h, 3).wait_send()

        @pl.when(z < PLANES - 1)
        def _():
            hop(me, h, 0).wait_send()

        @pl.when(z > 0)
        def _():
            hop(me, h, 1).wait_send()

        hop(me, h, 2).wait_send()
        hop(me, h, 3).wait_send()
        for d in range(1, PLANES):
            from_z(d, sent)
        for zb in range(PLANES):
            hop(across(zb), h, 3).wait_send()
        for b in range(n_dev):
            out_copy(b, h).wait()
    for d in range(n_dev):
        @pl.when(d != me)
        def _():
            route_copy(d).wait_send()
    for cp in tail:
        cp.wait()


def spread(r_max, tokens, expert_ids, norm_gain, w_router):
    tok, width = tokens.shape
    n_dev = PLANES * QUAD
    sub = width // LANES
    hbm = pl.BlockSpec(memory_space=pltpu.HBM)
    vmem = pl.BlockSpec(memory_space=pltpu.VMEM)
    return pl.pallas_call(
        functools.partial(spread_kernel, r_max),
        out_shape=(jax.ShapeDtypeStruct((n_dev, tok * sub, LANES), BF16),
                   jax.ShapeDtypeStruct((n_dev, 16, LANES), F32),
                   jax.ShapeDtypeStruct((64, 2 * LANES), jnp.int32)),
        in_specs=[vmem] * 4,
        out_specs=(hbm, hbm, hbm),
        scratch_shapes=[
            pltpu.VMEM((n_dev, tok * sub, LANES), BF16),
            pltpu.VMEM((tok * sub, LANES), F32),
            pltpu.VMEM((tok, width), BF16),
            pltpu.VMEM((tok, LANES), F32),
            pltpu.VMEM((tok, LANES), F32),
            pltpu.VMEM((PLANES, 16, LANES), F32),
            pltpu.VMEM((n_dev, 16, LANES), F32),
            pltpu.VMEM((64, 2 * LANES), jnp.int32),
            pltpu.SemaphoreType.DMA((n_dev, 2, 4)),
            pltpu.SemaphoreType.DMA((n_dev, 2)),
            pltpu.SemaphoreType.DMA((n_dev,)),
            pltpu.SemaphoreType.DMA((n_dev,)),
            pltpu.SemaphoreType.DMA((n_dev, 3)),
        ],
        compiler_params=pltpu.CompilerParams(collective_id=0, has_side_effects=True, vmem_limit_bytes=66_000_000),
        name="spread",
    )(tokens, expert_ids.T, norm_gain.reshape(1, width), w_router)


def expert_kernel(n_src, sub, r_max, ints, meta, u_hbm, w1_hbm, w3_hbm, w2_hbm, o_hbm, win_hbm,
                  u_vm, o_all, xf, xb, hb, ob, win, w1, w3, w2, pre, sems, sem_w):
    n_exp = w1_hbm.shape[0]
    me, z, q = place()
    lane0 = me * n_exp

    def load(e, names):
        slot = lax.rem(e, 2)
        copies = []
        for i, (src, dst) in enumerate(((w1_hbm, w1), (w3_hbm, w3), (w2_hbm, w2))):
            if i in names:
                size = src.shape[1] // PIECES
                for p in range(PIECES):
                    part = pl.ds(p * size, size)
                    copies.append(pltpu.make_async_copy(src.at[e, part], dst.at[slot, part], sem_w.at[slot, i, p]))
        return copies

    def start(copies):
        for i, w in enumerate(copies):
            w.start(priority=i % 2)

    def begin():
        cp = pltpu.make_async_copy(u_hbm, u_vm, sems.at[0])
        cp.start()
        for e in range(2):
            start(load(e, (0, 1, 2)))
        for s in range(n_src):
            pre[s] = 0

        @pl.loop(0, r_max * PITCH // 256)
        def _(i):
            o_all[pl.ds(pl.multiple_of(i * 256, 256), 256), :] = jnp.zeros((256, LANES), F32)

        @pl.loop(0, n_src)
        def _(s):
            for m in range(QUAD):
                t = meta[s, m:m + 1, :]
                g = meta[s, QUAD + m:QUAD + m + 1, :]
                hi = g.astype(BF16).astype(F32)
                mid = (g - hi).astype(BF16).astype(F32)
                lo = (g - hi - mid).astype(BF16).astype(F32)
                rows = jnp.concatenate([t, hi, mid, lo, t, t, t, t], axis=0)
                rows = jnp.concatenate([rows, jnp.zeros((8, WIN - LANES), F32)], axis=1)
                r = z * QUAD + m
                win[s * QUAD + m] = pltpu.roll(rows, ints[32 + s, r] - TILE * ints[48 + s, r], 1)

        pltpu.make_async_copy(win, win_hbm, sems.at[1]).start()
        cp.wait()

    begin()

    def expert(e, _):
        slot = lax.rem(e, 2)
        def take(s, j0, n, i, at):
            src = u_vm[pl.ds(pl.multiple_of(ints[s, j0 + i], sub), sub), :]
            xf[pl.ds(at, sub), :] = src.astype(F32)

        def give(s, j0, n, i, at):
            o_all[pl.ds(at, sub), :] = xf[pl.ds(n + i * PITCH, sub), :]

        def sweep(body, target, spare):
            n = jnp.int32(0)
            top = jnp.int32(0)
            starts = []
            for s in range(n_src):
                cnt = ints[16 + s, lane0 + e]
                to = target(s, n)
                for i in range(STEP):
                    at = to + i * PITCH if target is by_row else jnp.where(i < cnt, to + i * PITCH, spare)
                    body(s, pre[s], n, i, at)
                starts.append(n)
                n = n + cnt * PITCH
                top = jnp.maximum(top, cnt)
            for s in range(n_src):
                cnt = ints[16 + s, lane0 + e]

                @pl.when(cnt > STEP)
                def _():
                    to = target(s, starts[s])
                    for i in range(STEP, STEP + MORE):
                        body(s, pre[s], starts[s], i, jnp.where(i < cnt, to + i * PITCH, spare))

            @pl.when(top > STEP + MORE)
            def _():
                def source(s, n):
                    cnt = ints[16 + s, lane0 + e]

                    def row(i, _):
                        body(s, pre[s], n, i, target(s, n) + i * PITCH)
                        return 0

                    lax.fori_loop(STEP + MORE, cnt, row, 0)
                    return n + cnt * PITCH

                lax.fori_loop(0, n_src, source, jnp.int32(0))

            return n

        def by_row(s, n):
            return n

        def by_slot(s, n):
            return (ints[32 + s, me] + pre[s]) * PITCH

        n = sweep(take, by_row, (r_max + 2 * STEP) * PITCH)

        for w in load(e, (0, 1, 2)):
            w.wait()

        def block(b, _):
            r0 = b * (BM * PITCH)
            for j in range(sub):
                xb[:, j * LANES:(j + 1) * LANES] = xf[pl.ds(r0 + j, BM, stride=PITCH), :].astype(BF16)
            g = jnp.dot(xb[...], w1[slot], preferred_element_type=F32)
            v = jnp.dot(xb[...], w3[slot], preferred_element_type=F32)
            hb[...] = (jax.nn.silu(g) * v).astype(BF16)
            for k in range(sub // 4):
                o = jnp.dot(hb[...], w2[slot, :, k * 512:(k + 1) * 512], preferred_element_type=F32)
                for j in range(4):
                    xf[pl.ds(r0 + k * 4 + j, BM, stride=PITCH), :] = o[:, j * LANES:(j + 1) * LANES]
            return 0

        lax.fori_loop(0, (n + BM * PITCH - 1) // (BM * PITCH), block, 0)

        sweep(give, by_slot, r_max * PITCH)
        for s in range(n_src):
            pre[s] = pre[s] + ints[16 + s, lane0 + e]

        @pl.when(e + 2 < n_exp)
        def _():
            start(load(e + 2, (0, 1, 2)))

        return 0

    lax.fori_loop(0, n_exp, expert, 0)

    def put(j):
        return pltpu.make_async_copy(ob.at[j % 4], o_hbm.at[j], sems.at[2 + j % 4])

    for j in range(sub):
        if j >= 4:
            put(j - 4).wait()
        ob[j % 4] = o_all[pl.ds(j, r_max, stride=PITCH), :].astype(BF16)
        put(j).start()
    for j in range(sub - 4, sub):
        put(j).wait()
    pltpu.make_async_copy(win, win_hbm, sems.at[1]).wait()


def experts(n_src, r_max, ints, meta, u_rows, w1, w3, w2):
    n_exp, width, ff = w1.shape
    sub = width // LANES
    n_tok = u_rows.shape[0] // sub
    hbm = pl.BlockSpec(memory_space=pltpu.HBM)
    smem = pl.BlockSpec(memory_space=pltpu.SMEM)
    return pl.pallas_call(
        functools.partial(expert_kernel, n_src, sub, r_max),
        out_shape=(jax.ShapeDtypeStruct((sub, r_max, LANES), BF16),
                   jax.ShapeDtypeStruct((n_src * QUAD, 8, WIN), F32)),
        in_specs=[smem, pl.BlockSpec(memory_space=pltpu.VMEM), hbm, hbm, hbm, hbm],
        out_specs=(hbm, hbm),
        scratch_shapes=[
            pltpu.VMEM((n_tok * sub, LANES), BF16),
            pltpu.VMEM(((r_max + 8) * PITCH, LANES), F32),
            pltpu.VMEM(((r_max + 2 * STEP + 8) * PITCH, LANES), F32),
            pltpu.VMEM((BM, width), BF16),
            pltpu.VMEM((BM, ff), BF16),
            pltpu.VMEM((4, r_max, LANES), BF16),
            pltpu.VMEM((n_src * QUAD, 8, WIN), F32),
            pltpu.VMEM((2, width, ff), BF16),
            pltpu.VMEM((2, width, ff), BF16),
            pltpu.VMEM((2, ff, width), BF16),
            pltpu.SMEM((n_src,), jnp.int32),
            pltpu.SemaphoreType.DMA((6,)),
            pltpu.SemaphoreType.DMA((2, 3, PIECES)),
        ],
        compiler_params=pltpu.CompilerParams(vmem_limit_bytes=66_000_000),
        name="experts",
    )(ints, meta, u_rows, w1, w3, w2)


def collect_kernel(n_src, steps, ints, win, x_ref, o_hbm, out_ref,
                   mix, part, from_l, from_r, fin,
                   send_q, recv_q, send_z, recv_l, recv_r, send_f, recv_f, stage, stage_sem, *rows):
    me, z, q = place()
    y, c = q // 2, lax.rem(q, 2)
    tok = x_ref.shape[0]
    plane = QUAD * tok
    others = ((1 - y) * 2 + c, (1 - y) * 2 + 1 - c, y * 2 + 1 - c)

    barrier = pltpu.get_barrier_semaphore()

    def hello(dev):
        pl.semaphore_signal(barrier, inc=1, device_id={'ep': dev}, device_id_type=pl.DeviceIdType.MESH)

    def stage_copy(k, m):
        return pltpu.make_async_copy(o_hbm.at[m * steps + k], stage.at[k, m], stage_sem.at[k, m])

    def own_copy(k):
        return pltpu.make_async_copy(o_hbm.at[q * steps + k], rows[k].at[q], recv_q.at[k, q])

    for k in range(steps):
        for m in others:
            stage_copy(k, m).start()
        own_copy(k).start()

    for m in others:
        hello(z * QUAD + m)

    @pl.when(z > 0)
    def _():
        hello(me - QUAD)

    @pl.when(z < PLANES - 1)
    def _():
        hello(me + QUAD)

    pl.semaphore_wait(barrier, 4 + (z + PLANES - 1) // PLANES - (z + 1) // PLANES)

    def quad_copy(k, m):
        return remote(stage.at[k, m], rows[k].at[q], send_q.at[k, m], recv_q.at[k, q], z * QUAD + m)

    def quad_wait(k, m):
        remote(stage.at[k, m], rows[k].at[m], send_q.at[k, m], recv_q.at[k, m], z * QUAD + m).wait_recv()

    def quad_sends():
        for k in range(steps):
            for m in others:
                stage_copy(k, m).wait()
                quad_copy(k, m).start()

    @pl.when(c == 0)
    def _():
        quad_sends()

    row_id = iota((tok, WIN), 0).astype(F32)

    def build(i, _):
        w = win[i]
        at = w[0:1] == row_id
        for part_i in range(3):
            mix[i, part_i * tok:(part_i + 1) * tok, :] = jnp.where(at, w[1 + part_i:2 + part_i], 0.0).astype(BF16)
        return 0

    lax.fori_loop(0, n_src * QUAD, build, 0)

    @pl.when(c == 1)
    def _():
        quad_sends()

    def right(k, zd, h, n):
        rows_h = pl.ds(h * (plane // n), plane // n)
        return remote(part.at[k, zd, rows_h], from_l.at[k, zd, rows_h], send_z.at[k, zd, h], recv_l.at[k, zd, h], me + QUAD)

    def left(k, zd, h, n):
        rows_h = pl.ds(h * (plane // n), plane // n)
        return remote(part.at[k, zd, rows_h], from_r.at[k, zd, rows_h], send_z.at[k, zd, h], recv_r.at[k, zd, h], me - QUAD)

    def cut(k, farthest, body):
        if k == 0 and farthest:
            @pl.when(c == 0)
            def _():
                body(1)

            @pl.when(c == 1)
            def _():
                body(2)
        else:
            body(1)

    def combine(k):
        own_copy(k).wait()
        for m in others:
            quad_wait(k, m)

        def token_block(s):
            acc = jnp.zeros((3 * tok, LANES), F32)
            for m in range(QUAD):
                start = ints[48 + s, z * QUAD + m]
                span = jnp.concatenate([rows[k][m, start + i] for i in range(WIN // TILE)], axis=0)
                acc += jnp.dot(mix[s * QUAD + m], span, preferred_element_type=F32)
            part[k, s // QUAD, pl.ds(pl.multiple_of(lax.rem(s, QUAD) * tok, tok), tok), :] = acc[0:tok] + acc[tok:2 * tok] + acc[2 * tok:]

        def one_plane(i, _):
            zd = (PLANES - 1 - i) * (1 - z // 2) + i * (z // 2)

            def one_block(m, _):
                token_block(zd * QUAD + m)
                return 0

            lax.fori_loop(0, QUAD, one_block, 0)

            for j in range(PLANES - 1):
                @pl.when(i == j)
                def _():
                    def to_right(n):
                        for h in range(n):
                            right(k, PLANES - 1 - j, h, n).start()

                    def to_left(n):
                        for h in range(n):
                            left(k, j, h, n).start()

                    @pl.when(z == 0)
                    def _():
                        cut(k, j == 0, to_right)

                    @pl.when(z == PLANES - 1)
                    def _():
                        cut(k, j == 0, to_left)

            return 0

        lax.fori_loop(0, PLANES, one_plane, 0)

    def relay(k, at, zd, to_right):
        box = from_l if to_right else from_r
        go = right if to_right else left

        def body(n):
            for h in range(n):
                rows_h = pl.ds(h * (plane // n), plane // n)
                go(k, zd, h, n).wait_recv()
                part[k, zd, rows_h] += box[k, zd, rows_h]
                go(k, zd, h, n).start()

        @pl.when(z == at)
        def _():
            cut(k, zd == (PLANES - 1 if to_right else 0), body)

    def forward_first(k):
        relay(k, 1, 3, True)
        relay(k, 2, 0, False)

    def forward_rest(k):
        relay(k, 1, 2, True)
        relay(k, 2, 1, False)
        relay(k, 1, 0, False)
        relay(k, 2, 3, True)

    def final_copy(k, m):
        src = part.at[k, z, pl.ds(m * tok, tok)]
        return remote(src, fin.at[k, q], send_f.at[k, m], recv_f.at[k, q], z * QUAD + m)

    def finish(k):
        for zd in range(PLANES):
            @pl.when(z == zd)
            def _():
                def from_left(n):
                    for h in range(n):
                        right(k, zd, h, n).wait_recv()

                def from_right(n):
                    for h in range(n):
                        left(k, zd, h, n).wait_recv()

                if zd > 0:
                    cut(k, zd == PLANES - 1, from_left)
                    part[k, zd] += from_l[k, zd]
                if zd < PLANES - 1:
                    cut(k, zd == 0, from_right)
                    part[k, zd] += from_r[k, zd]

        for m in others:
            final_copy(k, m).start()
        fin[k, q] = part[k, z, pl.ds(pl.multiple_of(q * tok, tok), tok), :]

    for k in range(steps):
        combine(k)
        if k > 0:
            forward_rest(k - 1)
        forward_first(k)
        if k > 0:
            finish(k - 1)
    forward_rest(steps - 1)
    finish(steps - 1)

    for k in range(steps):
        for m in others:
            remote(part.at[k, z, pl.ds(0, tok)], fin.at[k, m], send_f.at[k, m], recv_f.at[k, m], z * QUAD + m).wait_recv()
        for m in range(QUAD):
            cols = pl.ds((m * steps + k) * LANES, LANES)
            out_ref[:, cols] = (x_ref[:, cols].astype(F32) + fin[k, m]).astype(BF16)

    for k in range(steps):
        for m in others:
            quad_copy(k, m).wait_send()
            final_copy(k, m).wait_send()
        for zd in range(PLANES):
            @pl.when(z < zd)
            def _():
                def done(n):
                    for h in range(n):
                        right(k, zd, h, n).wait_send()

                cut(k, zd == PLANES - 1, done)

            @pl.when(z > zd)
            def _():
                def done(n):
                    for h in range(n):
                        left(k, zd, h, n).wait_send()

                cut(k, zd == 0, done)


def collect(ints, win, tokens, o_rows):
    tok, width = tokens.shape
    sub, r_tiles = o_rows.shape[:2]
    n_src = PLANES * QUAD
    steps = sub // QUAD
    vmem = pl.BlockSpec(memory_space=pltpu.VMEM)
    return pl.pallas_call(
        functools.partial(collect_kernel, n_src, steps),
        out_shape=jax.ShapeDtypeStruct((tok, width), BF16),
        in_specs=[pl.BlockSpec(memory_space=pltpu.SMEM), vmem, vmem, pl.BlockSpec(memory_space=pltpu.HBM)],
        out_specs=vmem,
        scratch_shapes=[
            pltpu.VMEM((n_src * QUAD, 3 * tok, WIN), BF16),
            pltpu.VMEM((steps, PLANES, QUAD * tok, LANES), F32),
            pltpu.VMEM((steps, PLANES, QUAD * tok, LANES), F32),
            pltpu.VMEM((steps, PLANES, QUAD * tok, LANES), F32),
            pltpu.VMEM((steps, QUAD, tok, LANES), F32),
            pltpu.SemaphoreType.DMA((steps, QUAD)),
            pltpu.SemaphoreType.DMA((steps, QUAD)),
            pltpu.SemaphoreType.DMA((steps, PLANES, CUTS)),
            pltpu.SemaphoreType.DMA((steps, PLANES, CUTS)),
            pltpu.SemaphoreType.DMA((steps, PLANES, CUTS)),
            pltpu.SemaphoreType.DMA((steps, QUAD)),
            pltpu.SemaphoreType.DMA((steps, QUAD)),
            pltpu.VMEM((steps, QUAD, r_tiles, TILE, LANES), BF16),
            pltpu.SemaphoreType.DMA((steps, QUAD)),
        ] + [pltpu.VMEM((QUAD, r_tiles, TILE, LANES), BF16)] * steps,
        compiler_params=pltpu.CompilerParams(collective_id=1, has_side_effects=True, vmem_limit_bytes=56 * 2 ** 20),
        name="collect",
    )(ints, win, tokens, o_rows)


def solution(mesh):
    ep_size = mesh.shape['ep']

    def device_step(tokens, expert_ids, norm_gain, w_router, w_gate, w_up, w_down):
        pairs = expert_ids.shape[0] * expert_ids.shape[1]
        r_max = 3 * pairs // 2
        u_rows, meta, ints = spread(r_max, tokens, expert_ids, norm_gain, w_router)
        u_rows = u_rows.reshape(-1, LANES)
        o_rows, win = experts(ep_size, r_max, ints, meta, u_rows, w_gate, w_up, w_down)
        return collect(ints, win, tokens, o_rows.reshape(-1, r_max // TILE, TILE, LANES))

    row_spec = P(('dp', 'ep'), None)
    expert_spec = P('ep', None, None)
    return jax.shard_map(device_step, mesh=mesh, in_specs=(row_spec, row_spec, P(None), P(None, None), expert_spec, expert_spec, expert_spec), out_specs=row_spec, check_vma=False)
```

```python
import functools

import jax
import jax.numpy as jnp
from jax import lax
from jax.experimental import pallas as pl
from jax.experimental.pallas import tpu as pltpu
from jax.sharding import PartitionSpec as P

NORM_EPS = 1e-5
LANES = 128
BM = 128
WIN = 256
CUTS = 2
TILE = 16
PITCH = 17
STEP = 8
MORE = 8
PIECES = 4
QUAD = 4
PLANES = 4
F32 = jnp.float32
BF16 = jnp.bfloat16


def iota(shape, dim):
    return lax.broadcasted_iota(jnp.int32, shape, dim)


def place():
    me = lax.axis_index('ep')
    return me, me // QUAD, lax.rem(me, QUAD)


def remote(src, dst, send, recv, dev):
    return pltpu.make_async_remote_copy(src_ref=src, dst_ref=dst, send_sem=send, recv_sem=recv,
                                        device_id={'ep': dev}, device_id_type=pl.DeviceIdType.MESH)


def spread_kernel(r_max, x_ref, ids_ref, gain_ref, wr_ref, u_hbm, meta_hbm, ints_hbm,
                  u_all, xs, ub, pos_s, p_s, packet, meta, ints,
                  send_u, recv_u, send_m, recv_m, out_sem):
    n_dev = PLANES * QUAD
    me, z, q = place()
    y, c = q // 2, lax.rem(q, 2)
    half = u_all.shape[1] // 2
    tok = x_ref.shape[0]
    sub = u_all.shape[1] // tok

    barrier = pltpu.get_barrier_semaphore()
    for d in range(1, n_dev):
        pl.semaphore_signal(barrier, inc=1, device_id={'ep': lax.rem(me + d, n_dev)}, device_id_type=pl.DeviceIdType.MESH)

    x32 = x_ref[...].astype(F32)
    inv = lax.rsqrt(jnp.mean(x32 * x32, axis=1, keepdims=True) + NORM_EPS)
    ub[...] = (x32 * inv * gain_ref[...].astype(F32)).astype(BF16)
    for j in range(sub):
        xs[pl.ds(j, tok, stride=sub), :] = ub[:, j * LANES:(j + 1) * LANES].astype(F32)
    u_all[me] = xs[...].astype(BF16)
    pl.semaphore_wait(barrier, n_dev - 1)

    dest = (me + QUAD, me - QUAD, z * QUAD + (1 - y) * 2 + c, z * QUAD + y * 2 + 1 - c)

    def hop(b, h, way):
        rows = u_all.at[b, pl.ds(h * half, half)]
        return remote(rows, rows, send_u.at[b, h, way], recv_u.at[b, h], dest[way])

    def out_copy(b, h):
        rows = pl.ds(h * half, half)
        return pltpu.make_async_copy(u_all.at[b, rows], u_hbm.at[b, rows], out_sem.at[b, h])

    def own_sends():
        for h in range(2):
            @pl.when(z < PLANES - 1)
            def _():
                hop(me, h, 0).start()

            @pl.when(z > 0)
            def _():
                hop(me, h, 1).start()

            hop(me, h, 2).start()
            hop(me, h, 3).start()
            out_copy(me, h).start()

    own_sends()

    logits = jnp.dot(ub[...], wr_ref[...], preferred_element_type=F32)
    top = jnp.max(logits, axis=1, keepdims=True)
    ex = jnp.exp(logits - top)
    p_s[...] = ex / jnp.sum(ex, axis=1, keepdims=True)
    lane = iota((tok, LANES), 1)
    hit = lane < 0
    ids = ids_ref[...].T
    for k in range(ids.shape[1]):
        hit = jnp.logical_or(hit, ids[:, k:k + 1] == lane)
    hit32 = hit.astype(F32)
    hit_b = hit32.astype(BF16)
    tri = (iota((tok, tok), 0) > iota((tok, tok), 1)).astype(F32).astype(BF16)
    rank = jnp.dot(tri, hit_b, preferred_element_type=F32)
    count = jnp.sum(hit32, axis=0, keepdims=True)
    row_e, col_e = iota((LANES, LANES), 0), iota((LANES, LANES), 1)
    e_loc = LANES // n_dev
    before = jnp.logical_and(row_e < col_e, row_e // e_loc == col_e // e_loc).astype(F32).astype(BF16)
    count8 = jnp.broadcast_to(count, (8, LANES))
    base = jnp.dot(count8.astype(BF16), before, preferred_element_type=F32)[0:1]
    pos_s[...] = jnp.where(hit, base + rank, -1.0)
    t_id = iota((tok, LANES), 0).astype(F32)
    lane_f = lane.astype(F32)

    def pack(zd, _):
        for m in range(QUAD):
            tk = jnp.zeros((tok, LANES), F32)
            gt = jnp.zeros((tok, LANES), F32)
            for ee in range(e_loc):
                col = m * e_loc + ee
                at = pos_s[:, col:col + 1] == lane_f
                tk = jnp.where(at, t_id, tk)
                gt = jnp.where(at, p_s[:, col:col + 1], gt)
            packet[zd, m:m + 1, :] = jnp.sum(tk, axis=0, keepdims=True)
            packet[zd, QUAD + m:QUAD + m + 1, :] = jnp.sum(gt, axis=0, keepdims=True)
        packet[zd, 8:16, :] = count8
        pos_s[...] = pltpu.roll(pos_s[...], LANES - QUAD * e_loc, 1)
        p_s[...] = pltpu.roll(p_s[...], LANES - QUAD * e_loc, 1)
        return 0

    lax.fori_loop(0, PLANES, pack, 0)

    def route_copy(d):
        return remote(packet.at[d // QUAD], meta.at[me], send_m.at[d], recv_m.at[me], d)

    for d in range(n_dev):
        @pl.when(d != me)
        def _():
            route_copy(d).start()

    meta[me] = packet[z]

    def take(b, h, ways):
        hop(b, h, 3).wait_recv()
        out_copy(b, h).start()
        for way in ways:
            hop(b, h, way).start()

    def from_z(d, fn):
        @pl.when(z >= d)
        def _():
            fn(me - QUAD * d, 0, z < PLANES - 1)

        @pl.when(z + d < PLANES)
        def _():
            fn(me + QUAD * d, 1, z > 0)

    def across(zb):
        return zb * QUAD + (1 - y) * 2 + c

    def step_z(d):
        for h in range(2):
            def on(b, way, more):
                hop(b, h, 3).wait_recv()

                @pl.when(more)
                def _():
                    hop(b, h, way).start()

                hop(b, h, 2).start()
                hop(b, h, 3).start()
                out_copy(b, h).start()

            from_z(d, on)

    def step_y(d):
        for h in range(2):
            if d == 0:
                take(across(z), h, (3,))
            else:
                @pl.when(z >= d)
                def _():
                    take(across(z - d), h, (3,))

                @pl.when(z + d < PLANES)
                def _():
                    take(across(z + d), h, (3,))

    step_z(1)
    step_y(0)
    step_z(2)
    step_y(1)
    step_z(3)
    step_y(2)
    step_y(3)
    for b in range(n_dev):
        @pl.when(b % 2 != c)
        def _():
            for h in range(2):
                hop(b, h, 3).wait_recv()
                out_copy(b, h).start()

    for d in range(n_dev):
        @pl.when(d != me)
        def _():
            remote(packet.at[0], meta.at[d], send_m.at[d], recv_m.at[d], d).wait_recv()

    cnt = meta[:, 8, :]
    group = (iota((LANES, LANES), 0) // e_loc == iota((LANES, LANES), 1)).astype(F32).astype(BF16)
    n_rows = jnp.dot(cnt.astype(BF16), group, preferred_element_type=F32)
    ints[0:16, LANES:] = jnp.zeros((16, LANES), jnp.int32)
    ints[0:16, :LANES] = (meta[:, pl.ds(q, 1), :].reshape(n_dev, LANES).astype(jnp.int32) + iota((n_dev, LANES), 0) * tok) * sub
    ints[16:32, :LANES] = cnt.astype(jnp.int32)
    run = jnp.zeros((1, LANES), F32)
    for s in range(n_dev):
        off = run.astype(jnp.int32)
        ints[32 + s:33 + s, :LANES] = off
        ints[48 + s:49 + s, :LANES] = jnp.minimum(off // TILE, (r_max - WIN) // TILE)
        run = run + n_rows[s:s + 1]

    tail = [pltpu.make_async_copy(meta, meta_hbm, out_sem.at[0, 2]), pltpu.make_async_copy(ints, ints_hbm, out_sem.at[1, 2])]
    for cp in tail:
        cp.start()

    for h in range(2):
        def sent(b, way, more):
            @pl.when(more)
            def _():
                hop(b, h, way).wait_send()

            hop(b, h, 2).wait_send()
            hop(b, h, 3).wait_send()

        @pl.when(z < PLANES - 1)
        def _():
            hop(me, h, 0).wait_send()

        @pl.when(z > 0)
        def _():
            hop(me, h, 1).wait_send()

        hop(me, h, 2).wait_send()
        hop(me, h, 3).wait_send()
        for d in range(1, PLANES):
            from_z(d, sent)
        for zb in range(PLANES):
            hop(across(zb), h, 3).wait_send()
        for b in range(n_dev):
            out_copy(b, h).wait()
    for d in range(n_dev):
        @pl.when(d != me)
        def _():
            route_copy(d).wait_send()
    for cp in tail:
        cp.wait()


def spread(r_max, tokens, expert_ids, norm_gain, w_router):
    tok, width = tokens.shape
    n_dev = PLANES * QUAD
    sub = width // LANES
    hbm = pl.BlockSpec(memory_space=pltpu.HBM)
    vmem = pl.BlockSpec(memory_space=pltpu.VMEM)
    return pl.pallas_call(
        functools.partial(spread_kernel, r_max),
        out_shape=(jax.ShapeDtypeStruct((n_dev, tok * sub, LANES), BF16),
                   jax.ShapeDtypeStruct((n_dev, 16, LANES), F32),
                   jax.ShapeDtypeStruct((64, 2 * LANES), jnp.int32)),
        in_specs=[vmem] * 4,
        out_specs=(hbm, hbm, hbm),
        scratch_shapes=[
            pltpu.VMEM((n_dev, tok * sub, LANES), BF16),
            pltpu.VMEM((tok * sub, LANES), F32),
            pltpu.VMEM((tok, width), BF16),
            pltpu.VMEM((tok, LANES), F32),
            pltpu.VMEM((tok, LANES), F32),
            pltpu.VMEM((PLANES, 16, LANES), F32),
            pltpu.VMEM((n_dev, 16, LANES), F32),
            pltpu.VMEM((64, 2 * LANES), jnp.int32),
            pltpu.SemaphoreType.DMA((n_dev, 2, 4)),
            pltpu.SemaphoreType.DMA((n_dev, 2)),
            pltpu.SemaphoreType.DMA((n_dev,)),
            pltpu.SemaphoreType.DMA((n_dev,)),
            pltpu.SemaphoreType.DMA((n_dev, 3)),
        ],
        compiler_params=pltpu.CompilerParams(collective_id=0, has_side_effects=True, vmem_limit_bytes=66_000_000),
        name="spread",
    )(tokens, expert_ids.T, norm_gain.reshape(1, width), w_router)


def expert_kernel(n_src, sub, r_max, ints, meta, u_hbm, w1_hbm, w3_hbm, w2_hbm, o_hbm, win_hbm,
                  u_vm, o_all, xf, xb, hb, ob, win, w1, w3, w2, pre, sems, sem_w):
    n_exp = w1_hbm.shape[0]
    me, z, q = place()
    lane0 = me * n_exp

    def load(e, names):
        slot = lax.rem(e, 2)
        copies = []
        for i, (src, dst) in enumerate(((w1_hbm, w1), (w3_hbm, w3), (w2_hbm, w2))):
            if i in names:
                size = src.shape[1] // PIECES
                for p in range(PIECES):
                    part = pl.ds(p * size, size)
                    copies.append(pltpu.make_async_copy(src.at[e, part], dst.at[slot, part], sem_w.at[slot, i, p]))
        return copies

    def start(copies):
        for i, w in enumerate(copies):
            w.start(priority=i % 2)

    def begin():
        cp = pltpu.make_async_copy(u_hbm, u_vm, sems.at[0])
        cp.start()
        for e in range(2):
            start(load(e, (0, 1, 2)))
        for s in range(n_src):
            pre[s] = 0

        @pl.loop(0, r_max * PITCH // 256)
        def _(i):
            o_all[pl.ds(pl.multiple_of(i * 256, 256), 256), :] = jnp.zeros((256, LANES), F32)

        @pl.loop(0, n_src)
        def _(s):
            for m in range(QUAD):
                t = meta[s, m:m + 1, :]
                g = meta[s, QUAD + m:QUAD + m + 1, :]
                hi = g.astype(BF16).astype(F32)
                mid = (g - hi).astype(BF16).astype(F32)
                lo = (g - hi - mid).astype(BF16).astype(F32)
                rows = jnp.concatenate([t, hi, mid, lo, t, t, t, t], axis=0)
                rows = jnp.concatenate([rows, jnp.zeros((8, WIN - LANES), F32)], axis=1)
                r = z * QUAD + m
                win[s * QUAD + m] = pltpu.roll(rows, ints[32 + s, r] - TILE * ints[48 + s, r], 1)

        pltpu.make_async_copy(win, win_hbm, sems.at[1]).start()
        cp.wait()

    begin()

    def expert(e, _):
        slot = lax.rem(e, 2)
        def take(s, j0, n, i, at):
            src = u_vm[pl.ds(pl.multiple_of(ints[s, j0 + i], sub), sub), :]
            xf[pl.ds(at, sub), :] = src.astype(F32)

        def give(s, j0, n, i, at):
            o_all[pl.ds(at, sub), :] = xf[pl.ds(n + i * PITCH, sub), :]

        def sweep(body, target, spare):
            n = jnp.int32(0)
            top = jnp.int32(0)
            starts = []
            for s in range(n_src):
                cnt = ints[16 + s, lane0 + e]
                to = target(s, n)
                for i in range(STEP):
                    at = to + i * PITCH if target is by_row else jnp.where(i < cnt, to + i * PITCH, spare)
                    body(s, pre[s], n, i, at)
                starts.append(n)
                n = n + cnt * PITCH
                top = jnp.maximum(top, cnt)
            for s in range(n_src):
                cnt = ints[16 + s, lane0 + e]

                @pl.when(cnt > STEP)
                def _():
                    to = target(s, starts[s])
                    for i in range(STEP, STEP + MORE):
                        body(s, pre[s], starts[s], i, jnp.where(i < cnt, to + i * PITCH, spare))

                    @pl.when(cnt > STEP + MORE)
                    def _():
                        for i in range(STEP + MORE, STEP + 2 * MORE):
                            body(s, pre[s], starts[s], i, jnp.where(i < cnt, to + i * PITCH, spare))

            @pl.when(top > STEP + 2 * MORE)
            def _():
                def source(s, n):
                    cnt = ints[16 + s, lane0 + e]

                    def row(i, _):
                        body(s, pre[s], n, i, target(s, n) + i * PITCH)
                        return 0

                    lax.fori_loop(STEP + 2 * MORE, cnt, row, 0)
                    return n + cnt * PITCH

                lax.fori_loop(0, n_src, source, jnp.int32(0))

            return n

        def by_row(s, n):
            return n

        def by_slot(s, n):
            return (ints[32 + s, me] + pre[s]) * PITCH

        n = sweep(take, by_row, (r_max + 2 * STEP) * PITCH)

        for w in load(e, (0, 1, 2)):
            w.wait()

        def block(b, _):
            r0 = b * (BM * PITCH)
            for j in range(sub):
                xb[:, j * LANES:(j + 1) * LANES] = xf[pl.ds(r0 + j, BM, stride=PITCH), :].astype(BF16)
            g = jnp.dot(xb[...], w1[slot], preferred_element_type=F32)
            v = jnp.dot(xb[...], w3[slot], preferred_element_type=F32)
            hb[...] = (jax.nn.silu(g) * v).astype(BF16)
            for k in range(sub // 4):
                o = jnp.dot(hb[...], w2[slot, :, k * 512:(k + 1) * 512], preferred_element_type=F32)
                for j in range(4):
                    xf[pl.ds(r0 + k * 4 + j, BM, stride=PITCH), :] = o[:, j * LANES:(j + 1) * LANES]
            return 0

        lax.fori_loop(0, (n + BM * PITCH - 1) // (BM * PITCH), block, 0)

        sweep(give, by_slot, r_max * PITCH)
        for s in range(n_src):
            pre[s] = pre[s] + ints[16 + s, lane0 + e]

        @pl.when(e + 2 < n_exp)
        def _():
            start(load(e + 2, (0, 1, 2)))

        return 0

    lax.fori_loop(0, n_exp, expert, 0)

    def put(j):
        return pltpu.make_async_copy(ob.at[j % 4], o_hbm.at[j], sems.at[2 + j % 4])

    for j in range(sub):
        if j >= 4:
            put(j - 4).wait()
        ob[j % 4] = o_all[pl.ds(j, r_max, stride=PITCH), :].astype(BF16)
        put(j).start()
    for j in range(sub - 4, sub):
        put(j).wait()
    pltpu.make_async_copy(win, win_hbm, sems.at[1]).wait()


def experts(n_src, r_max, ints, meta, u_rows, w1, w3, w2):
    n_exp, width, ff = w1.shape
    sub = width // LANES
    n_tok = u_rows.shape[0] // sub
    hbm = pl.BlockSpec(memory_space=pltpu.HBM)
    smem = pl.BlockSpec(memory_space=pltpu.SMEM)
    return pl.pallas_call(
        functools.partial(expert_kernel, n_src, sub, r_max),
        out_shape=(jax.ShapeDtypeStruct((sub, r_max, LANES), BF16),
                   jax.ShapeDtypeStruct((n_src * QUAD, 8, WIN), F32)),
        in_specs=[smem, pl.BlockSpec(memory_space=pltpu.VMEM), hbm, hbm, hbm, hbm],
        out_specs=(hbm, hbm),
        scratch_shapes=[
            pltpu.VMEM((n_tok * sub, LANES), BF16),
            pltpu.VMEM(((r_max + 8) * PITCH, LANES), F32),
            pltpu.VMEM(((r_max + 2 * STEP + 8) * PITCH, LANES), F32),
            pltpu.VMEM((BM, width), BF16),
            pltpu.VMEM((BM, ff), BF16),
            pltpu.VMEM((4, r_max, LANES), BF16),
            pltpu.VMEM((n_src * QUAD, 8, WIN), F32),
            pltpu.VMEM((2, width, ff), BF16),
            pltpu.VMEM((2, width, ff), BF16),
            pltpu.VMEM((2, ff, width), BF16),
            pltpu.SMEM((n_src,), jnp.int32),
            pltpu.SemaphoreType.DMA((6,)),
            pltpu.SemaphoreType.DMA((2, 3, PIECES)),
        ],
        compiler_params=pltpu.CompilerParams(vmem_limit_bytes=66_000_000),
        name="experts",
    )(ints, meta, u_rows, w1, w3, w2)


def collect_kernel(n_src, steps, ints, win, x_ref, o_hbm, out_ref,
                   mix, part, from_l, from_r, fin,
                   send_q, recv_q, send_z, recv_l, recv_r, send_f, recv_f, stage, stage_sem, *rows):
    me, z, q = place()
    y, c = q // 2, lax.rem(q, 2)
    tok = x_ref.shape[0]
    plane = QUAD * tok
    others = ((1 - y) * 2 + c, (1 - y) * 2 + 1 - c, y * 2 + 1 - c)

    barrier = pltpu.get_barrier_semaphore()

    def hello(dev):
        pl.semaphore_signal(barrier, inc=1, device_id={'ep': dev}, device_id_type=pl.DeviceIdType.MESH)

    def stage_copy(k, m):
        return pltpu.make_async_copy(o_hbm.at[m * steps + k], stage.at[k, m], stage_sem.at[k, m])

    def own_copy(k):
        return pltpu.make_async_copy(o_hbm.at[q * steps + k], rows[k].at[q], recv_q.at[k, q])

    for k in range(steps):
        for m in others:
            stage_copy(k, m).start()
        own_copy(k).start()

    for m in others:
        hello(z * QUAD + m)

    @pl.when(z > 0)
    def _():
        hello(me - QUAD)

    @pl.when(z < PLANES - 1)
    def _():
        hello(me + QUAD)

    pl.semaphore_wait(barrier, 4 + (z + PLANES - 1) // PLANES - (z + 1) // PLANES)

    def quad_copy(k, m):
        return remote(stage.at[k, m], rows[k].at[q], send_q.at[k, m], recv_q.at[k, q], z * QUAD + m)

    def quad_wait(k, m):
        remote(stage.at[k, m], rows[k].at[m], send_q.at[k, m], recv_q.at[k, m], z * QUAD + m).wait_recv()

    def quad_sends():
        for k in range(steps):
            for m in others:
                stage_copy(k, m).wait()
                quad_copy(k, m).start()

    @pl.when(c == 0)
    def _():
        quad_sends()

    row_id = iota((tok, WIN), 0).astype(F32)

    def build(i, _):
        w = win[i]
        at = w[0:1] == row_id
        for part_i in range(3):
            mix[i, part_i * tok:(part_i + 1) * tok, :] = jnp.where(at, w[1 + part_i:2 + part_i], 0.0).astype(BF16)
        return 0

    lax.fori_loop(0, n_src * QUAD, build, 0)

    @pl.when(c == 1)
    def _():
        quad_sends()

    def right(k, zd, h, n):
        rows_h = pl.ds(h * (plane // n), plane // n)
        return remote(part.at[k, zd, rows_h], from_l.at[k, zd, rows_h], send_z.at[k, zd, h], recv_l.at[k, zd, h], me + QUAD)

    def left(k, zd, h, n):
        rows_h = pl.ds(h * (plane // n), plane // n)
        return remote(part.at[k, zd, rows_h], from_r.at[k, zd, rows_h], send_z.at[k, zd, h], recv_r.at[k, zd, h], me - QUAD)

    def cut(k, farthest, body):
        if k == 0 and farthest:
            @pl.when(c == 0)
            def _():
                body(1)

            @pl.when(c == 1)
            def _():
                body(2)
        else:
            body(1)

    def combine(k):
        own_copy(k).wait()
        for m in others:
            quad_wait(k, m)

        def token_block(s):
            acc = jnp.zeros((3 * tok, LANES), F32)
            for m in range(QUAD):
                start = ints[48 + s, z * QUAD + m]
                span = jnp.concatenate([rows[k][m, start + i] for i in range(WIN // TILE)], axis=0)
                acc += jnp.dot(mix[s * QUAD + m], span, preferred_element_type=F32)
            part[k, s // QUAD, pl.ds(pl.multiple_of(lax.rem(s, QUAD) * tok, tok), tok), :] = acc[0:tok] + acc[tok:2 * tok] + acc[2 * tok:]

        def one_plane(i, _):
            zd = (PLANES - 1 - i) * (1 - z // 2) + i * (z // 2)

            def one_block(m, _):
                token_block(zd * QUAD + m)
                return 0

            lax.fori_loop(0, QUAD, one_block, 0)

            for j in range(PLANES - 1):
                @pl.when(i == j)
                def _():
                    def to_right(n):
                        for h in range(n):
                            right(k, PLANES - 1 - j, h, n).start()

                    def to_left(n):
                        for h in range(n):
                            left(k, j, h, n).start()

                    @pl.when(z == 0)
                    def _():
                        cut(k, j == 0, to_right)

                    @pl.when(z == PLANES - 1)
                    def _():
                        cut(k, j == 0, to_left)

            return 0

        lax.fori_loop(0, PLANES, one_plane, 0)

    def relay(k, at, zd, to_right):
        box = from_l if to_right else from_r
        go = right if to_right else left

        def body(n):
            for h in range(n):
                rows_h = pl.ds(h * (plane // n), plane // n)
                go(k, zd, h, n).wait_recv()
                part[k, zd, rows_h] += box[k, zd, rows_h]
                go(k, zd, h, n).start()

        @pl.when(z == at)
        def _():
            cut(k, zd == (PLANES - 1 if to_right else 0), body)

    def forward_first(k):
        relay(k, 1, 3, True)
        relay(k, 2, 0, False)

    def forward_rest(k):
        relay(k, 1, 2, True)
        relay(k, 2, 1, False)
        relay(k, 1, 0, False)
        relay(k, 2, 3, True)

    def final_copy(k, m):
        src = part.at[k, z, pl.ds(m * tok, tok)]
        return remote(src, fin.at[k, q], send_f.at[k, m], recv_f.at[k, q], z * QUAD + m)

    def finish(k):
        for zd in range(PLANES):
            @pl.when(z == zd)
            def _():
                def from_left(n):
                    for h in range(n):
                        right(k, zd, h, n).wait_recv()

                def from_right(n):
                    for h in range(n):
                        left(k, zd, h, n).wait_recv()

                if zd > 0:
                    cut(k, zd == PLANES - 1, from_left)
                    part[k, zd] += from_l[k, zd]
                if zd < PLANES - 1:
                    cut(k, zd == 0, from_right)
                    part[k, zd] += from_r[k, zd]

        for m in others:
            final_copy(k, m).start()
        fin[k, q] = part[k, z, pl.ds(pl.multiple_of(q * tok, tok), tok), :]

    for k in range(steps):
        combine(k)
        if k > 0:
            forward_rest(k - 1)
        forward_first(k)
        if k > 0:
            finish(k - 1)
    forward_rest(steps - 1)
    finish(steps - 1)

    for k in range(steps):
        for m in others:
            remote(part.at[k, z, pl.ds(0, tok)], fin.at[k, m], send_f.at[k, m], recv_f.at[k, m], z * QUAD + m).wait_recv()
        for m in range(QUAD):
            cols = pl.ds((m * steps + k) * LANES, LANES)
            out_ref[:, cols] = (x_ref[:, cols].astype(F32) + fin[k, m]).astype(BF16)

    for k in range(steps):
        for m in others:
            quad_copy(k, m).wait_send()
            final_copy(k, m).wait_send()
        for zd in range(PLANES):
            @pl.when(z < zd)
            def _():
                def done(n):
                    for h in range(n):
                        right(k, zd, h, n).wait_send()

                cut(k, zd == PLANES - 1, done)

            @pl.when(z > zd)
            def _():
                def done(n):
                    for h in range(n):
                        left(k, zd, h, n).wait_send()

                cut(k, zd == 0, done)


def collect(ints, win, tokens, o_rows):
    tok, width = tokens.shape
    sub, r_tiles = o_rows.shape[:2]
    n_src = PLANES * QUAD
    steps = sub // QUAD
    vmem = pl.BlockSpec(memory_space=pltpu.VMEM)
    return pl.pallas_call(
        functools.partial(collect_kernel, n_src, steps),
        out_shape=jax.ShapeDtypeStruct((tok, width), BF16),
        in_specs=[pl.BlockSpec(memory_space=pltpu.SMEM), vmem, vmem, pl.BlockSpec(memory_space=pltpu.HBM)],
        out_specs=vmem,
        scratch_shapes=[
            pltpu.VMEM((n_src * QUAD, 3 * tok, WIN), BF16),
            pltpu.VMEM((steps, PLANES, QUAD * tok, LANES), F32),
            pltpu.VMEM((steps, PLANES, QUAD * tok, LANES), F32),
            pltpu.VMEM((steps, PLANES, QUAD * tok, LANES), F32),
            pltpu.VMEM((steps, QUAD, tok, LANES), F32),
            pltpu.SemaphoreType.DMA((steps, QUAD)),
            pltpu.SemaphoreType.DMA((steps, QUAD)),
            pltpu.SemaphoreType.DMA((steps, PLANES, CUTS)),
            pltpu.SemaphoreType.DMA((steps, PLANES, CUTS)),
            pltpu.SemaphoreType.DMA((steps, PLANES, CUTS)),
            pltpu.SemaphoreType.DMA((steps, QUAD)),
            pltpu.SemaphoreType.DMA((steps, QUAD)),
            pltpu.VMEM((steps, QUAD, r_tiles, TILE, LANES), BF16),
            pltpu.SemaphoreType.DMA((steps, QUAD)),
        ] + [pltpu.VMEM((QUAD, r_tiles, TILE, LANES), BF16)] * steps,
        compiler_params=pltpu.CompilerParams(collective_id=1, has_side_effects=True, vmem_limit_bytes=56 * 2 ** 20),
        name="collect",
    )(ints, win, tokens, o_rows)


def solution(mesh):
    ep_size = mesh.shape['ep']

    def device_step(tokens, expert_ids, norm_gain, w_router, w_gate, w_up, w_down):
        pairs = expert_ids.shape[0] * expert_ids.shape[1]
        r_max = 3 * pairs // 2
        u_rows, meta, ints = spread(r_max, tokens, expert_ids, norm_gain, w_router)
        u_rows = u_rows.reshape(-1, LANES)
        o_rows, win = experts(ep_size, r_max, ints, meta, u_rows, w_gate, w_up, w_down)
        return collect(ints, win, tokens, o_rows.reshape(-1, r_max // TILE, TILE, LANES))

    row_spec = P(('dp', 'ep'), None)
    expert_spec = P('ep', None, None)
    return jax.shard_map(device_step, mesh=mesh, in_specs=(row_spec, row_spec, P(None), P(None, None), expert_spec, expert_spec, expert_spec), out_specs=row_spec, check_vma=False)
```

```python
import functools

import jax
import jax.numpy as jnp
from jax import lax
from jax.experimental import pallas as pl
from jax.experimental.pallas import tpu as pltpu
from jax.sharding import PartitionSpec as P

NORM_EPS = 1e-5
LANES = 128
BM = 128
WIN = 256
CUTS = 2
TILE = 16
PITCH = 17
STEP = 8
MORE = 8
PIECES = 4
QUAD = 4
PLANES = 4
F32 = jnp.float32
BF16 = jnp.bfloat16


def iota(shape, dim):
    return lax.broadcasted_iota(jnp.int32, shape, dim)


def place():
    me = lax.axis_index('ep')
    return me, me // QUAD, lax.rem(me, QUAD)


def remote(src, dst, send, recv, dev):
    return pltpu.make_async_remote_copy(src_ref=src, dst_ref=dst, send_sem=send, recv_sem=recv,
                                        device_id={'ep': dev}, device_id_type=pl.DeviceIdType.MESH)


def spread_kernel(r_max, x_ref, ids_ref, gain_ref, wr_ref, u_hbm, meta_hbm, ints_hbm,
                  u_all, xs, ub, pos_s, p_s, packet, meta, ints,
                  send_u, recv_u, send_m, recv_m, out_sem):
    n_dev = PLANES * QUAD
    me, z, q = place()
    y, c = q // 2, lax.rem(q, 2)
    half = u_all.shape[1] // 2
    tok = x_ref.shape[0]
    sub = u_all.shape[1] // tok

    barrier = pltpu.get_barrier_semaphore()
    for d in range(1, n_dev):
        pl.semaphore_signal(barrier, inc=1, device_id={'ep': lax.rem(me + d, n_dev)}, device_id_type=pl.DeviceIdType.MESH)

    x32 = x_ref[...].astype(F32)
    inv = lax.rsqrt(jnp.mean(x32 * x32, axis=1, keepdims=True) + NORM_EPS)
    ub[...] = (x32 * inv * gain_ref[...].astype(F32)).astype(BF16)
    for j in range(sub):
        xs[pl.ds(j, tok, stride=sub), :] = ub[:, j * LANES:(j + 1) * LANES].astype(F32)
    u_all[me] = xs[...].astype(BF16)
    pl.semaphore_wait(barrier, n_dev - 1)

    dest = (me + QUAD, me - QUAD, z * QUAD + (1 - y) * 2 + c, z * QUAD + y * 2 + 1 - c)

    def hop(b, h, way):
        rows = u_all.at[b, pl.ds(h * half, half)]
        return remote(rows, rows, send_u.at[b, h, way], recv_u.at[b, h], dest[way])

    def out_copy(b, h):
        rows = pl.ds(h * half, half)
        return pltpu.make_async_copy(u_all.at[b, rows], u_hbm.at[b, rows], out_sem.at[b, h])

    def own_sends():
        for h in range(2):
            @pl.when(z < PLANES - 1)
            def _():
                hop(me, h, 0).start()

            @pl.when(z > 0)
            def _():
                hop(me, h, 1).start()

            hop(me, h, 2).start()
            hop(me, h, 3).start()
            out_copy(me, h).start()

    own_sends()

    logits = jnp.dot(ub[...], wr_ref[...], preferred_element_type=F32)
    top = jnp.max(logits, axis=1, keepdims=True)
    ex = jnp.exp(logits - top)
    p_s[...] = ex / jnp.sum(ex, axis=1, keepdims=True)
    lane = iota((tok, LANES), 1)
    hit = lane < 0
    ids = ids_ref[...].T
    for k in range(ids.shape[1]):
        hit = jnp.logical_or(hit, ids[:, k:k + 1] == lane)
    hit32 = hit.astype(F32)
    hit_b = hit32.astype(BF16)
    tri = (iota((tok, tok), 0) > iota((tok, tok), 1)).astype(F32).astype(BF16)
    rank = jnp.dot(tri, hit_b, preferred_element_type=F32)
    count = jnp.sum(hit32, axis=0, keepdims=True)
    row_e, col_e = iota((LANES, LANES), 0), iota((LANES, LANES), 1)
    e_loc = LANES // n_dev
    before = jnp.logical_and(row_e < col_e, row_e // e_loc == col_e // e_loc).astype(F32).astype(BF16)
    count8 = jnp.broadcast_to(count, (8, LANES))
    base = jnp.dot(count8.astype(BF16), before, preferred_element_type=F32)[0:1]
    pos_s[...] = jnp.where(hit, base + rank, -1.0)
    t_id = iota((tok, LANES), 0).astype(F32)
    lane_f = lane.astype(F32)

    def pack(zd, _):
        for m in range(QUAD):
            tk = jnp.zeros((tok, LANES), F32)
            gt = jnp.zeros((tok, LANES), F32)
            for ee in range(e_loc):
                col = m * e_loc + ee
                at = pos_s[:, col:col + 1] == lane_f
                tk = jnp.where(at, t_id, tk)
                gt = jnp.where(at, p_s[:, col:col + 1], gt)
            packet[zd, m:m + 1, :] = jnp.sum(tk, axis=0, keepdims=True)
            packet[zd, QUAD + m:QUAD + m + 1, :] = jnp.sum(gt, axis=0, keepdims=True)
        packet[zd, 8:16, :] = count8
        pos_s[...] = pltpu.roll(pos_s[...], LANES - QUAD * e_loc, 1)
        p_s[...] = pltpu.roll(p_s[...], LANES - QUAD * e_loc, 1)
        return 0

    lax.fori_loop(0, PLANES, pack, 0)

    def route_copy(d):
        return remote(packet.at[d // QUAD], meta.at[me], send_m.at[d], recv_m.at[me], d)

    meta[me] = packet[z]

    def take(b, h, ways):
        hop(b, h, 3).wait_recv()
        out_copy(b, h).start()
        for way in ways:
            hop(b, h, way).start()

    def from_z(d, fn):
        @pl.when(z >= d)
        def _():
            fn(me - QUAD * d, 0, z < PLANES - 1)

        @pl.when(z + d < PLANES)
        def _():
            fn(me + QUAD * d, 1, z > 0)

    def across(zb):
        return zb * QUAD + (1 - y) * 2 + c

    def step_z(d):
        for h in range(2):
            def on(b, way, more):
                hop(b, h, 3).wait_recv()

                @pl.when(more)
                def _():
                    hop(b, h, way).start()

                hop(b, h, 2).start()
                hop(b, h, 3).start()
                out_copy(b, h).start()

            from_z(d, on)

    def step_y(d):
        for h in range(2):
            if d == 0:
                take(across(z), h, (3,))
            else:
                @pl.when(z >= d)
                def _():
                    take(across(z - d), h, (3,))

                @pl.when(z + d < PLANES)
                def _():
                    take(across(z + d), h, (3,))

    step_z(1)
    step_y(0)
    step_z(2)
    step_y(1)
    step_z(3)
    for d in range(n_dev):
        @pl.when(d != me)
        def _():
            route_copy(d).start()

    step_y(2)
    step_y(3)
    for b in range(n_dev):
        @pl.when(b % 2 != c)
        def _():
            for h in range(2):
                hop(b, h, 3).wait_recv()
                out_copy(b, h).start()

    for d in range(n_dev):
        @pl.when(d != me)
        def _():
            remote(packet.at[0], meta.at[d], send_m.at[d], recv_m.at[d], d).wait_recv()

    cnt = meta[:, 8, :]
    group = (iota((LANES, LANES), 0) // e_loc == iota((LANES, LANES), 1)).astype(F32).astype(BF16)
    n_rows = jnp.dot(cnt.astype(BF16), group, preferred_element_type=F32)
    ints[0:16, LANES:] = jnp.zeros((16, LANES), jnp.int32)
    ints[0:16, :LANES] = (meta[:, pl.ds(q, 1), :].reshape(n_dev, LANES).astype(jnp.int32) + iota((n_dev, LANES), 0) * tok) * sub
    ints[16:32, :LANES] = cnt.astype(jnp.int32)
    run = jnp.zeros((1, LANES), F32)
    for s in range(n_dev):
        off = run.astype(jnp.int32)
        ints[32 + s:33 + s, :LANES] = off
        ints[48 + s:49 + s, :LANES] = jnp.minimum(off // TILE, (r_max - WIN) // TILE)
        run = run + n_rows[s:s + 1]

    tail = [pltpu.make_async_copy(meta, meta_hbm, out_sem.at[0, 2]), pltpu.make_async_copy(ints, ints_hbm, out_sem.at[1, 2])]
    for cp in tail:
        cp.start()

    for h in range(2):
        def sent(b, way, more):
            @pl.when(more)
            def _():
                hop(b, h, way).wait_send()

            hop(b, h, 2).wait_send()
            hop(b, h, 3).wait_send()

        @pl.when(z < PLANES - 1)
        def _():
            hop(me, h, 0).wait_send()

        @pl.when(z > 0)
        def _():
            hop(me, h, 1).wait_send()

        hop(me, h, 2).wait_send()
        hop(me, h, 3).wait_send()
        for d in range(1, PLANES):
            from_z(d, sent)
        for zb in range(PLANES):
            hop(across(zb), h, 3).wait_send()
        for b in range(n_dev):
            out_copy(b, h).wait()
    for d in range(n_dev):
        @pl.when(d != me)
        def _():
            route_copy(d).wait_send()
    for cp in tail:
        cp.wait()


def spread(r_max, tokens, expert_ids, norm_gain, w_router):
    tok, width = tokens.shape
    n_dev = PLANES * QUAD
    sub = width // LANES
    hbm = pl.BlockSpec(memory_space=pltpu.HBM)
    vmem = pl.BlockSpec(memory_space=pltpu.VMEM)
    return pl.pallas_call(
        functools.partial(spread_kernel, r_max),
        out_shape=(jax.ShapeDtypeStruct((n_dev, tok * sub, LANES), BF16),
                   jax.ShapeDtypeStruct((n_dev, 16, LANES), F32),
                   jax.ShapeDtypeStruct((64, 2 * LANES), jnp.int32)),
        in_specs=[vmem] * 4,
        out_specs=(hbm, hbm, hbm),
        scratch_shapes=[
            pltpu.VMEM((n_dev, tok * sub, LANES), BF16),
            pltpu.VMEM((tok * sub, LANES), F32),
            pltpu.VMEM((tok, width), BF16),
            pltpu.VMEM((tok, LANES), F32),
            pltpu.VMEM((tok, LANES), F32),
            pltpu.VMEM((PLANES, 16, LANES), F32),
            pltpu.VMEM((n_dev, 16, LANES), F32),
            pltpu.VMEM((64, 2 * LANES), jnp.int32),
            pltpu.SemaphoreType.DMA((n_dev, 2, 4)),
            pltpu.SemaphoreType.DMA((n_dev, 2)),
            pltpu.SemaphoreType.DMA((n_dev,)),
            pltpu.SemaphoreType.DMA((n_dev,)),
            pltpu.SemaphoreType.DMA((n_dev, 3)),
        ],
        compiler_params=pltpu.CompilerParams(collective_id=0, has_side_effects=True, vmem_limit_bytes=66_000_000),
        name="spread",
    )(tokens, expert_ids.T, norm_gain.reshape(1, width), w_router)


def expert_kernel(n_src, sub, r_max, ints, meta, u_hbm, w1_hbm, w3_hbm, w2_hbm, o_hbm, win_hbm,
                  u_vm, o_all, xf, xb, hb, ob, win, w1, w3, w2, pre, sems, sem_w):
    n_exp = w1_hbm.shape[0]
    me, z, q = place()
    lane0 = me * n_exp

    def load(e, names):
        slot = lax.rem(e, 2)
        copies = []
        for i, (src, dst) in enumerate(((w1_hbm, w1), (w3_hbm, w3), (w2_hbm, w2))):
            if i in names:
                size = src.shape[1] // PIECES
                for p in range(PIECES):
                    part = pl.ds(p * size, size)
                    copies.append(pltpu.make_async_copy(src.at[e, part], dst.at[slot, part], sem_w.at[slot, i, p]))
        return copies

    def start(copies):
        for i, w in enumerate(copies):
            w.start(priority=i % 2)

    def begin():
        cp = pltpu.make_async_copy(u_hbm, u_vm, sems.at[0])
        cp.start()
        for e in range(2):
            start(load(e, (0, 1, 2)))
        for s in range(n_src):
            pre[s] = 0

        @pl.loop(0, r_max * PITCH // 256)
        def _(i):
            o_all[pl.ds(pl.multiple_of(i * 256, 256), 256), :] = jnp.zeros((256, LANES), F32)

        @pl.loop(0, n_src)
        def _(s):
            for m in range(QUAD):
                t = meta[s, m:m + 1, :]
                g = meta[s, QUAD + m:QUAD + m + 1, :]
                hi = g.astype(BF16).astype(F32)
                mid = (g - hi).astype(BF16).astype(F32)
                lo = (g - hi - mid).astype(BF16).astype(F32)
                rows = jnp.concatenate([t, hi, mid, lo, t, t, t, t], axis=0)
                rows = jnp.concatenate([rows, jnp.zeros((8, WIN - LANES), F32)], axis=1)
                r = z * QUAD + m
                win[s * QUAD + m] = pltpu.roll(rows, ints[32 + s, r] - TILE * ints[48 + s, r], 1)

        pltpu.make_async_copy(win, win_hbm, sems.at[1]).start()
        cp.wait()

    begin()

    def expert(e, _):
        slot = lax.rem(e, 2)
        def take(s, j0, n, i, at):
            src = u_vm[pl.ds(pl.multiple_of(ints[s, j0 + i], sub), sub), :]
            xf[pl.ds(at, sub), :] = src.astype(F32)

        def give(s, j0, n, i, at):
            o_all[pl.ds(at, sub), :] = xf[pl.ds(n + i * PITCH, sub), :]

        def sweep(body, target, spare):
            n = jnp.int32(0)
            top = jnp.int32(0)
            starts = []
            for s in range(n_src):
                cnt = ints[16 + s, lane0 + e]
                to = target(s, n)
                for i in range(STEP):
                    at = to + i * PITCH if target is by_row else jnp.where(i < cnt, to + i * PITCH, spare)
                    body(s, pre[s], n, i, at)
                starts.append(n)
                n = n + cnt * PITCH
                top = jnp.maximum(top, cnt)
            for s in range(n_src):
                cnt = ints[16 + s, lane0 + e]

                @pl.when(cnt > STEP)
                def _():
                    to = target(s, starts[s])
                    for i in range(STEP, STEP + MORE):
                        body(s, pre[s], starts[s], i, jnp.where(i < cnt, to + i * PITCH, spare))

                    @pl.when(cnt > STEP + MORE)
                    def _():
                        for i in range(STEP + MORE, STEP + 2 * MORE):
                            body(s, pre[s], starts[s], i, jnp.where(i < cnt, to + i * PITCH, spare))

            @pl.when(top > STEP + 2 * MORE)
            def _():
                def source(s, n):
                    cnt = ints[16 + s, lane0 + e]

                    def row(i, _):
                        body(s, pre[s], n, i, target(s, n) + i * PITCH)
                        return 0

                    lax.fori_loop(STEP + 2 * MORE, cnt, row, 0)
                    return n + cnt * PITCH

                lax.fori_loop(0, n_src, source, jnp.int32(0))

            return n

        def by_row(s, n):
            return n

        def by_slot(s, n):
            return (ints[32 + s, me] + pre[s]) * PITCH

        n = sweep(take, by_row, (r_max + 2 * STEP) * PITCH)

        for w in load(e, (0, 1, 2)):
            w.wait()

        def block(b, _):
            r0 = b * (BM * PITCH)
            for j in range(sub):
                xb[:, j * LANES:(j + 1) * LANES] = xf[pl.ds(r0 + j, BM, stride=PITCH), :].astype(BF16)
            g = jnp.dot(xb[...], w1[slot], preferred_element_type=F32)
            v = jnp.dot(xb[...], w3[slot], preferred_element_type=F32)
            hb[...] = (jax.nn.silu(g) * v).astype(BF16)
            for k in range(sub // 4):
                o = jnp.dot(hb[...], w2[slot, :, k * 512:(k + 1) * 512], preferred_element_type=F32)
                for j in range(4):
                    xf[pl.ds(r0 + k * 4 + j, BM, stride=PITCH), :] = o[:, j * LANES:(j + 1) * LANES]
            return 0

        lax.fori_loop(0, (n + BM * PITCH - 1) // (BM * PITCH), block, 0)

        sweep(give, by_slot, r_max * PITCH)
        for s in range(n_src):
            pre[s] = pre[s] + ints[16 + s, lane0 + e]

        @pl.when(e + 2 < n_exp)
        def _():
            start(load(e + 2, (0, 1, 2)))

        return 0

    lax.fori_loop(0, n_exp, expert, 0)

    def put(j):
        return pltpu.make_async_copy(ob.at[j % 4], o_hbm.at[j], sems.at[2 + j % 4])

    for j in range(sub):
        if j >= 4:
            put(j - 4).wait()
        ob[j % 4] = o_all[pl.ds(j, r_max, stride=PITCH), :].astype(BF16)
        put(j).start()
    for j in range(sub - 4, sub):
        put(j).wait()
    pltpu.make_async_copy(win, win_hbm, sems.at[1]).wait()


def experts(n_src, r_max, ints, meta, u_rows, w1, w3, w2):
    n_exp, width, ff = w1.shape
    sub = width // LANES
    n_tok = u_rows.shape[0] // sub
    hbm = pl.BlockSpec(memory_space=pltpu.HBM)
    smem = pl.BlockSpec(memory_space=pltpu.SMEM)
    return pl.pallas_call(
        functools.partial(expert_kernel, n_src, sub, r_max),
        out_shape=(jax.ShapeDtypeStruct((sub, r_max, LANES), BF16),
                   jax.ShapeDtypeStruct((n_src * QUAD, 8, WIN), F32)),
        in_specs=[smem, pl.BlockSpec(memory_space=pltpu.VMEM), hbm, hbm, hbm, hbm],
        out_specs=(hbm, hbm),
        scratch_shapes=[
            pltpu.VMEM((n_tok * sub, LANES), BF16),
            pltpu.VMEM(((r_max + 8) * PITCH, LANES), F32),
            pltpu.VMEM(((r_max + 2 * STEP + 8) * PITCH, LANES), F32),
            pltpu.VMEM((BM, width), BF16),
            pltpu.VMEM((BM, ff), BF16),
            pltpu.VMEM((4, r_max, LANES), BF16),
            pltpu.VMEM((n_src * QUAD, 8, WIN), F32),
            pltpu.VMEM((2, width, ff), BF16),
            pltpu.VMEM((2, width, ff), BF16),
            pltpu.VMEM((2, ff, width), BF16),
            pltpu.SMEM((n_src,), jnp.int32),
            pltpu.SemaphoreType.DMA((6,)),
            pltpu.SemaphoreType.DMA((2, 3, PIECES)),
        ],
        compiler_params=pltpu.CompilerParams(vmem_limit_bytes=66_000_000),
        name="experts",
    )(ints, meta, u_rows, w1, w3, w2)


def collect_kernel(n_src, steps, ints, win, x_ref, o_hbm, out_ref,
                   mix, part, from_l, from_r, fin,
                   send_q, recv_q, send_z, recv_l, recv_r, send_f, recv_f, stage, stage_sem, *rows):
    me, z, q = place()
    y, c = q // 2, lax.rem(q, 2)
    tok = x_ref.shape[0]
    plane = QUAD * tok
    others = ((1 - y) * 2 + c, (1 - y) * 2 + 1 - c, y * 2 + 1 - c)

    barrier = pltpu.get_barrier_semaphore()

    def hello(dev):
        pl.semaphore_signal(barrier, inc=1, device_id={'ep': dev}, device_id_type=pl.DeviceIdType.MESH)

    def stage_copy(k, m):
        return pltpu.make_async_copy(o_hbm.at[m * steps + k], stage.at[k, m], stage_sem.at[k, m])

    def own_copy(k):
        return pltpu.make_async_copy(o_hbm.at[q * steps + k], rows[k].at[q], recv_q.at[k, q])

    for k in range(steps):
        for m in others:
            stage_copy(k, m).start()
        own_copy(k).start()

    for m in others:
        hello(z * QUAD + m)

    @pl.when(z > 0)
    def _():
        hello(me - QUAD)

    @pl.when(z < PLANES - 1)
    def _():
        hello(me + QUAD)

    pl.semaphore_wait(barrier, 4 + (z + PLANES - 1) // PLANES - (z + 1) // PLANES)

    def quad_copy(k, m):
        return remote(stage.at[k, m], rows[k].at[q], send_q.at[k, m], recv_q.at[k, q], z * QUAD + m)

    def quad_wait(k, m):
        remote(stage.at[k, m], rows[k].at[m], send_q.at[k, m], recv_q.at[k, m], z * QUAD + m).wait_recv()

    def quad_sends():
        for k in range(steps):
            for m in others:
                stage_copy(k, m).wait()
                quad_copy(k, m).start()

    @pl.when(c == 0)
    def _():
        quad_sends()

    row_id = iota((tok, WIN), 0).astype(F32)

    def build(i, _):
        w = win[i]
        at = w[0:1] == row_id
        for part_i in range(3):
            mix[i, part_i * tok:(part_i + 1) * tok, :] = jnp.where(at, w[1 + part_i:2 + part_i], 0.0).astype(BF16)
        return 0

    lax.fori_loop(0, n_src * QUAD, build, 0)

    @pl.when(c == 1)
    def _():
        quad_sends()

    def right(k, zd, h, n):
        rows_h = pl.ds(h * (plane // n), plane // n)
        return remote(part.at[k, zd, rows_h], from_l.at[k, zd, rows_h], send_z.at[k, zd, h], recv_l.at[k, zd, h], me + QUAD)

    def left(k, zd, h, n):
        rows_h = pl.ds(h * (plane // n), plane // n)
        return remote(part.at[k, zd, rows_h], from_r.at[k, zd, rows_h], send_z.at[k, zd, h], recv_r.at[k, zd, h], me - QUAD)

    def cut(k, farthest, body):
        if k == 0 and farthest:
            @pl.when(c == 0)
            def _():
                body(1)

            @pl.when(c == 1)
            def _():
                body(2)
        else:
            body(1)

    def combine(k):
        own_copy(k).wait()
        for m in others:
            quad_wait(k, m)

        def token_block(s):
            acc = jnp.zeros((3 * tok, LANES), F32)
            for m in range(QUAD):
                start = ints[48 + s, z * QUAD + m]
                span = jnp.concatenate([rows[k][m, start + i] for i in range(WIN // TILE)], axis=0)
                acc += jnp.dot(mix[s * QUAD + m], span, preferred_element_type=F32)
            part[k, s // QUAD, pl.ds(pl.multiple_of(lax.rem(s, QUAD) * tok, tok), tok), :] = acc[0:tok] + acc[tok:2 * tok] + acc[2 * tok:]

        def one_plane(i, _):
            zd = (PLANES - 1 - i) * (1 - z // 2) + i * (z // 2)

            def one_block(m, _):
                token_block(zd * QUAD + m)
                return 0

            lax.fori_loop(0, QUAD, one_block, 0)

            for j in range(PLANES - 1):
                @pl.when(i == j)
                def _():
                    def to_right(n):
                        for h in range(n):
                            right(k, PLANES - 1 - j, h, n).start()

                    def to_left(n):
                        for h in range(n):
                            left(k, j, h, n).start()

                    @pl.when(z == 0)
                    def _():
                        cut(k, j == 0, to_right)

                    @pl.when(z == PLANES - 1)
                    def _():
                        cut(k, j == 0, to_left)

            return 0

        lax.fori_loop(0, PLANES, one_plane, 0)

    def relay(k, at, zd, to_right):
        box = from_l if to_right else from_r
        go = right if to_right else left

        def body(n):
            for h in range(n):
                rows_h = pl.ds(h * (plane // n), plane // n)
                go(k, zd, h, n).wait_recv()
                part[k, zd, rows_h] += box[k, zd, rows_h]
                go(k, zd, h, n).start()

        @pl.when(z == at)
        def _():
            cut(k, zd == (PLANES - 1 if to_right else 0), body)

    def forward_first(k):
        relay(k, 1, 3, True)
        relay(k, 2, 0, False)

    def forward_rest(k):
        relay(k, 1, 2, True)
        relay(k, 2, 1, False)
        relay(k, 1, 0, False)
        relay(k, 2, 3, True)

    def final_copy(k, m):
        src = part.at[k, z, pl.ds(m * tok, tok)]
        return remote(src, fin.at[k, q], send_f.at[k, m], recv_f.at[k, q], z * QUAD + m)

    def finish(k):
        for zd in range(PLANES):
            @pl.when(z == zd)
            def _():
                def from_left(n):
                    for h in range(n):
                        right(k, zd, h, n).wait_recv()

                def from_right(n):
                    for h in range(n):
                        left(k, zd, h, n).wait_recv()

                if zd > 0:
                    cut(k, zd == PLANES - 1, from_left)
                    part[k, zd] += from_l[k, zd]
                if zd < PLANES - 1:
                    cut(k, zd == 0, from_right)
                    part[k, zd] += from_r[k, zd]

        for m in others:
            final_copy(k, m).start()
        fin[k, q] = part[k, z, pl.ds(pl.multiple_of(q * tok, tok), tok), :]

    for k in range(steps):
        combine(k)
        if k > 0:
            forward_rest(k - 1)
        forward_first(k)
        if k > 0:
            finish(k - 1)
    forward_rest(steps - 1)
    finish(steps - 1)

    for k in range(steps):
        for m in others:
            remote(part.at[k, z, pl.ds(0, tok)], fin.at[k, m], send_f.at[k, m], recv_f.at[k, m], z * QUAD + m).wait_recv()
        for m in range(QUAD):
            cols = pl.ds((m * steps + k) * LANES, LANES)
            out_ref[:, cols] = (x_ref[:, cols].astype(F32) + fin[k, m]).astype(BF16)

    for k in range(steps):
        for m in others:
            quad_copy(k, m).wait_send()
            final_copy(k, m).wait_send()
        for zd in range(PLANES):
            @pl.when(z < zd)
            def _():
                def done(n):
                    for h in range(n):
                        right(k, zd, h, n).wait_send()

                cut(k, zd == PLANES - 1, done)

            @pl.when(z > zd)
            def _():
                def done(n):
                    for h in range(n):
                        left(k, zd, h, n).wait_send()

                cut(k, zd == 0, done)


def collect(ints, win, tokens, o_rows):
    tok, width = tokens.shape
    sub, r_tiles = o_rows.shape[:2]
    n_src = PLANES * QUAD
    steps = sub // QUAD
    vmem = pl.BlockSpec(memory_space=pltpu.VMEM)
    return pl.pallas_call(
        functools.partial(collect_kernel, n_src, steps),
        out_shape=jax.ShapeDtypeStruct((tok, width), BF16),
        in_specs=[pl.BlockSpec(memory_space=pltpu.SMEM), vmem, vmem, pl.BlockSpec(memory_space=pltpu.HBM)],
        out_specs=vmem,
        scratch_shapes=[
            pltpu.VMEM((n_src * QUAD, 3 * tok, WIN), BF16),
            pltpu.VMEM((steps, PLANES, QUAD * tok, LANES), F32),
            pltpu.VMEM((steps, PLANES, QUAD * tok, LANES), F32),
            pltpu.VMEM((steps, PLANES, QUAD * tok, LANES), F32),
            pltpu.VMEM((steps, QUAD, tok, LANES), F32),
            pltpu.SemaphoreType.DMA((steps, QUAD)),
            pltpu.SemaphoreType.DMA((steps, QUAD)),
            pltpu.SemaphoreType.DMA((steps, PLANES, CUTS)),
            pltpu.SemaphoreType.DMA((steps, PLANES, CUTS)),
            pltpu.SemaphoreType.DMA((steps, PLANES, CUTS)),
            pltpu.SemaphoreType.DMA((steps, QUAD)),
            pltpu.SemaphoreType.DMA((steps, QUAD)),
            pltpu.VMEM((steps, QUAD, r_tiles, TILE, LANES), BF16),
            pltpu.SemaphoreType.DMA((steps, QUAD)),
        ] + [pltpu.VMEM((QUAD, r_tiles, TILE, LANES), BF16)] * steps,
        compiler_params=pltpu.CompilerParams(collective_id=1, has_side_effects=True, vmem_limit_bytes=56 * 2 ** 20),
        name="collect",
    )(ints, win, tokens, o_rows)


def solution(mesh):
    ep_size = mesh.shape['ep']

    def device_step(tokens, expert_ids, norm_gain, w_router, w_gate, w_up, w_down):
        pairs = expert_ids.shape[0] * expert_ids.shape[1]
        r_max = 3 * pairs // 2
        u_rows, meta, ints = spread(r_max, tokens, expert_ids, norm_gain, w_router)
        u_rows = u_rows.reshape(-1, LANES)
        o_rows, win = experts(ep_size, r_max, ints, meta, u_rows, w_gate, w_up, w_down)
        return collect(ints, win, tokens, o_rows.reshape(-1, r_max // TILE, TILE, LANES))

    row_spec = P(('dp', 'ep'), None)
    expert_spec = P('ep', None, None)
    return jax.shard_map(device_step, mesh=mesh, in_specs=(row_spec, row_spec, P(None), P(None, None), expert_spec, expert_spec, expert_spec), out_specs=row_spec, check_vma=False)
```
